32 devices in a mesh: xz: 16 (over z, y, x), gy: 2 (over core).
Axes of the slice: x: 2, y: 2, z: 4, core: 2. Of those that a mesh axis runs over, the one named last changes fastest.
Arguments:
- initial_state: float32 [3, 2, 16, 512, 512], P(None, None, 'gy', 'xz'), may hold values from -6 to 6
- drag_rate: float32 [16, 512, 1024], P('gy', 'xz'), may hold values from 0.02 to 0.6
- wall_control: float32 [512, 1024], P('xz'), may hold values from -6 to 6
- lift_profile: float32 [16], replicated, may hold values from 0.05 to 0.3
- schur_inverse: float32 [16, 8, 512, 512], P('gy', None, 'xz'), may hold values from -1 to 3, as said below
Outputs:
- final_state: float32 [3, 2, 16, 512, 512], P(None, None, 'gy', 'xz')
- control_gradient: float32 [512, 1024], P('xz', 'gy')
The draws below stay inside these ranges and needn't reach their ends.
Inputs may be any that keep to these rules, and one draw needn't show every extreme that they name: `schur_inverse`: each 8 x 8 block of one wavenumber holds the precomputed inverse of a Schur complement; dimension 1 indexes the block's columns.
All inputs are finite; a program needn't handle non-finite values.
Results may differ from the reference program's by a relative error of at most 0.00014.
Values sent between devices are 32-bit elements; how exact they have to be, the bound alone decides.
A program may use at most 128 MiB of HBM per device.

```python
import math
import jax
import jax.numpy as jnp
from jax import lax

NX = 1024
NZ = 512
KX = 512
CY = 8
NY = 16
STEPS = 2
N_GY = 2


def draw_schur_inverse(key, part):
    subkeys = jax.random.split(key, 4)
    blocks = NY // CY
    full_shape = (blocks, CY, CY, NX // 2, NZ)
    diag_low = 0.4
    rank_weight = 0.6
    spread = 0.5
    diagonal = jax.random.uniform(subkeys[0], (blocks, CY, 1, NX // 2, NZ), jnp.float32, diag_low, 1.0)
    identity = (jnp.arange(CY)[:, None] == jnp.arange(CY)[None, :]).astype(jnp.float32)[None, :, :, None, None]
    jitter = jax.random.uniform(subkeys[1], full_shape, jnp.float32, -1.0, 1.0) * (spread / math.sqrt(CY))
    left_side = jax.random.uniform(subkeys[2], (blocks, CY, 1, NX // 2, NZ), jnp.float32, 0.5, 1.0)
    right_side = jax.random.uniform(subkeys[3], (blocks, 1, CY, NX // 2, NZ), jnp.float32, 0.5, 1.0)
    blocked = identity * diagonal + jitter + rank_weight * left_side * right_side
    stream_wave = 2.0 * math.pi / NX * jnp.arange(NX // 2).astype(jnp.float32)
    span_ids = jnp.arange(NZ)
    signed = jnp.where(span_ids < NZ // 2, span_ids, span_ids - NZ)
    span_wave = jnp.where(span_ids == NZ // 2, 0.0, 2.0 * math.pi / NZ * signed.astype(jnp.float32))
    damping = 1.0 + stream_wave[:, None] ** 2 + span_wave[None, :] ** 2
    return (blocked / damping).reshape(NY, CY, NX // 2, NZ)


def level_of(own_key, extent, cuts, least, top_value):
    gain = 1.0
    for axis_at, blocks in cuts:
        steps = jax.random.uniform(jax.random.fold_in(jax.random.fold_in(own_key, 6), axis_at), (blocks,), jnp.float32, least / len(cuts), top_value / len(cuts))
        gain = gain * jnp.repeat(jnp.exp(steps), extent[axis_at] // blocks).reshape((-1,) + (1,) * (len(extent) - 1 - axis_at))
    return gain


def gaussian(rng, shape, width, reach, cuts=(), dtype=jnp.bfloat16):
    level = level_of(rng, shape, cuts, -0.22, 0.18) if cuts else 1.0
    entries = jax.random.normal(rng, shape, jnp.float32) * width * level
    return jnp.minimum(jnp.maximum(entries, -reach), reach).astype(dtype)


def setup_inputs(seed: int = 0) -> dict:
    seeds = jax.random.split(jax.random.key(seed), 6)
    return {
        "initial_state": gaussian(seeds[0], (3, 2, NY, KX, NZ), 1.0, 6.0, ((2, 2), (3, 16)), jnp.float32),
        "drag_rate": jnp.clip(jnp.exp(math.log(0.6) - 3.4011974 * jax.random.uniform(seeds[1], (NY, NZ, NX), jnp.float32) ** level_of(seeds[1], (NY, NZ, NX), ((0, 2), (1, 16)), -0.2, 0.2)), 0.02, 0.6),
        "wall_control": gaussian(seeds[2], (NZ, NX), 1.0, 6.0, ((0, 16),), jnp.float32),
        "lift_profile": jnp.clip(jnp.exp(jax.random.uniform(seeds[3], (NY,), jnp.float32, math.log(0.05), math.log(0.3))), 0.05, 0.3),
        "schur_inverse": draw_schur_inverse(jax.random.fold_in(seeds[5], 71), 0),
    }


DIFFUSION = 0.04

def pair_rotate(spectrum, factor):
    return jnp.stack([-factor * spectrum[1], factor * spectrum[0]])

def reference(initial_state, drag_rate, wall_control, lift_profile, schur_inverse):
    mode_ids = jnp.arange(KX)
    stream_factor = (2.0 * math.pi / NX * mode_ids.astype(jnp.float32))[:, None]
    span_ids = jnp.arange(NZ)
    signed = jnp.where(span_ids < NZ // 2, span_ids, span_ids - NZ)
    span_wave = jnp.where(span_ids == NZ // 2, 0.0, 2.0 * math.pi / NZ * signed.astype(jnp.float32))
    wave_square = stream_factor ** 2 + span_wave[None, :] ** 2

    def to_physical(spectral):
        values = lax.complex(spectral[0], spectral[1])
        values = jnp.fft.ifft(values, axis=2, norm='ortho')
        values = jnp.swapaxes(values, 1, 2)
        values = jnp.pad(values, ((0, 0), (0, 0), (0, 1)))
        return jnp.fft.irfft(values, n=NX, axis=2, norm='ortho')

    def to_spectral(physical):
        values = jnp.fft.rfft(physical, axis=2, norm='ortho')[:, :, :KX]
        values = jnp.swapaxes(values, 1, 2)
        values = jnp.fft.fft(values, axis=2, norm='ortho')
        return jnp.stack([jnp.real(values), jnp.imag(values)])

    def curvature(spectrum):
        padded = jnp.pad(spectrum, ((0, 0), (1, 1), (0, 0), (0, 0)))
        return padded[:, 2:] - 2.0 * spectrum + padded[:, :-2]

    def centred(spectrum):
        padded = jnp.pad(spectrum, ((0, 0), (1, 1), (0, 0), (0, 0)))
        return (padded[:, 2:] - padded[:, :-2]) / 2.0

    def solve(source):
        running = jnp.zeros((2, KX, NZ), jnp.float32)
        partials = []
        for block_index in range(N_GY):
            matrix = schur_inverse[block_index * CY:(block_index + 1) * CY]
            values = source[:, block_index * CY:(block_index + 1) * CY]
            summed = jnp.einsum('ijkq,cjkq->cikq', matrix, values, precision=lax.Precision.HIGHEST)
            partial_value = summed + matrix[:, 0][None] * running[:, None]
            running = partial_value[:, CY - 1]
            partials.append(partial_value)
        running = jnp.zeros((2, KX, NZ), jnp.float32)
        solved = [None] * N_GY
        for block_index in reversed(range(N_GY)):
            matrix = schur_inverse[block_index * CY:(block_index + 1) * CY]
            complete = partials[block_index] + matrix[:, CY - 1][None] * running[:, None]
            running = complete[:, 0]
            solved[block_index] = complete
        return jnp.concatenate(solved, axis=1)

    def evolve(control_plane):
        control_hat = to_spectral(control_plane[None])[:, 0]
        fields = initial_state
        for section_index in range(STEPS):
            stream_part = fields[0]
            normal_part = fields[1]
            span_part = fields[2]
            drag_term = to_spectral(drag_rate * to_physical(stream_part))
            stream_star = stream_part + DIFFUSION * (curvature(stream_part) - wave_square * stream_part) - drag_term
            normal_star = normal_part + DIFFUSION * (curvature(normal_part) - wave_square * normal_part) + lift_profile[:, None, None] * control_hat[:, None]
            span_star = span_part + DIFFUSION * (curvature(span_part) - wave_square * span_part)
            divergence = pair_rotate(stream_star, stream_factor) + centred(normal_star) + pair_rotate(span_star, span_wave)
            pressure = solve(divergence)
            fields = jnp.stack([stream_star - pair_rotate(pressure, stream_factor), normal_star - centred(pressure), span_star - pair_rotate(pressure, span_wave)])
        return fields
    final_state, pullback = jax.vjp(evolve, wall_control)
    control_gradient = pullback(final_state)[0]
    return (final_state, control_gradient)
```

```python
import functools
import math

import jax
import jax.numpy as jnp
import ml_dtypes
import numpy as np
from jax import lax
from jax.experimental import pallas as pl
from jax.experimental.pallas import tpu as pltpu
from jax.sharding import PartitionSpec as P

STEPS = 2


DIFFUSION = 0.04
HIGHEST = lax.Precision.HIGHEST
MESH = pl.DeviceIdType.MESH
LANES = 128
QUAD = 4
HALVES = 2
SUBLANES = 8


def split_host(table):
    high = table.astype(ml_dtypes.bfloat16)
    low = (table - high.astype(np.float64)).astype(ml_dtypes.bfloat16)
    return np.stack([high, low])


def host_tables(stream_len, span_count, count):
    z = np.arange(span_count)
    angle = 2.0 * math.pi / span_count * (np.outer(z, z) % span_count)
    span = np.concatenate([np.cos(angle), np.sin(angle)], axis=1) / math.sqrt(span_count)
    n = np.arange(stream_len)
    k = np.arange(stream_len // 2)
    angle = 2.0 * math.pi / stream_len * (np.outer(k, n) % stream_len)
    stream = np.stack([np.cos(angle), -np.sin(angle)]) / math.sqrt(stream_len)
    stream = stream.reshape(2, count, HALVES, -1, stream_len).transpose(2, 1, 0, 3, 4).reshape(-1, stream_len)
    return split_host(span), split_host(stream.T.copy()), split_host(stream)


def split_pair(x):
    high = x.astype(jnp.bfloat16)
    low = (x - high.astype(jnp.float32)).astype(jnp.bfloat16)
    return high, low


def mxu(a, b):
    return jnp.dot(a, b, preferred_element_type=jnp.float32)


def span_product(x, table):
    high, low = split_pair(x)
    both = mxu(jnp.concatenate([high, low], axis=0), table[0])
    return both[: x.shape[0]] + (both[x.shape[0] :] + mxu(high, table[1]))


def stream_product(table, pair, store):
    tile = table.shape[1] // HALVES

    def body(index, carry):
        rows = pl.ds(pl.multiple_of(index * tile, tile), tile)
        wide = mxu(table[0, rows, :], pair[...])
        narrow = mxu(table[1, rows, :], pair[:, :LANES])
        store(index, rows, wide[:, :LANES] + (wide[:, LANES:] + narrow))
        return carry

    lax.fori_loop(0, HALVES, body, 0)


def fill_pair(pair, rows, x):
    high, low = split_pair(x)
    pair[rows, :LANES] = high
    pair[rows, LANES:] = low


def swap_groups(tiles):
    a0, a1, a2, a3 = tiles
    group = lax.broadcasted_iota(jnp.int32, a0.shape, a0.ndim - 1) // (LANES // QUAD)
    lower = group < 2
    even = group % 2 == 0
    axis = a0.ndim - 1
    half = LANES // 2
    step = LANES // QUAD

    def far(x, y):
        return (
            jnp.where(lower, x, pltpu.roll(y, half, axis)),
            jnp.where(lower, pltpu.roll(x, half, axis), y),
        )

    def near(x, y):
        return (
            jnp.where(even, x, pltpu.roll(y, step, axis)),
            jnp.where(even, pltpu.roll(x, LANES - step, axis), y),
        )

    b0, b2 = far(a0, a2)
    b1, b3 = far(a1, a3)
    return near(b0, b1) + near(b2, b3)


def peer_at(count, me, step):
    peer = 0
    unit = 1
    while unit < count:
        peer = peer + lax.rem(lax.div(me, unit) + lax.div(step, unit), 2) * unit
        unit *= 2
    return peer


class Exchange:
    def __init__(self, count, me, outbox, inbox, send_sem, recv_sem):
        self.count, self.me = count, me
        self.outbox, self.inbox, self.send_sem, self.recv_sem = outbox, inbox, send_sem, recv_sem

    def copy(self, peer, slot):
        return pltpu.make_async_remote_copy(
            src_ref=self.outbox.at[peer],
            dst_ref=self.inbox.at[slot],
            send_sem=self.send_sem.at[peer],
            recv_sem=self.recv_sem.at[slot],
            device_id={"xz": peer},
            device_id_type=MESH,
        )

    def loop(self, action):
        def body(step, carry):
            action(peer_at(self.count, self.me, step))
            return carry

        lax.fori_loop(1, self.count, body, 0)

    def start(self):
        self.loop(lambda peer: self.copy(peer, self.me).start())
        self.inbox[self.me] = self.outbox[self.me]

    def arrive(self):
        self.loop(lambda peer: self.copy(peer, peer).wait_recv())

    def finish(self):
        self.loop(lambda peer: self.copy(peer, peer).wait_send())


def fused_kernel(count, stream_len, *refs):
    refs = list(refs)
    lift, state_far, drag_far, control_far, schur_far, span_far, inverse_far, forward_far = refs[:8]
    final_far, gradient = refs[8:10]
    (
        fields, final, base, source, drag_term, direct, schur, drag_raw, drag, control, control_hat,
        span, inverse, forward, out1, in1, out2, in2, pair, damped, outc, inc, outp, inp,
        halo_u, halo_v, halo_w, halo_final, rim, corner, wall, share, share_in,
        load_sem, send_sem, recv_sem, plane_send, plane_recv, near_send, near_recv, store_sem,
    ) = refs[10:]
    me = lax.axis_index("xz")
    slab = lax.axis_index("gy")
    rows, width, span_count = fields.shape[2], fields.shape[4], fields.shape[5]
    modes = HALVES * width
    chunks = rows // QUAD
    groups = count // QUAD
    tiles_q = span_count // LANES
    tiles = width // SUBLANES * tiles_q
    block = rows * width
    edge = (rows - 1) * (1 - slab)
    has_above = slab.astype(jnp.float32)
    has_below = 1.0 - has_above

    loads = {
        "stream": (state_far.at[0], fields.at[0]),
        "span": (span_far, span),
        "forward": (forward_far, forward),
        "control": (control_far, control),
        "inverse": (inverse_far, inverse),
        "drag": (drag_far, drag_raw),
        "rest": (state_far.at[1:3], fields.at[1:3]),
        "schur": (schur_far, schur),
    }
    loads = {
        name: pltpu.make_async_copy(far, near, load_sem.at[i]) for i, (name, (far, near)) in enumerate(loads.items())
    }
    for load in loads.values():
        load.start()

    barrier = pltpu.get_barrier_semaphore()

    def greet(step, carry):
        pl.semaphore_signal(barrier, inc=1, device_id={"xz": peer_at(count, me, step)}, device_id_type=MESH)
        return carry

    lax.fori_loop(1, count, greet, 0)
    pl.semaphore_signal(barrier, inc=1, device_id={"gy": 1 - slab}, device_id_type=MESH)
    pl.semaphore_wait(barrier, count)

    def first(h, g):
        return Exchange(count, me, out1.at[h, g], in1.at[h, g], send_sem.at[0, h, g], recv_sem.at[0, h, g])

    def second(h, g):
        return Exchange(count, me, out2.at[h, g], in2.at[h, g], send_sem.at[1, h, g], recv_sem.at[1, h, g])

    def across(src, dst, index):
        return pltpu.make_async_remote_copy(
            src_ref=src,
            dst_ref=dst,
            send_sem=near_send.at[index],
            recv_sem=near_recv.at[index],
            device_id={"gy": 1 - slab},
            device_id_type=MESH,
        )

    def halo_copies(h):
        pair_row = (rows - 2) * (1 - slab)
        return [
            across(fields.at[0, :, edge, h], halo_u.at[h], h),
            across(fields.at[1, :, pl.ds(pair_row, 2), h], halo_v.at[h], HALVES + h),
            across(fields.at[2, :, edge, h], halo_w.at[h], 2 * HALVES + h),
        ]

    def rim_copy(h):
        return across(direct.at[:, edge], rim.at[h], 3 * HALVES + h)

    def final_copy(h):
        return across(final.at[1, :, edge, h], halo_final.at[h], 4 * HALVES + h)

    corner_copy = across(schur.at[edge, edge], corner, 5 * HALVES)
    share_copy = across(share.at[1 - slab], share_in, 5 * HALVES + 1)

    def store_copy(h):
        return pltpu.make_async_copy(final.at[:, :, :, h], final_far.at[:, :, :, h], store_sem.at[h])

    def every_half(action):
        def body(h, carry):
            action(h)
            return carry

        lax.fori_loop(0, HALVES, body, 0)

    def every_tile(action):
        def body(t, carry):
            sub = lax.div(t, tiles_q)
            column = lax.rem(t, tiles_q)
            at = (
                pl.ds(pl.multiple_of(sub * SUBLANES, SUBLANES), SUBLANES),
                pl.ds(pl.multiple_of(column * LANES, LANES), LANES),
            )
            action(at, sub, column)
            return carry

        lax.fori_loop(0, tiles, body, 0)

    def mode_ids(h, sub):
        return me * modes + h * width + sub * SUBLANES + lax.broadcasted_iota(jnp.int32, (SUBLANES, LANES), 0)

    def waves(h, sub, column):
        kx = 2.0 * math.pi / stream_len * mode_ids(h, sub).astype(jnp.float32)
        q = column * LANES + lax.broadcasted_iota(jnp.int32, (SUBLANES, LANES), 1)
        signed = jnp.where(q < span_count // 2, q, q - span_count)
        kz = jnp.where(q == span_count // 2, 0.0, 2.0 * math.pi / span_count * signed.astype(jnp.float32))
        return kx, kz

    def mode_weight(h, sub):
        return jnp.where(mode_ids(h, sub) == 0, 1.0, 2.0)

    def send_first(h, weighted):
        x = fields[0, :, :, h]
        if weighted:
            ids = me * modes + h * width + lax.broadcasted_iota(jnp.int32, x.shape, 2)
            x = x * jnp.where(ids == 0, 1.0, 2.0)
        w = span_product(x.reshape(2 * block, span_count), span)
        halfway = (
            w[:block, :span_count] - w[block:, span_count:],
            w[:block, span_count:] + w[block:, :span_count],
        )
        for g in range(chunks):
            for part in range(2):
                for group in range(groups):
                    lanes = slice(LANES * group, LANES * (group + 1))
                    start = width * QUAD * g
                    parts = [halfway[part][start + width * y : start + width * (y + 1), lanes] for y in range(QUAD)]
                    for i, tile in enumerate(swap_groups(parts)):
                        out1[h, g, QUAD * group + i, part] = tile
            first(h, g).start()

    def physical(again):
        for g in range(chunks):
            for h in range(HALVES):
                first(h, g).arrive()
                fill_pair(pair, slice(h * block * 4, (h + 1) * block * 4), in1[h, g].reshape(-1, LANES))
                if again:
                    second(h, g).finish()

            def damp(index, at, y):
                fill_pair(damped, at, y * drag[g, at, :])

            stream_product(inverse, pair, damp)

            def keep(index, at, y):
                out2[index, g] = y.reshape(count, 2, width, LANES)

            stream_product(forward, damped, keep)
            second(0, g).start()
        for h in range(1, HALVES):
            for g in range(chunks):
                second(h, g).start()

    def collect(h):
        for g in range(chunks):
            second(h, g).arrive()
            first(h, g).finish()
        parts = []
        for part in range(2):
            for g in range(chunks):
                columns = []
                for group in range(groups):
                    pieces = [in2[h, g, QUAD * group + i, part] for i in range(QUAD)]
                    columns.append(jnp.concatenate(swap_groups(pieces), axis=0))
                parts.append(jnp.concatenate(columns, axis=1))
        w = span_product(jnp.concatenate(parts, axis=0), span)
        shape = (rows, width, span_count)
        drag_term[0] = (w[:block, :span_count] + w[block:, span_count:]).reshape(shape)
        drag_term[1] = (w[block:, :span_count] - w[:block, span_count:]).reshape(shape)

    def spread(h, forced):
        def body(at, sub, column):
            kx, kz = waves(h, sub, column)
            keep = 1.0 - DIFFUSION * (2.0 + kx * kx + kz * kz)

            def smooth(lines):
                return [
                    lines[i] * keep + DIFFUSION * (lines[i - 1] + lines[i + 1]) for i in range(1, len(lines) - 1)
                ]

            def wide(halo, c, p):
                line = halo[(h, p) + at]
                return [has_above * line] + [fields[(c, p, y, h) + at] for y in range(rows)] + [has_below * line]

            stream = [smooth(wide(halo_u, 0, p)) for p in range(2)]
            across_span = [smooth(wide(halo_w, 2, p)) for p in range(2)]
            for p in range(2):
                outer, inner = halo_v[(h, p, 0) + at], halo_v[(h, p, 1) + at]
                lines = [has_above * outer, has_above * inner]
                lines += [fields[(1, p, y, h) + at] for y in range(rows)]
                lines += [has_below * outer, has_below * inner]
                lines = smooth(lines)
                if forced:
                    hat = control_hat[(p, h) + at]
                    places = [slab * (rows - 1)] + [slab * rows + y for y in range(rows)] + [rows]
                    lines = [line + lift[place] * hat for line, place in zip(lines, places)]
                lines = [has_above * lines[0]] + lines[1:-1] + [has_below * lines[-1]]
                sign = -1.0 if p == 0 else 1.0
                for y in range(rows):
                    base[(0, p, y, h) + at] = stream[p][y]
                    base[(1, p, y, h) + at] = lines[y + 1]
                    base[(2, p, y, h) + at] = across_span[p][y]
                    turned = sign * (kx * stream[1 - p][y] + kz * across_span[1 - p][y])
                    source[(p, y, h) + at] = turned + 0.5 * (lines[y + 2] - lines[y])

        every_tile(body)

    def apply_blocks(h, at, values, transposed):
        for i in range(rows):
            totals = [None, None]
            for j in range(rows):
                place = (j, i) if transposed else (i, j)
                factor = schur[place + (h,) + at]
                for p in range(2):
                    term = factor * values[p][j]
                    totals[p] = term if totals[p] is None else totals[p] + term
            for p in range(2):
                direct[(p, i) + at] = totals[p]

    def begin_solve(h, transposed):
        def body(at, sub, column):
            kx, _ = waves(h, sub, column)
            if transposed:
                kx = kx * mode_weight(h, sub)
            values = [
                [source[(0, y, h) + at] + kx * drag_term[(1, y) + at] for y in range(rows)],
                [source[(1, y, h) + at] - kx * drag_term[(0, y) + at] for y in range(rows)],
            ]
            apply_blocks(h, at, values, transposed)

        every_tile(body)

    def begin_adjoint(h):
        def body(at, sub, column):
            kx, kz = waves(h, sub, column)
            values = []
            for p in range(2):
                line = halo_final[(h, p) + at]
                lines = [has_above * line] + [final[(1, p, y, h) + at] for y in range(rows)] + [has_below * line]
                sign = -1.0 if p == 0 else 1.0
                values.append(
                    [
                        sign * (kx * final[(0, 1 - p, y, h) + at] + kz * final[(2, 1 - p, y, h) + at])
                        + 0.5 * (lines[y + 2] - lines[y])
                        for y in range(rows)
                    ]
                )
            apply_blocks(h, at, values, True)

        every_tile(body)

    def swap_rims(h):
        copy = rim_copy(h)
        copy.start()
        copy.wait_recv()
        copy.wait_send()

    def pressure_at(h, at, transposed):
        turn = corner[(h,) + at]
        reach = [schur[((edge, i) if transposed else (i, edge)) + (h,) + at] for i in range(rows)]
        own = schur[(edge, edge, h) + at]
        wide = []
        for p in range(2):
            near = direct[(p, edge) + at]
            far = rim[(h, p) + at]
            outer = far + has_below * (turn * near)
            above = has_above * (far + turn * (near + own * far))
            inside = [direct[(p, y) + at] + reach[y] * outer for y in range(rows)]
            wide.append([above] + inside + [has_below * outer])
        return wide

    def finish_solve(h, target):
        def body(at, sub, column):
            kx, kz = waves(h, sub, column)
            wide = pressure_at(h, at, False)
            for p in range(2):
                sign = 1.0 if p == 0 else -1.0
                for y in range(rows):
                    turned = sign * wide[1 - p][y + 1]
                    slope = 0.5 * (wide[p][y + 2] - wide[p][y])
                    target[(0, p, y, h) + at] = base[(0, p, y, h) + at] - drag_term[(p, y) + at] + kx * turned
                    target[(1, p, y, h) + at] = base[(1, p, y, h) + at] - slope
                    target[(2, p, y, h) + at] = base[(2, p, y, h) + at] + kz * turned

        every_tile(body)

    def finish_adjoint(h, last):
        def body(at, sub, column):
            kx, kz = waves(h, sub, column)
            wide = pressure_at(h, at, True)
            for p in range(2):
                sign = 1.0 if p == 0 else -1.0
                total = None
                for y in range(rows):
                    slope = 0.5 * (wide[p][y + 2] - wide[p][y])
                    if last:
                        normal = base[(1, p, y, h) + at] - slope
                    else:
                        turned = sign * wide[1 - p][y + 1]
                        normal = final[(1, p, y, h) + at] - slope
                        fields[(0, p, y, h) + at] = final[(0, p, y, h) + at] + kx * turned
                        fields[(1, p, y, h) + at] = normal
                        fields[(2, p, y, h) + at] = final[(2, p, y, h) + at] + kz * turned
                    term = lift[slab * rows + y] * normal
                    total = term if total is None else total + term
                wall[(p, h) + at] = wall[(p, h) + at] + total if last else total

        every_tile(body)

    def start_halos(h):
        for copy in halo_copies(h):
            copy.start()

    def spread_all(forced):
        def body(h):
            for copy in halo_copies(h):
                copy.wait_recv()
                copy.wait_send()
            spread(h, forced)

        every_half(body)

    loads["stream"].wait()
    loads["span"].wait()
    every_half(lambda h: send_first(h, True))

    loads["control"].wait()
    loads["forward"].wait()
    third = Exchange(count, me, outc, inc, plane_send.at[0], plane_recv.at[0])
    lines = control[...]
    blank = jnp.zeros((LANES - lines.shape[0], stream_len), jnp.float32)
    fill_pair(pair, slice(None), jnp.concatenate([lines, blank], axis=0).T)

    def pack(index, at, y):
        y = y.reshape(count, 2, HALVES, SUBLANES, LANES)
        damped_rows = y[:, :, 0] + pltpu.roll(y[:, :, 1], LANES // QUAD, 3)

        @pl.when(index == 0)
        def _():
            outc[...] = damped_rows

        @pl.when(index != 0)
        def _():
            outc[...] = outc[...] + pltpu.roll(damped_rows, LANES // 2, 3)

    stream_product(forward, pair, pack)
    third.start()
    loads["rest"].wait()
    every_half(start_halos)
    loads["schur"].wait()
    corner_copy.start()
    loads["drag"].wait()
    for g in range(chunks):
        drag[g] = drag_raw[QUAD * g : QUAD * (g + 1)].reshape(LANES, stream_len).T
    loads["inverse"].wait()
    physical(False)
    third.arrive()
    parts = []
    for part in range(2):
        columns = []
        for group in range(groups):
            pieces = [inc[QUAD * group + i, part] for i in range(QUAD)]
            columns.append(jnp.concatenate(swap_groups(pieces), axis=0))
        parts.append(jnp.concatenate(columns, axis=1))
    w = span_product(jnp.concatenate(parts, axis=0), span)
    shape = (HALVES, width, span_count)
    control_hat[0] = (w[:modes, :span_count] + w[modes:, span_count:]).reshape(shape)
    control_hat[1] = (w[modes:, :span_count] - w[:modes, span_count:]).reshape(shape)
    corner_copy.wait_recv()
    corner_copy.wait_send()
    spread_all(True)

    def step(h):
        collect(h)
        begin_solve(h, False)
        swap_rims(h)
        finish_solve(h, fields)
        send_first(h, True)
        start_halos(h)

    every_half(step)
    physical(True)
    spread_all(True)

    def turn(h):
        collect(h)
        begin_solve(h, False)
        swap_rims(h)
        finish_solve(h, final)
        copy = final_copy(h)
        copy.start()
        store_copy(h).start()
        copy.wait_recv()
        copy.wait_send()
        begin_adjoint(h)
        swap_rims(h)
        finish_adjoint(h, False)
        send_first(h, False)
        start_halos(h)

    every_half(turn)
    physical(True)
    spread_all(False)

    def close(h):
        collect(h)
        begin_solve(h, True)
        swap_rims(h)
        finish_adjoint(h, True)

    every_half(close)
    fourth = Exchange(count, me, outp, inp, plane_send.at[1], plane_recv.at[1])
    w = span_product(wall[...].reshape(2 * modes, span_count), span)
    halfway = (
        w[:modes, :span_count] - w[modes:, span_count:],
        w[:modes, span_count:] + w[modes:, :span_count],
    )
    for part in range(2):
        for group in range(groups):
            lanes = slice(LANES * group, LANES * (group + 1))
            pieces = [halfway[part][SUBLANES * j : SUBLANES * (j + 1), lanes] for j in range(QUAD)]
            for i, tile in enumerate(swap_groups(pieces)):
                outp[QUAD * group + i, part] = tile
    fourth.start()
    fourth.arrive()
    x = inp[...]
    turned = [x] + [pltpu.roll(x, LANES - j * LANES // QUAD, 3) for j in range(1, QUAD)]
    for h in range(HALVES):
        both = jnp.concatenate(turned[2 * h : 2 * h + 2], axis=2)
        fill_pair(pair, slice(h * block * 4, (h + 1) * block * 4), both.reshape(-1, LANES))

    def keep_share(index, at, y):
        share[index] = y.T[: share.shape[1]]

    stream_product(inverse, pair, keep_share)
    share_copy.start()
    third.finish()
    fourth.finish()
    for h in range(HALVES):
        store_copy(h).wait()
        for g in range(chunks):
            second(h, g).finish()
    share_copy.wait_recv()
    share_copy.wait_send()
    gradient[...] = share[slab] + share_in[...]


VMEM = pl.BlockSpec(memory_space=pltpu.VMEM)
SMEM = pl.BlockSpec(memory_space=pltpu.SMEM)
FAR = pl.BlockSpec(memory_space=pl.ANY)


def fused_call(count, initial_state, drag_rate, wall_control, lift_profile, schur_inverse):
    _, _, rows, modes, span_count = initial_state.shape
    stream_len = drag_rate.shape[2]
    narrow = wall_control.shape[0]
    width = modes // HALVES
    chunks = rows // QUAD
    span, inverse, forward = host_tables(stream_len, span_count, count)
    state = initial_state.reshape(3, 2, rows, HALVES, width, span_count)
    schur = schur_inverse.reshape(rows, rows, HALVES, width, span_count)
    plane = (2, rows, HALVES, width, span_count)
    half_plane = (2, rows, width, span_count)
    box = (HALVES, chunks, count, 2, width, LANES)
    thin = (count, 2, SUBLANES, LANES)
    line = (HALVES, 2, width, span_count)

    def buffer(*shape):
        return pltpu.VMEM(shape, jnp.float32)

    pairs = pltpu.VMEM((stream_len, 2 * LANES), jnp.bfloat16)
    scratch = [buffer(*state.shape)] * 3 + [buffer(*plane), buffer(*half_plane), buffer(*half_plane)]
    scratch += [buffer(*schur.shape), buffer(*drag_rate.shape), buffer(chunks, stream_len, LANES)]
    scratch += [buffer(*wall_control.shape), buffer(*line)]
    scratch += [pltpu.VMEM(table.shape, jnp.bfloat16) for table in (span, inverse, forward)]
    scratch += [buffer(*box)] * 4 + [pairs] * 2 + [buffer(*thin)] * 4
    scratch += [buffer(*line), buffer(HALVES, 2, 2, width, span_count), buffer(*line), buffer(*line), buffer(*line)]
    scratch += [buffer(HALVES, width, span_count), buffer(*line)]
    scratch += [buffer(2, narrow, stream_len // 2), buffer(narrow, stream_len // 2)]
    scratch += [pltpu.SemaphoreType.DMA((8,))]
    scratch += [pltpu.SemaphoreType.DMA((2, HALVES, chunks, count))] * 2
    scratch += [pltpu.SemaphoreType.DMA((2, count))] * 2
    scratch += [pltpu.SemaphoreType.DMA((5 * HALVES + 2,))] * 2
    scratch += [pltpu.SemaphoreType.DMA((HALVES,))]
    final, gradient = pl.pallas_call(
        functools.partial(fused_kernel, count, stream_len),
        out_shape=[
            jax.ShapeDtypeStruct(state.shape, jnp.float32),
            jax.ShapeDtypeStruct((narrow, stream_len // 2), jnp.float32),
        ],
        in_specs=[SMEM] + [FAR] * 7,
        out_specs=[FAR, VMEM],
        scratch_shapes=scratch,
        compiler_params=pltpu.CompilerParams(
            collective_id=0, has_side_effects=True, vmem_limit_bytes=63 * 1024 * 1024
        ),
        cost_estimate=pl.CostEstimate(flops=60_000_000_000, bytes_accessed=32_000_000, transcendentals=0),
    )(lift_profile, state, drag_rate, wall_control, schur, span, inverse, forward)
    return final.reshape(initial_state.shape), gradient


def phase_pair(outer_size, inner_size, period, factor):
    outer_ids = jnp.arange(outer_size, dtype=jnp.int32)[:, None]
    inner_ids = jnp.arange(inner_size, dtype=jnp.int32)[None, :]
    angle = 2.0 * math.pi / period * (outer_ids * inner_ids % period).astype(jnp.float32)
    return (jnp.cos(angle) * factor, jnp.sin(angle) * factor)


def plain_transforms(count, rows, modes, span_count, stream_len):
    half_len = stream_len // 2
    cos_x, sin_x = phase_pair(stream_len, half_len, stream_len, 1.0 / math.sqrt(stream_len))
    cos_z, sin_z = phase_pair(span_count, span_count, span_count, 1.0 / math.sqrt(span_count))

    def to_spectral(physical):
        real_half = jnp.einsum("yzn,nk->yzk", physical, cos_x, precision=HIGHEST)
        imag_half = -jnp.einsum("yzn,nk->yzk", physical, sin_x, precision=HIGHEST)
        halfway = jnp.stack([real_half, imag_half])
        pieces = lax.all_to_all(halfway, "xz", split_axis=3, concat_axis=2, tiled=True)
        with_cos = jnp.einsum("cyzk,zq->cykq", pieces, cos_z, precision=HIGHEST)
        with_sin = jnp.einsum("cyzk,zq->cykq", pieces, sin_z, precision=HIGHEST)
        return jnp.stack([with_cos[0] + with_sin[1], with_cos[1] - with_sin[0]])

    def to_physical(spectral):
        with_cos = jnp.einsum("cykq,qz->cykz", spectral, cos_z, precision=HIGHEST)
        with_sin = jnp.einsum("cykq,qz->cykz", spectral, sin_z, precision=HIGHEST)
        halfway = jnp.stack([with_cos[0] - with_sin[1], with_sin[0] + with_cos[1]])
        pieces = lax.all_to_all(halfway, "xz", split_axis=3, concat_axis=2, tiled=True)
        return jnp.einsum("ykz,nk->yzn", pieces[0], cos_x, precision=HIGHEST) - jnp.einsum(
            "ykz,nk->yzn", pieces[1], sin_x, precision=HIGHEST
        )

    def begin(drag_rate, control):
        def drag_map(s):
            return to_spectral(drag_rate * to_physical(s))

        return drag_map, (lambda s: (drag_map(s), to_spectral(control[None])[:, 0]))

    def plane(spectral):
        return to_physical(spectral[:, None])[0]

    return begin, plane


def rotate(spectrum, factor):
    return jnp.stack([-factor * spectrum[1], factor * spectrum[0]])


def per_device(initial_state, drag_rate, wall_control, lift_profile, schur_inverse):
    row_count = initial_state.shape[2]
    mode_count = initial_state.shape[3]
    span_count = initial_state.shape[4]
    stream_len = drag_rate.shape[2]
    last_row = row_count - 1
    slab_count = lax.axis_size("gy")
    slab_index = lax.axis_index("gy")
    pencil_count = lax.axis_size("xz")
    pencil_index = lax.axis_index("xz")
    mode_ids = pencil_index * mode_count + jnp.arange(mode_count)
    stream_factor = (2.0 * math.pi / stream_len * mode_ids.astype(jnp.float32))[:, None]
    mode_weight = jnp.where(mode_ids == 0, 1.0, 2.0).astype(jnp.float32)[:, None]
    span_ids = jnp.arange(span_count)
    signed = jnp.where(span_ids < span_count // 2, span_ids, span_ids - span_count)
    span_wave = jnp.where(
        span_ids == span_count // 2, 0.0, 2.0 * math.pi / span_count * signed.astype(jnp.float32)
    )
    wave_square = stream_factor**2 + span_wave[None, :] ** 2
    fits = (
        slab_count == 2
        and QUAD * mode_count == LANES
        and QUAD * drag_rate.shape[1] == LANES
        and row_count == SUBLANES
        and pencil_count * mode_count * 2 == stream_len
        and pencil_count * drag_rate.shape[1] == span_count
        and pencil_count & (pencil_count - 1) == 0
        and pencil_count % QUAD == 0
    )
    if fits:
        return fused_call(pencil_count, initial_state, drag_rate, wall_control, lift_profile, schur_inverse)
    begin, plane = plain_transforms(pencil_count, row_count, mode_count, span_count, stream_len)
    drag_map, first_map = begin(drag_rate, wall_control)

    ends = slab_count - 1

    def from_above(tail):
        return lax.ppermute(tail, "gy", [(i, i + 1) for i in range(ends)])

    def from_below(head):
        return lax.ppermute(head, "gy", [(i + 1, i) for i in range(ends)])

    def every_slab(values):
        if slab_count == 2:
            other = lax.ppermute(values, "gy", [(0, 1), (1, 0)])
            return [jnp.where(slab_index == 0, values, other), jnp.where(slab_index == 0, other, values)]
        gathered = lax.all_gather(values, "gy", axis=0)
        return [gathered[i] for i in range(slab_count)]

    has_above = (slab_index > 0).astype(jnp.float32)
    has_below = (slab_index < slab_count - 1).astype(jnp.float32)
    corners = every_slab(
        jnp.stack(
            [
                schur_inverse[0, 0],
                schur_inverse[0, last_row],
                schur_inverse[last_row, 0],
                schur_inverse[last_row, last_row],
            ]
        )
    )
    corner_above = jnp.zeros_like(corners[0][3])
    for member in range(slab_count - 1):
        corner_above = jnp.where(slab_index == member + 1, corners[member][3], corner_above)

    padded_lift = jnp.pad(lift_profile, 1)
    lift_near = lax.dynamic_slice_in_dim(padded_lift, slab_index * row_count, row_count + 2)
    lift_own = lift_near[1 : row_count + 1]

    def halos(fields):
        tail = jnp.concatenate([fields[0, :, last_row:], fields[1, :, last_row - 1 :], fields[2, :, last_row:]], axis=1)
        head = jnp.concatenate([fields[0, :, :1], fields[1, :, :2], fields[2, :, :1]], axis=1)
        return from_above(tail), from_below(head)

    def smooth(wide):
        own = wide[:, 1:-1]
        laplace = wide[:, 2:] - 2.0 * own + wide[:, :-2]
        return own + DIFFUSION * (laplace - wave_square * own)

    def slope(wide):
        return 0.5 * (wide[:, 2:] - wide[:, :-2])

    def advance(fields, drag_term, control_hat):
        above, below = halos(fields)
        stream_star = smooth(jnp.concatenate([above[:, 0:1], fields[0], below[:, 0:1]], axis=1)) - drag_term
        span_star = smooth(jnp.concatenate([above[:, 3:4], fields[2], below[:, 3:4]], axis=1))
        normal_wide = smooth(jnp.concatenate([above[:, 1:3], fields[1], below[:, 1:3]], axis=1))
        if control_hat is not None:
            normal_wide = normal_wide + lift_near[:, None, None] * control_hat[:, None]
        normal_wide = jnp.concatenate(
            [has_above * normal_wide[:, :1], normal_wide[:, 1:-1], has_below * normal_wide[:, -1:]], axis=1
        )
        return stream_star, normal_wide[:, 1:-1], span_star, slope(normal_wide)

    def apply_blocks(values, transposed):
        summed = None
        for column in range(row_count):
            factor = schur_inverse[column] if transposed else schur_inverse[:, column]
            term = factor[None] * values[:, column : column + 1]
            summed = term if summed is None else summed + term
        return summed

    def solve(source, transposed):
        if transposed:
            first_column, last_column = schur_inverse[0], schur_inverse[last_row]
            ratio_at, turn_at = 1, 2
        else:
            first_column, last_column = schur_inverse[:, 0], schur_inverse[:, last_row]
            ratio_at, turn_at = 2, 1
        direct = apply_blocks(source, transposed)
        rims = every_slab(jnp.stack([direct[:, 0], direct[:, last_row]]))
        running = jnp.zeros_like(direct[:, 0])
        before = []
        for member in range(slab_count):
            before.append(running)
            running = rims[member][1] + corners[member][ratio_at][None] * running
        running = jnp.zeros_like(direct[:, 0])
        behind = [running] * slab_count
        for member in reversed(range(slab_count)):
            behind[member] = running
            top = rims[member][0] + corners[member][0][None] * before[member]
            running = top + corners[member][turn_at][None] * running
        entering, leaving = before[0], behind[0]
        for member in range(1, slab_count):
            entering = jnp.where(slab_index == member, before[member], entering)
            leaving = jnp.where(slab_index == member, behind[member], leaving)
        pressure = direct + first_column[None] * entering[:, None] + last_column[None] * leaving[:, None]
        row_above = entering + corner_above[None] * pressure[:, 0]
        return jnp.concatenate([row_above[:, None], pressure, leaving[:, None]], axis=1)

    def project(stream_part, normal_part, span_part, normal_slope, transposed):
        divergence = rotate(stream_part, stream_factor) + normal_slope + rotate(span_part, span_wave)
        wide = solve(divergence, transposed)
        pressure = wide[:, 1:-1]
        return jnp.stack(
            [
                stream_part - rotate(pressure, stream_factor),
                normal_part - slope(wide),
                span_part - rotate(pressure, span_wave),
            ]
        )

    fields = initial_state
    control_hat = None
    for section_index in range(STEPS):
        weighted = mode_weight * fields[0]
        if section_index == 0:
            drag_term, control_hat = first_map(weighted)
        else:
            drag_term = drag_map(weighted)
        fields = project(*advance(fields, drag_term, control_hat), False)
    final = fields
    normal_slope = slope(
        jnp.concatenate([from_above(final[1, :, last_row:]), final[1], from_below(final[1, :, :1])], axis=1)
    )
    parts = (final[0], final[1], final[2], normal_slope)
    wall_sum = jnp.zeros_like(control_hat)
    for section_index in range(STEPS):
        projected = project(*parts, True)
        wall_sum = wall_sum + jnp.sum(lift_own[:, None, None] * projected[1], axis=1)
        if section_index + 1 < STEPS:
            parts = advance(projected, mode_weight * drag_map(projected[0]), None)
    share = plane(wall_sum)
    if slab_count == 2:
        half = stream_len // 2
        first, second = share[:, :half], share[:, half:]
        upper = slab_index == 0
        other = lax.ppermute(jnp.where(upper, second, first), "gy", [(0, 1), (1, 0)])
        control_gradient = jnp.where(upper, first, second) + other
    else:
        control_gradient = lax.psum_scatter(share, "gy", scatter_dimension=1, tiled=True)
    return (final, control_gradient)


def solution(mesh):
    return jax.shard_map(
        per_device,
        mesh=mesh,
        in_specs=(
            P(None, None, "gy", "xz", None),
            P("gy", "xz", None),
            P("xz", None),
            P(),
            P("gy", None, "xz", None),
        ),
        out_specs=(P(None, None, "gy", "xz", None), P("xz", "gy")),
        check_vma=False,
    )
```

```python
import functools
import math

import jax
import jax.numpy as jnp
import ml_dtypes
import numpy as np
from jax import lax
from jax.experimental import pallas as pl
from jax.experimental.pallas import tpu as pltpu
from jax.sharding import PartitionSpec as P

STEPS = 2


DIFFUSION = 0.04
HIGHEST = lax.Precision.HIGHEST
MESH = pl.DeviceIdType.MESH
LANES = 128
QUAD = 4
HALVES = 2
SUBLANES = 8
FAR_FIRST = (3, 2, 0, 1)
VMEM_BYTES = 67_043_328


def split_host(table):
    high = table.astype(ml_dtypes.bfloat16)
    low = (table - high.astype(np.float64)).astype(ml_dtypes.bfloat16)
    return np.stack([high, low])


def host_tables(stream_len, span_count, count):
    z = np.arange(span_count)
    angle = 2.0 * math.pi / span_count * (np.outer(z, z) % span_count)
    span = np.concatenate([np.cos(angle), np.sin(angle)], axis=1) / math.sqrt(span_count)
    n = np.arange(stream_len)
    k = np.arange(stream_len // 2)
    angle = 2.0 * math.pi / stream_len * (np.outer(k, n) % stream_len)
    stream = np.stack([np.cos(angle), -np.sin(angle)]) / math.sqrt(stream_len)
    stream = stream.reshape(2, count, HALVES, -1, stream_len).transpose(2, 1, 0, 3, 4).reshape(-1, stream_len)
    return split_host(span), split_host(stream.T.copy()), split_host(stream)


def split_pair(x):
    high = x.astype(jnp.bfloat16)
    low = (x - high.astype(jnp.float32)).astype(jnp.bfloat16)
    return high, low


def mxu(a, b):
    return jnp.dot(a, b, preferred_element_type=jnp.float32)


def span_product(x, table):
    high, low = split_pair(x)
    both = mxu(jnp.concatenate([high, low], axis=0), table[0])
    return both[: x.shape[0]] + (both[x.shape[0] :] + mxu(high, table[1]))


def stream_product(table, pair, store):
    tile = table.shape[1] // HALVES

    def body(index, carry):
        rows = pl.ds(pl.multiple_of(index * tile, tile), tile)
        wide = mxu(table[0, rows, :], pair[...])
        narrow = mxu(table[1, rows, :], pair[:, :LANES])
        store(index, rows, wide[:, :LANES] + (wide[:, LANES:] + narrow))
        return carry

    lax.fori_loop(0, HALVES, body, 0)


def fill_pair(pair, rows, x):
    high, low = split_pair(x)
    pair[rows, :LANES] = high
    pair[rows, LANES:] = low


def swap_groups(tiles):
    a0, a1, a2, a3 = tiles
    group = lax.broadcasted_iota(jnp.int32, a0.shape, a0.ndim - 1) // (LANES // QUAD)
    lower = group < 2
    even = group % 2 == 0
    axis = a0.ndim - 1
    half = LANES // 2
    step = LANES // QUAD

    def far(x, y):
        return (
            jnp.where(lower, x, pltpu.roll(y, half, axis)),
            jnp.where(lower, pltpu.roll(x, half, axis), y),
        )

    def near(x, y):
        return (
            jnp.where(even, x, pltpu.roll(y, step, axis)),
            jnp.where(even, pltpu.roll(x, LANES - step, axis), y),
        )

    b0, b2 = far(a0, a2)
    b1, b3 = far(a1, a3)
    return near(b0, b1) + near(b2, b3)


def peer_at(count, me, step):
    peer = 0
    unit = 1
    while unit < count:
        peer = peer + lax.rem(lax.div(me, unit) + lax.div(step, unit), 2) * unit
        unit *= 2
    return peer


class Exchange:
    def __init__(self, peers, me, outbox, inbox, send_sem, recv_sem):
        self.peers, self.me = peers, me
        self.outbox, self.inbox, self.send_sem, self.recv_sem = outbox, inbox, send_sem, recv_sem

    def copy(self, src, dst, peer):
        return pltpu.make_async_remote_copy(
            src_ref=self.outbox.at[src],
            dst_ref=self.inbox.at[dst],
            send_sem=self.send_sem,
            recv_sem=self.recv_sem,
            device_id={"xz": peer},
            device_id_type=MESH,
        )

    def every(self):
        others = pl.ds(0, len(self.peers))
        return self.copy(others, others, self.peers[0])

    def start(self):
        for peer in self.peers:
            self.copy(peer, self.me, peer).start()
        self.inbox[self.me] = self.outbox[self.me]

    def arrive(self):
        self.every().wait_recv()

    def finish(self):
        self.every().wait_send()


def fused_kernel(count, stream_len, *refs):
    refs = list(refs)
    lift, state_far, drag_far, control_far, schur_far, span_far, inverse_far, forward_far = refs[:8]
    final, gradient = refs[8:10]
    (
        fields, base, source, drag_term, direct, schur, drag_raw, drag, control, control_hat,
        span, inverse, forward, out1, in1, out2, in2, pair, damped, outc, inc, outp, inp,
        halo_u, halo_v, halo_w, beyond, rim, corner, wall, reply, reply_rim, inp_other, share,
        load_sem, send_sem, recv_sem, plane_send, plane_recv, near_send, near_recv,
    ) = refs[10:]
    me = lax.axis_index("xz")
    slab = lax.axis_index("gy")
    rows, width, span_count = fields.shape[2], fields.shape[4], fields.shape[5]
    modes = HALVES * width
    chunks = rows // QUAD
    groups = count // QUAD
    tiles_q = span_count // LANES
    tiles = width // SUBLANES * tiles_q
    block = rows * width
    edge = (rows - 1) * (1 - slab)
    edge_pair = (rows - 2) * (1 - slab)
    edge_at = 1 - slab
    has_above = slab.astype(jnp.float32)
    has_below = 1.0 - has_above
    reach_up = [has_above * lift[slab * (rows - 1)]] + [lift[slab * rows + y] for y in range(rows - 1)]
    reach_down = [lift[slab * rows + y] for y in range(1, rows)] + [has_below * lift[rows]]
    lift_slope = [0.5 * (down - up) for up, down in zip(reach_up, reach_down)]

    loads = {
        "stream": (state_far.at[0], fields.at[0]),
        "span": (span_far, span),
        "forward": (forward_far, forward),
        "control": (control_far, control),
        "inverse": (inverse_far, inverse),
        "drag": (drag_far, drag_raw),
        "rest": (state_far.at[1:3], fields.at[1:3]),
        "schur": (schur_far, schur),
    }
    loads = {
        name: pltpu.make_async_copy(far, near, load_sem.at[i]) for i, (name, (far, near)) in enumerate(loads.items())
    }
    loads["stream"].start()
    loads["span"].start()
    order = sorted(range(1, count), key=lambda step: (FAR_FIRST[step * QUAD // count], -step))
    peers = [peer_at(count, me, step) for step in order]
    barrier = pltpu.get_barrier_semaphore()
    for peer in peers:
        pl.semaphore_signal(barrier, inc=1, device_id={"xz": peer}, device_id_type=MESH)
    pl.semaphore_signal(barrier, inc=1, device_id={"gy": 1 - slab}, device_id_type=MESH)

    def first(h, g):
        return Exchange(peers, me, out1.at[h, g], in1.at[h, g], send_sem.at[0, h, g], recv_sem.at[0, h, g])

    def second(h, g):
        return Exchange(peers, me, out2.at[h, g], in2.at[h, g], send_sem.at[1, h, g], recv_sem.at[1, h, g])

    def third(h):
        return Exchange(peers, me, outc.at[h], inc.at[h], plane_send.at[0, h], plane_recv.at[0, h])

    def fourth(h):
        return Exchange(peers, me, outp.at[h], inp.at[h], plane_send.at[1, h], plane_recv.at[1, h])

    def across(src, dst, index):
        return pltpu.make_async_remote_copy(
            src_ref=src,
            dst_ref=dst,
            send_sem=near_send.at[index],
            recv_sem=near_recv.at[index],
            device_id={"gy": 1 - slab},
            device_id_type=MESH,
        )

    def halo_copies(h):
        return [
            across(fields.at[0, :, edge, h], halo_u.at[h], h),
            across(fields.at[1, :, pl.ds(edge_pair, 2), h], halo_v.at[h], HALVES + h),
            across(fields.at[2, :, edge, h], halo_w.at[h], 2 * HALVES + h),
        ]

    def rim_copy(h, turn):
        return across(direct.at[:, pl.ds(edge_pair, 2)], rim.at[turn, h], (3 + turn) * HALVES + h)

    def plane_copy(h):
        return across(inp.at[h], inp_other.at[h], 5 * HALVES + h)

    corner_copy = across(schur.at[pl.ds(edge_pair, 2), edge], corner, 6 * HALVES)
    reply_copy = across(reply.at[edge], reply_rim, 6 * HALVES + 1)

    def every_half(action):
        def body(h, carry):
            action(h)
            return carry

        lax.fori_loop(0, HALVES, body, 0)

    def every_tile(action):
        def body(t, carry):
            sub = lax.div(t, tiles_q)
            column = lax.rem(t, tiles_q)
            at = (
                pl.ds(pl.multiple_of(sub * SUBLANES, SUBLANES), SUBLANES),
                pl.ds(pl.multiple_of(column * LANES, LANES), LANES),
            )
            action(at, sub, column)
            return carry

        lax.fori_loop(0, tiles, body, 0)

    def mode_ids(h, sub):
        return me * modes + h * width + sub * SUBLANES + lax.broadcasted_iota(jnp.int32, (SUBLANES, LANES), 0)

    def waves(h, sub, column):
        kx = 2.0 * math.pi / stream_len * mode_ids(h, sub).astype(jnp.float32)
        q = column * LANES + lax.broadcasted_iota(jnp.int32, (SUBLANES, LANES), 1)
        signed = jnp.where(q < span_count // 2, q, q - span_count)
        kz = jnp.where(q == span_count // 2, 0.0, 2.0 * math.pi / span_count * signed.astype(jnp.float32))
        return kx, kz

    def mode_weight(h, sub):
        return jnp.where(mode_ids(h, sub) == 0, 1.0, 2.0)

    def pack_first(h, weighted):
        x = fields[0, :, :, h]
        if weighted:
            ids = me * modes + h * width + lax.broadcasted_iota(jnp.int32, x.shape, 2)
            x = x * jnp.where(ids == 0, 1.0, 2.0)
        w = span_product(x.reshape(2 * block, span_count), span)
        halfway = (
            w[:block, :span_count] - w[block:, span_count:],
            w[:block, span_count:] + w[block:, :span_count],
        )
        for g in range(chunks):
            for part in range(2):
                for group in range(groups):
                    lanes = slice(LANES * group, LANES * (group + 1))
                    start = width * QUAD * g
                    parts = [halfway[part][start + width * y : start + width * (y + 1), lanes] for y in range(QUAD)]
                    for i, tile in enumerate(swap_groups(parts)):
                        out1[h, g, QUAD * group + i, part] = tile

    def send_first(h, weighted):
        pack_first(h, weighted)
        first(h, 0).start()

        @pl.when(h == 0)
        def _():
            for g in range(1, chunks):
                first(0, g).start()

    def physical(again):
        first(1, 0).finish()
        for g in range(1, chunks):
            first(1, g).start()
        for g in range(chunks):
            for h in range(HALVES):
                first(h, g).arrive()
                fill_pair(pair, slice(h * block * 4, (h + 1) * block * 4), in1[h, g].reshape(-1, LANES))
            if again:
                second(1, g).finish()

            def damp(index, at, y):
                fill_pair(damped, at, y * drag[g, at, :])

            stream_product(inverse, pair, damp)

            def keep(index, at, y):
                out2[index, g] = y.reshape(count, 2, width, LANES)

            stream_product(forward, damped, keep)
            second(0, g).start()
        for g in range(chunks):
            first(0, g).finish()
            if g:
                first(1, g).finish()

    def send_rest():
        second(0, 0).finish()
        second(1, 0).start()
        for g in range(1, chunks):
            second(0, g).finish()

    def collect(h):
        for g in range(chunks):
            second(h, g).arrive()

        @pl.when(h == 0)
        def _():
            for g in range(1, chunks):
                second(1, g).start()

        parts = []
        for part in range(2):
            for g in range(chunks):
                columns = []
                for group in range(groups):
                    pieces = [in2[h, g, QUAD * group + i, part] for i in range(QUAD)]
                    columns.append(jnp.concatenate(swap_groups(pieces), axis=0))
                parts.append(jnp.concatenate(columns, axis=1))
        w = span_product(jnp.concatenate(parts, axis=0), span)
        shape = (rows, width, span_count)
        drag_term[0] = (w[:block, :span_count] + w[block:, span_count:]).reshape(shape)
        drag_term[1] = (w[block:, :span_count] - w[:block, span_count:]).reshape(shape)

    def spread(h, forced):
        def body(at, sub, column):
            kx, kz = waves(h, sub, column)
            keep = 1.0 - DIFFUSION * (2.0 + kx * kx + kz * kz)

            def smooth(lines):
                return [
                    lines[i] * keep + DIFFUSION * (lines[i - 1] + lines[i + 1]) for i in range(1, len(lines) - 1)
                ]

            def wide(halo, c, p):
                line = halo[(h, p) + at]
                return [has_above * line] + [fields[(c, p, y, h) + at] for y in range(rows)] + [has_below * line]

            stream = [smooth(wide(halo_u, 0, p)) for p in range(2)]
            across_span = [smooth(wide(halo_w, 2, p)) for p in range(2)]
            for p in range(2):
                outer, inner = halo_v[(h, p, 0) + at], halo_v[(h, p, 1) + at]
                lines = [has_above * outer, has_above * inner]
                lines += [fields[(1, p, y, h) + at] for y in range(rows)]
                lines += [has_below * outer, has_below * inner]
                lines = smooth(lines)
                if forced:
                    hat = control_hat[(p, h) + at]
                    places = [slab * (rows - 1)] + [slab * rows + y for y in range(rows)] + [rows]
                    lines = [line + lift[place] * hat for line, place in zip(lines, places)]
                lines = [has_above * lines[0]] + lines[1:-1] + [has_below * lines[-1]]
                beyond[(h, p) + at] = lines[0] + lines[-1]
                if not forced:
                    total = wall[(p, h) + at]
                    for y in range(rows):
                        total = total + lift[slab * rows + y] * lines[y + 1]
                    wall[(p, h) + at] = total
                sign = -1.0 if p == 0 else 1.0
                for y in range(rows):
                    base[(0, p, y, h) + at] = stream[p][y]
                    base[(1, p, y, h) + at] = lines[y + 1]
                    base[(2, p, y, h) + at] = across_span[p][y]
                    turned = sign * (kx * stream[1 - p][y] + kz * across_span[1 - p][y])
                    source[(p, y, h) + at] = turned + 0.5 * (lines[y + 2] - lines[y])

        every_tile(body)

    def apply_blocks(h, at, values, transposed):
        for i in range(rows):
            totals = [None, None]
            for j in range(rows):
                place = (j, i) if transposed else (i, j)
                factor = schur[place + (h,) + at]
                for p in range(2):
                    term = factor * values[p][j]
                    totals[p] = term if totals[p] is None else totals[p] + term
            for p in range(2):
                direct[(p, i) + at] = totals[p]

    def begin_solve(h):
        def body(at, sub, column):
            kx, _ = waves(h, sub, column)
            values = [
                [source[(0, y, h) + at] + kx * drag_term[(1, y) + at] for y in range(rows)],
                [source[(1, y, h) + at] - kx * drag_term[(0, y) + at] for y in range(rows)],
            ]
            apply_blocks(h, at, values, False)

        every_tile(body)

    def swap_rims(h, turn):
        copy = rim_copy(h, turn)
        copy.start()
        copy.wait_recv()
        copy.wait_send()

    def pressure_at(h, at, transposed):
        turn = corner[(1 - edge_at, h) + at]
        reach = [schur[((edge, i) if transposed else (i, edge)) + (h,) + at] for i in range(rows)]
        own = schur[(edge, edge, h) + at]
        wide = []
        for p in range(2):
            far = rim[(int(transposed), h, p, 1 - edge_at) + at]
            known = direct[(p, edge) + at] + has_above * (own * far)
            next_row = far + turn * known
            outer = has_above * far + has_below * next_row
            inside = [direct[(p, y) + at] + reach[y] * outer for y in range(rows)]
            wide.append([has_above * next_row] + inside + [has_below * next_row])
        return wide

    def finish_solve(h, target):
        def body(at, sub, column):
            kx, kz = waves(h, sub, column)
            wide = pressure_at(h, at, False)
            for p in range(2):
                sign = 1.0 if p == 0 else -1.0
                for y in range(rows):
                    turned = sign * wide[1 - p][y + 1]
                    slope = 0.5 * (wide[p][y + 2] - wide[p][y])
                    target[(0, p, y, h) + at] = base[(0, p, y, h) + at] - drag_term[(p, y) + at] + kx * turned
                    target[(1, p, y, h) + at] = base[(1, p, y, h) + at] - slope
                    target[(2, p, y, h) + at] = base[(2, p, y, h) + at] + kz * turned

        every_tile(body)

    def finish_and_reverse(h):
        def body(at, sub, column):
            kx, kz = waves(h, sub, column)
            wide = pressure_at(h, at, False)
            turn = corner[(edge_at, h) + at]
            own = schur[(edge, edge, h) + at]
            stream, normal, across_span = [], [], []
            for p in range(2):
                sign = 1.0 if p == 0 else -1.0
                far = rim[(0, h, p, 1 - edge_at) + at]
                known = direct[(p, edge) + at] + has_above * (own * far)
                inner_row = rim[(0, h, p, edge_at) + at] + turn * known
                edge_row = has_below * wide[p][rows] + has_above * wide[p][1]
                outside = beyond[(h, p) + at] + 0.5 * (has_above - has_below) * (inner_row - edge_row)
                lines = [has_above * outside]
                for y in range(rows):
                    turned = sign * wide[1 - p][y + 1]
                    slope = 0.5 * (wide[p][y + 2] - wide[p][y])
                    stream.append(base[(0, p, y, h) + at] - drag_term[(p, y) + at] + kx * turned)
                    lines.append(base[(1, p, y, h) + at] - slope)
                    across_span.append(base[(2, p, y, h) + at] + kz * turned)
                    final[(0, p, y, h) + at] = stream[-1]
                    final[(1, p, y, h) + at] = lines[-1]
                    final[(2, p, y, h) + at] = across_span[-1]
                normal.append(lines + [has_below * outside])
            values = []
            for p in range(2):
                sign = -1.0 if p == 0 else 1.0
                values.append(
                    [
                        sign * (kx * stream[rows * (1 - p) + y] + kz * across_span[rows * (1 - p) + y])
                        + 0.5 * (normal[p][y + 2] - normal[p][y])
                        for y in range(rows)
                    ]
                )
            for p in range(2):
                for y in range(rows):
                    source[(p, y, h) + at] = values[p][y]

        every_tile(body)

        def reverse(at, sub, column):
            values = [[source[(p, y, h) + at] for y in range(rows)] for p in range(2)]
            apply_blocks(h, at, values, True)

        every_tile(reverse)

    def finish_adjoint(h):
        def body(at, sub, column):
            kx, kz = waves(h, sub, column)
            wide = pressure_at(h, at, True)
            for p in range(2):
                sign = 1.0 if p == 0 else -1.0
                total = None
                for y in range(rows):
                    turned = sign * wide[1 - p][y + 1]
                    normal = final[(1, p, y, h) + at] - 0.5 * (wide[p][y + 2] - wide[p][y])
                    fields[(0, p, y, h) + at] = final[(0, p, y, h) + at] + kx * turned
                    fields[(1, p, y, h) + at] = normal
                    fields[(2, p, y, h) + at] = final[(2, p, y, h) + at] + kz * turned
                    term = lift[slab * rows + y] * normal
                    total = term if total is None else total + term
                wall[(p, h) + at] = total

        every_tile(body)

    def start_reply():
        def body(h):
            def tile(at, sub, column):
                for i in range(rows):
                    total = None
                    for j in range(rows):
                        term = schur[(i, j, h) + at] * lift_slope[j]
                        total = term if total is None else total + term
                    reply[(i, h) + at] = total

            every_tile(tile)

        every_half(body)
        reply_copy.start()

    def finish_reply():
        reply_copy.wait_recv()
        reply_copy.wait_send()

        def body(h):
            def tile(at, sub, column):
                far = reply_rim[(h,) + at]
                outer = far + has_below * (corner[(1 - edge_at, h) + at] * reply[(edge, h) + at])
                for y in range(rows):
                    reply[(y, h) + at] = reply[(y, h) + at] + schur[(y, edge, h) + at] * outer

            every_tile(tile)

        every_half(body)

    def close_wall(h):
        def body(at, sub, column):
            kx, _ = waves(h, sub, column)
            kx = kx * mode_weight(h, sub)
            for p in range(2):
                sign = 1.0 if p == 0 else -1.0
                total = wall[(p, h) + at]
                for y in range(rows):
                    value = source[(p, y, h) + at] + sign * (kx * drag_term[(1 - p, y) + at])
                    total = total + reply[(y, h) + at] * value
                wall[(p, h) + at] = total

        every_tile(body)

    def start_halos(h):
        for copy in halo_copies(h):
            copy.start()

    def spread_all(forced):
        def body(h):
            for copy in halo_copies(h):
                copy.wait_recv()
                copy.wait_send()
            spread(h, forced)

        every_half(body)

    loads["stream"].wait()
    loads["span"].wait()
    for name in ("control", "forward", "rest", "schur", "drag", "inverse"):
        loads[name].start()
    pack_first(0, True)
    pl.semaphore_wait(barrier, count)
    for g in range(chunks):
        first(0, g).start()
    pack_first(1, True)
    first(1, 0).start()

    loads["control"].wait()
    loads["forward"].wait()
    lines = control[...]
    blank = jnp.zeros((LANES - lines.shape[0], stream_len), jnp.float32)
    fill_pair(pair, slice(None), jnp.concatenate([lines, blank], axis=0).T)

    def pack(index, at, y):
        y = y.reshape(count, QUAD, SUBLANES, LANES)
        moved = y[:, 0]
        for j in range(1, QUAD):
            moved = moved + pltpu.roll(y[:, j], j * LANES // QUAD, 2)
        outc[index] = moved

    stream_product(forward, pair, pack)
    every_half(lambda h: third(h).start())
    loads["rest"].wait()
    every_half(start_halos)
    loads["schur"].wait()
    corner_copy.start()
    start_reply()
    loads["drag"].wait()
    for g in range(chunks):
        drag[g] = drag_raw[QUAD * g : QUAD * (g + 1)].reshape(LANES, stream_len).T
    loads["inverse"].wait()
    physical(False)

    def control_half(h):
        third(h).arrive()
        columns = []
        for group in range(groups):
            pieces = [inc[h, QUAD * group + i] for i in range(QUAD)]
            columns.append(jnp.concatenate(swap_groups(pieces), axis=0))
        w = span_product(jnp.concatenate(columns, axis=1), span)
        control_hat[0, h] = w[:width, :span_count] + w[width:, span_count:]
        control_hat[1, h] = w[width:, :span_count] - w[:width, span_count:]
        third(h).finish()

    every_half(control_half)
    corner_copy.wait_recv()
    corner_copy.wait_send()
    finish_reply()
    spread_all(True)
    send_rest()

    def step(h):
        collect(h)
        begin_solve(h)
        swap_rims(h, 0)
        finish_solve(h, fields)
        send_first(h, True)
        start_halos(h)

    every_half(step)
    physical(True)
    spread_all(True)
    send_rest()

    def turn(h):
        collect(h)
        begin_solve(h)
        swap_rims(h, 0)
        finish_and_reverse(h)
        swap_rims(h, 1)
        finish_adjoint(h)
        send_first(h, False)
        start_halos(h)

    every_half(turn)
    physical(True)
    spread_all(False)
    send_rest()

    def close(h):
        collect(h)
        close_wall(h)
        w = span_product(wall[:, h].reshape(2 * width, span_count), span)
        halfway = (
            w[:width, :span_count] - w[width:, span_count:],
            w[:width, span_count:] + w[width:, :span_count],
        )
        for group in range(groups):
            lanes = slice(LANES * group, LANES * (group + 1))
            pieces = [half[at : at + SUBLANES, lanes] for half in halfway for at in range(0, width, SUBLANES)]
            for i, tile in enumerate(swap_groups(pieces)):
                outp[h, QUAD * group + i] = tile
        fourth(h).start()

    def open_plane(h):
        fourth(h).arrive()
        copy = plane_copy(h)
        copy.start()
        copy.wait_recv()
        copy.wait_send()
        x = inp[h] + inp_other[h]
        turned = [x] + [pltpu.roll(x, LANES - j * LANES // QUAD, 2) for j in range(1, QUAD)]
        x = jnp.concatenate(turned, axis=1).reshape(-1, LANES)
        terms = slice(h * x.shape[0], (h + 1) * x.shape[0])
        fill_pair(pair, terms, x)
        places = pl.ds(pl.multiple_of(slab * gradient.shape[1], LANES), gradient.shape[1])
        y = mxu(inverse[0, places, terms], pair[terms, :])
        return y[:, :LANES] + (y[:, LANES:] + mxu(inverse[1, places, terms], pair[terms, :LANES]))

    every_half(close)
    share[...] = open_plane(0)
    gradient[...] = (share[...] + open_plane(1)).T[: gradient.shape[0]]
    for h in range(HALVES):
        fourth(h).finish()
    for g in range(chunks):
        second(1, g).finish()


VMEM = pl.BlockSpec(memory_space=pltpu.VMEM)
SMEM = pl.BlockSpec(memory_space=pltpu.SMEM)
FAR = pl.BlockSpec(memory_space=pltpu.HBM)


def fused_call(count, initial_state, drag_rate, wall_control, lift_profile, schur_inverse):
    _, _, rows, modes, span_count = initial_state.shape
    stream_len = drag_rate.shape[2]
    narrow = wall_control.shape[0]
    width = modes // HALVES
    chunks = rows // QUAD
    span, inverse, forward = host_tables(stream_len, span_count, count)
    state = initial_state.reshape(3, 2, rows, HALVES, width, span_count)
    schur = schur_inverse.reshape(rows, rows, HALVES, width, span_count)
    plane = (2, rows, HALVES, width, span_count)
    half_plane = (2, rows, width, span_count)
    box = (HALVES, chunks, count, 2, width, LANES)
    thin = (HALVES, count, SUBLANES, LANES)
    line = (HALVES, 2, width, span_count)

    kept = 4 * (math.prod(state.shape) + narrow * stream_len // 2 + 16 * SUBLANES * LANES)

    def buffer(*shape):
        return pltpu.VMEM(shape, jnp.float32)

    pairs = pltpu.VMEM((stream_len, 2 * LANES), jnp.bfloat16)
    scratch = [buffer(*state.shape)] * 2 + [buffer(*plane), buffer(*half_plane), buffer(*half_plane)]
    scratch += [buffer(*schur.shape), buffer(*drag_rate.shape), buffer(chunks, stream_len, LANES)]
    scratch += [buffer(*wall_control.shape), buffer(*line)]
    scratch += [pltpu.VMEM(table.shape, jnp.bfloat16) for table in (span, inverse, forward)]
    scratch += [buffer(*box)] * 4 + [pairs] * 2 + [buffer(*thin)] * 4
    scratch += [buffer(*line), buffer(HALVES, 2, 2, width, span_count), buffer(*line), buffer(*line)]
    scratch += [buffer(2, HALVES, 2, 2, width, span_count), buffer(2, HALVES, width, span_count), buffer(*line)]
    scratch += [buffer(rows, HALVES, width, span_count), buffer(HALVES, width, span_count)]
    scratch += [buffer(*thin), buffer(stream_len // 2, LANES)]
    scratch += [pltpu.SemaphoreType.DMA((8,))]
    scratch += [pltpu.SemaphoreType.DMA((2, HALVES, chunks))] * 2
    scratch += [pltpu.SemaphoreType.DMA((2, HALVES))] * 2
    scratch += [pltpu.SemaphoreType.DMA((6 * HALVES + 2,))] * 2
    final, gradient = pl.pallas_call(
        functools.partial(fused_kernel, count, stream_len),
        out_shape=[
            pltpu.VMEM(state.shape, jnp.float32),
            pltpu.VMEM((narrow, stream_len // 2), jnp.float32),
        ],
        in_specs=[SMEM] + [FAR] * 7,
        out_specs=[VMEM, VMEM],
        scratch_shapes=scratch,
        compiler_params=pltpu.CompilerParams(
            collective_id=0, has_side_effects=True, vmem_limit_bytes=VMEM_BYTES - kept
        ),
        cost_estimate=pl.CostEstimate(flops=60_000_000_000, bytes_accessed=32_000_000, transcendentals=0),
    )(lift_profile, state, drag_rate, wall_control, schur, span, inverse, forward)
    return final.reshape(initial_state.shape), gradient


def phase_pair(outer_size, inner_size, period, factor):
    outer_ids = jnp.arange(outer_size, dtype=jnp.int32)[:, None]
    inner_ids = jnp.arange(inner_size, dtype=jnp.int32)[None, :]
    angle = 2.0 * math.pi / period * (outer_ids * inner_ids % period).astype(jnp.float32)
    return (jnp.cos(angle) * factor, jnp.sin(angle) * factor)


def plain_transforms(count, rows, modes, span_count, stream_len):
    half_len = stream_len // 2
    cos_x, sin_x = phase_pair(stream_len, half_len, stream_len, 1.0 / math.sqrt(stream_len))
    cos_z, sin_z = phase_pair(span_count, span_count, span_count, 1.0 / math.sqrt(span_count))

    def to_spectral(physical):
        real_half = jnp.einsum("yzn,nk->yzk", physical, cos_x, precision=HIGHEST)
        imag_half = -jnp.einsum("yzn,nk->yzk", physical, sin_x, precision=HIGHEST)
        halfway = jnp.stack([real_half, imag_half])
        pieces = lax.all_to_all(halfway, "xz", split_axis=3, concat_axis=2, tiled=True)
        with_cos = jnp.einsum("cyzk,zq->cykq", pieces, cos_z, precision=HIGHEST)
        with_sin = jnp.einsum("cyzk,zq->cykq", pieces, sin_z, precision=HIGHEST)
        return jnp.stack([with_cos[0] + with_sin[1], with_cos[1] - with_sin[0]])

    def to_physical(spectral):
        with_cos = jnp.einsum("cykq,qz->cykz", spectral, cos_z, precision=HIGHEST)
        with_sin = jnp.einsum("cykq,qz->cykz", spectral, sin_z, precision=HIGHEST)
        halfway = jnp.stack([with_cos[0] - with_sin[1], with_sin[0] + with_cos[1]])
        pieces = lax.all_to_all(halfway, "xz", split_axis=3, concat_axis=2, tiled=True)
        return jnp.einsum("ykz,nk->yzn", pieces[0], cos_x, precision=HIGHEST) - jnp.einsum(
            "ykz,nk->yzn", pieces[1], sin_x, precision=HIGHEST
        )

    def begin(drag_rate, control):
        def drag_map(s):
            return to_spectral(drag_rate * to_physical(s))

        return drag_map, (lambda s: (drag_map(s), to_spectral(control[None])[:, 0]))

    def plane(spectral):
        return to_physical(spectral[:, None])[0]

    return begin, plane


def rotate(spectrum, factor):
    return jnp.stack([-factor * spectrum[1], factor * spectrum[0]])


def per_device(initial_state, drag_rate, wall_control, lift_profile, schur_inverse):
    row_count = initial_state.shape[2]
    mode_count = initial_state.shape[3]
    span_count = initial_state.shape[4]
    stream_len = drag_rate.shape[2]
    last_row = row_count - 1
    slab_count = lax.axis_size("gy")
    slab_index = lax.axis_index("gy")
    pencil_count = lax.axis_size("xz")
    pencil_index = lax.axis_index("xz")
    mode_ids = pencil_index * mode_count + jnp.arange(mode_count)
    stream_factor = (2.0 * math.pi / stream_len * mode_ids.astype(jnp.float32))[:, None]
    mode_weight = jnp.where(mode_ids == 0, 1.0, 2.0).astype(jnp.float32)[:, None]
    span_ids = jnp.arange(span_count)
    signed = jnp.where(span_ids < span_count // 2, span_ids, span_ids - span_count)
    span_wave = jnp.where(
        span_ids == span_count // 2, 0.0, 2.0 * math.pi / span_count * signed.astype(jnp.float32)
    )
    wave_square = stream_factor**2 + span_wave[None, :] ** 2
    fits = (
        slab_count == 2
        and QUAD * mode_count == LANES
        and QUAD * drag_rate.shape[1] == LANES
        and row_count == SUBLANES
        and pencil_count * mode_count * 2 == stream_len
        and pencil_count * drag_rate.shape[1] == span_count
        and pencil_count & (pencil_count - 1) == 0
        and pencil_count % QUAD == 0
    )
    if fits:
        return fused_call(pencil_count, initial_state, drag_rate, wall_control, lift_profile, schur_inverse)
    begin, plane = plain_transforms(pencil_count, row_count, mode_count, span_count, stream_len)
    drag_map, first_map = begin(drag_rate, wall_control)

    ends = slab_count - 1

    def from_above(tail):
        return lax.ppermute(tail, "gy", [(i, i + 1) for i in range(ends)])

    def from_below(head):
        return lax.ppermute(head, "gy", [(i + 1, i) for i in range(ends)])

    def every_slab(values):
        if slab_count == 2:
            other = lax.ppermute(values, "gy", [(0, 1), (1, 0)])
            return [jnp.where(slab_index == 0, values, other), jnp.where(slab_index == 0, other, values)]
        gathered = lax.all_gather(values, "gy", axis=0)
        return [gathered[i] for i in range(slab_count)]

    has_above = (slab_index > 0).astype(jnp.float32)
    has_below = (slab_index < slab_count - 1).astype(jnp.float32)
    corners = every_slab(
        jnp.stack(
            [
                schur_inverse[0, 0],
                schur_inverse[0, last_row],
                schur_inverse[last_row, 0],
                schur_inverse[last_row, last_row],
            ]
        )
    )
    corner_above = jnp.zeros_like(corners[0][3])
    for member in range(slab_count - 1):
        corner_above = jnp.where(slab_index == member + 1, corners[member][3], corner_above)

    padded_lift = jnp.pad(lift_profile, 1)
    lift_near = lax.dynamic_slice_in_dim(padded_lift, slab_index * row_count, row_count + 2)
    lift_own = lift_near[1 : row_count + 1]

    def halos(fields):
        tail = jnp.concatenate([fields[0, :, last_row:], fields[1, :, last_row - 1 :], fields[2, :, last_row:]], axis=1)
        head = jnp.concatenate([fields[0, :, :1], fields[1, :, :2], fields[2, :, :1]], axis=1)
        return from_above(tail), from_below(head)

    def smooth(wide):
        own = wide[:, 1:-1]
        laplace = wide[:, 2:] - 2.0 * own + wide[:, :-2]
        return own + DIFFUSION * (laplace - wave_square * own)

    def slope(wide):
        return 0.5 * (wide[:, 2:] - wide[:, :-2])

    def advance(fields, drag_term, control_hat):
        above, below = halos(fields)
        stream_star = smooth(jnp.concatenate([above[:, 0:1], fields[0], below[:, 0:1]], axis=1)) - drag_term
        span_star = smooth(jnp.concatenate([above[:, 3:4], fields[2], below[:, 3:4]], axis=1))
        normal_wide = smooth(jnp.concatenate([above[:, 1:3], fields[1], below[:, 1:3]], axis=1))
        if control_hat is not None:
            normal_wide = normal_wide + lift_near[:, None, None] * control_hat[:, None]
        normal_wide = jnp.concatenate(
            [has_above * normal_wide[:, :1], normal_wide[:, 1:-1], has_below * normal_wide[:, -1:]], axis=1
        )
        return stream_star, normal_wide[:, 1:-1], span_star, slope(normal_wide)

    def apply_blocks(values, transposed):
        summed = None
        for column in range(row_count):
            factor = schur_inverse[column] if transposed else schur_inverse[:, column]
            term = factor[None] * values[:, column : column + 1]
            summed = term if summed is None else summed + term
        return summed

    def solve(source, transposed):
        if transposed:
            first_column, last_column = schur_inverse[0], schur_inverse[last_row]
            ratio_at, turn_at = 1, 2
        else:
            first_column, last_column = schur_inverse[:, 0], schur_inverse[:, last_row]
            ratio_at, turn_at = 2, 1
        direct = apply_blocks(source, transposed)
        rims = every_slab(jnp.stack([direct[:, 0], direct[:, last_row]]))
        running = jnp.zeros_like(direct[:, 0])
        before = []
        for member in range(slab_count):
            before.append(running)
            running = rims[member][1] + corners[member][ratio_at][None] * running
        running = jnp.zeros_like(direct[:, 0])
        behind = [running] * slab_count
        for member in reversed(range(slab_count)):
            behind[member] = running
            top = rims[member][0] + corners[member][0][None] * before[member]
            running = top + corners[member][turn_at][None] * running
        entering, leaving = before[0], behind[0]
        for member in range(1, slab_count):
            entering = jnp.where(slab_index == member, before[member], entering)
            leaving = jnp.where(slab_index == member, behind[member], leaving)
        pressure = direct + first_column[None] * entering[:, None] + last_column[None] * leaving[:, None]
        row_above = entering + corner_above[None] * pressure[:, 0]
        return jnp.concatenate([row_above[:, None], pressure, leaving[:, None]], axis=1)

    def project(stream_part, normal_part, span_part, normal_slope, transposed):
        divergence = rotate(stream_part, stream_factor) + normal_slope + rotate(span_part, span_wave)
        wide = solve(divergence, transposed)
        pressure = wide[:, 1:-1]
        return jnp.stack(
            [
                stream_part - rotate(pressure, stream_factor),
                normal_part - slope(wide),
                span_part - rotate(pressure, span_wave),
            ]
        )

    fields = initial_state
    control_hat = None
    for section_index in range(STEPS):
        weighted = mode_weight * fields[0]
        if section_index == 0:
            drag_term, control_hat = first_map(weighted)
        else:
            drag_term = drag_map(weighted)
        fields = project(*advance(fields, drag_term, control_hat), False)
    final = fields
    normal_slope = slope(
        jnp.concatenate([from_above(final[1, :, last_row:]), final[1], from_below(final[1, :, :1])], axis=1)
    )
    parts = (final[0], final[1], final[2], normal_slope)
    wall_sum = jnp.zeros_like(control_hat)
    for section_index in range(STEPS):
        projected = project(*parts, True)
        wall_sum = wall_sum + jnp.sum(lift_own[:, None, None] * projected[1], axis=1)
        if section_index + 1 < STEPS:
            parts = advance(projected, mode_weight * drag_map(projected[0]), None)
    share = plane(wall_sum)
    if slab_count == 2:
        half = stream_len // 2
        first, second = share[:, :half], share[:, half:]
        upper = slab_index == 0
        other = lax.ppermute(jnp.where(upper, second, first), "gy", [(0, 1), (1, 0)])
        control_gradient = jnp.where(upper, first, second) + other
    else:
        control_gradient = lax.psum_scatter(share, "gy", scatter_dimension=1, tiled=True)
    return (final, control_gradient)


def solution(mesh):
    return jax.shard_map(
        per_device,
        mesh=mesh,
        in_specs=(
            P(None, None, "gy", "xz", None),
            P("gy", "xz", None),
            P("xz", None),
            P(),
            P("gy", None, "xz", None),
        ),
        out_specs=(P(None, None, "gy", "xz", None), P("xz", "gy")),
        check_vma=False,
    )
```

```python
import functools
import math

import jax
import jax.numpy as jnp
import ml_dtypes
import numpy as np
from jax import lax
from jax.experimental import pallas as pl
from jax.experimental.pallas import tpu as pltpu
from jax.sharding import PartitionSpec as P

STEPS = 2


DIFFUSION = 0.04
HIGHEST = lax.Precision.HIGHEST
MESH = pl.DeviceIdType.MESH
LANES = 128
QUAD = 4
HALVES = 2
SUBLANES = 8
FAR_FIRST = (3, 2, 0, 1)
VMEM_BYTES = 67_043_328


def split_host(table):
    high = table.astype(ml_dtypes.bfloat16)
    low = (table - high.astype(np.float64)).astype(ml_dtypes.bfloat16)
    return np.stack([high, low])


def host_tables(stream_len, span_count, count):
    z = np.arange(span_count)
    angle = 2.0 * math.pi / span_count * (np.outer(z, z) % span_count)
    span = np.concatenate([np.cos(angle), np.sin(angle)], axis=1) / math.sqrt(span_count)
    n = np.arange(stream_len)
    k = np.arange(stream_len // 2)
    angle = 2.0 * math.pi / stream_len * (np.outer(k, n) % stream_len)
    stream = np.stack([np.cos(angle), -np.sin(angle)]) / math.sqrt(stream_len)
    stream = stream.reshape(2, count, HALVES, -1, stream_len).transpose(2, 1, 0, 3, 4).reshape(-1, stream_len)
    return split_host(span), split_host(stream.T.copy()), split_host(stream)


def split_pair(x):
    high = x.astype(jnp.bfloat16)
    low = (x - high.astype(jnp.float32)).astype(jnp.bfloat16)
    return high, low


def mxu(a, b):
    return jnp.dot(a, b, preferred_element_type=jnp.float32)


def span_product(x, table):
    high, low = split_pair(x)
    both = mxu(jnp.concatenate([high, low], axis=0), table[0])
    return both[: x.shape[0]] + (both[x.shape[0] :] + mxu(high, table[1]))


def split_product(table, rows, terms, pair):
    wide = mxu(table[0, rows, terms], pair[...])
    narrow = mxu(table[1, rows, terms], pair[:, :LANES])
    return wide[:, :LANES] + (wide[:, LANES:] + narrow)


def fill_pair(pair, rows, x):
    high, low = split_pair(x)
    pair[rows, :LANES] = high
    pair[rows, LANES:] = low


def swap_groups(tiles):
    a0, a1, a2, a3 = tiles
    group = lax.broadcasted_iota(jnp.int32, a0.shape, a0.ndim - 1) // (LANES // QUAD)
    lower = group < 2
    even = group % 2 == 0
    axis = a0.ndim - 1
    half = LANES // 2
    step = LANES // QUAD

    def far(x, y):
        return (
            jnp.where(lower, x, pltpu.roll(y, half, axis)),
            jnp.where(lower, pltpu.roll(x, half, axis), y),
        )

    def near(x, y):
        return (
            jnp.where(even, x, pltpu.roll(y, step, axis)),
            jnp.where(even, pltpu.roll(x, LANES - step, axis), y),
        )

    b0, b2 = far(a0, a2)
    b1, b3 = far(a1, a3)
    return near(b0, b1) + near(b2, b3)


def peer_at(count, me, step):
    peer = 0
    unit = 1
    while unit < count:
        peer = peer + lax.rem(lax.div(me, unit) + lax.div(step, unit), 2) * unit
        unit *= 2
    return peer


class Exchange:
    def __init__(self, peers, me, outbox, inbox, send_sem, recv_sem):
        self.peers, self.me = peers, me
        self.outbox, self.inbox, self.send_sem, self.recv_sem = outbox, inbox, send_sem, recv_sem

    def copy(self, src, dst, peer):
        return pltpu.make_async_remote_copy(
            src_ref=self.outbox.at[src],
            dst_ref=self.inbox.at[dst],
            send_sem=self.send_sem,
            recv_sem=self.recv_sem,
            device_id={"xz": peer},
            device_id_type=MESH,
        )

    def every(self):
        others = pl.ds(0, len(self.peers))
        return self.copy(others, others, self.peers[0])

    def start(self):
        for peer in self.peers:
            self.copy(peer, self.me, peer).start()
        self.inbox[self.me] = self.outbox[self.me]

    def arrive(self):
        self.every().wait_recv()

    def finish(self):
        self.every().wait_send()


def fused_kernel(count, stream_len, *refs):
    refs = list(refs)
    lift_far, state_far, drag_far, control_far, schur_far, span_far, inverse_far, forward_far = refs[:8]
    final, gradient = refs[8:10]
    (
        lift, fields, base, source, drag_term, direct, schur, drag_raw, drag, control, control_hat,
        span, inverse, forward, out1, in1, out2, in2, pair, damped, partial, outc, inc, outp, inp,
        halo_u, halo_v, halo_w, beyond, rim, corner, wall, reply, reply_rim, inp_other, share,
        load_sem, send_sem, recv_sem, plane_send, plane_recv, near_send, near_recv,
    ) = refs[10:]
    me = lax.axis_index("xz")
    slab = lax.axis_index("gy")
    rows, width, span_count = fields.shape[2], fields.shape[4], fields.shape[5]
    modes = HALVES * width
    chunks = rows // QUAD
    groups = count // QUAD
    tiles_q = span_count // LANES
    tiles = width // SUBLANES * tiles_q
    block = rows * width
    edge = (rows - 1) * (1 - slab)
    edge_pair = (rows - 2) * (1 - slab)
    edge_at = 1 - slab
    has_above = slab.astype(jnp.float32)
    has_below = 1.0 - has_above

    loads = {
        "stream": (state_far.at[0], fields.at[0]),
        "span": (span_far, span),
        "forward": (forward_far, forward),
        "control": (control_far, control),
        "inverse": (inverse_far, inverse),
        "drag": (drag_far, drag_raw),
        "rest": (state_far.at[1:3], fields.at[1:3]),
        "schur": (schur_far, schur),
        "lift": (lift_far, lift),
    }
    loads = {
        name: pltpu.make_async_copy(far, near, load_sem.at[i]) for i, (name, (far, near)) in enumerate(loads.items())
    }
    loads["stream"].start()
    loads["span"].start()
    order = sorted(range(1, count), key=lambda step: (FAR_FIRST[step * QUAD // count], -step))
    peers = [peer_at(count, me, step) for step in order]
    barrier = pltpu.get_barrier_semaphore()
    for peer in peers:
        pl.semaphore_signal(barrier, inc=1, device_id={"xz": peer}, device_id_type=MESH)
    pl.semaphore_signal(barrier, inc=1, device_id={"gy": 1 - slab}, device_id_type=MESH)

    def first(h, g):
        return Exchange(peers, me, out1.at[h, g], in1.at[h, g], send_sem.at[0, h, g], recv_sem.at[0, h, g])

    def second(h, g):
        return Exchange(peers, me, out2.at[h, g], in2.at[h, g], send_sem.at[1, h, g], recv_sem.at[1, h, g])

    third = Exchange(peers, me, outc, inc, plane_send.at[0, 0], plane_recv.at[0, 0])

    def fourth(h):
        return Exchange(peers, me, outp.at[h], inp.at[h], plane_send.at[1, h], plane_recv.at[1, h])

    def across(src, dst, index):
        return pltpu.make_async_remote_copy(
            src_ref=src,
            dst_ref=dst,
            send_sem=near_send.at[index],
            recv_sem=near_recv.at[index],
            device_id={"gy": 1 - slab},
            device_id_type=MESH,
        )

    def halo_copies(h):
        return [
            across(fields.at[0, :, edge, h], halo_u.at[h], h),
            across(fields.at[1, :, pl.ds(edge_pair, 2), h], halo_v.at[h], HALVES + h),
            across(fields.at[2, :, edge, h], halo_w.at[h], 2 * HALVES + h),
        ]

    def rim_copy(h, turn):
        return across(direct.at[:, pl.ds(edge_pair, 2)], rim.at[turn, h], (3 + turn) * HALVES + h)

    def plane_copy(h):
        return across(inp.at[h], inp_other.at[h], 5 * HALVES + h)

    corner_copy = across(schur.at[pl.ds(edge_pair, 2), edge], corner, 6 * HALVES)
    control_copy = across(control_hat.at[:, slab], control_hat.at[:, slab], 6 * HALVES + 2)
    reply_copy = across(reply.at[edge], reply_rim, 6 * HALVES + 1)

    def every_half(action):
        def body(h, carry):
            action(h)
            return carry

        lax.fori_loop(0, HALVES, body, 0)

    def every_tile(action):
        def body(t, carry):
            sub = lax.div(t, tiles_q)
            column = lax.rem(t, tiles_q)
            at = (
                pl.ds(pl.multiple_of(sub * SUBLANES, SUBLANES), SUBLANES),
                pl.ds(pl.multiple_of(column * LANES, LANES), LANES),
            )
            action(at, sub, column)
            return carry

        lax.fori_loop(0, tiles, body, 0)

    def mode_ids(h, sub):
        return me * modes + h * width + sub * SUBLANES + lax.broadcasted_iota(jnp.int32, (SUBLANES, LANES), 0)

    def waves(h, sub, column):
        kx = 2.0 * math.pi / stream_len * mode_ids(h, sub).astype(jnp.float32)
        q = column * LANES + lax.broadcasted_iota(jnp.int32, (SUBLANES, LANES), 1)
        signed = jnp.where(q < span_count // 2, q, q - span_count)
        kz = jnp.where(q == span_count // 2, 0.0, 2.0 * math.pi / span_count * signed.astype(jnp.float32))
        return kx, kz

    def mode_weight(h, sub):
        return jnp.where(mode_ids(h, sub) == 0, 1.0, 2.0)

    def pack_first(h, weighted, low=0, high=chunks):
        x = fields[0, :, QUAD * low : QUAD * high, h]
        if weighted:
            ids = me * modes + h * width + lax.broadcasted_iota(jnp.int32, x.shape, 2)
            x = x * jnp.where(ids == 0, 1.0, 2.0)
        size = x.shape[1] * width
        w = span_product(x.reshape(2 * size, span_count), span)
        halfway = (
            w[:size, :span_count] - w[size:, span_count:],
            w[:size, span_count:] + w[size:, :span_count],
        )
        for g in range(low, high):
            for part in range(2):
                for group in range(groups):
                    lanes = slice(LANES * group, LANES * (group + 1))
                    start = width * QUAD * (g - low)
                    parts = [halfway[part][start + width * y : start + width * (y + 1), lanes] for y in range(QUAD)]
                    for i, tile in enumerate(swap_groups(parts)):
                        out1[h, g, QUAD * group + i, part] = tile

    def send_first(h, weighted):
        pack_first(h, weighted)
        first(h, 0).start()

        @pl.when(h == 0)
        def _():
            for g in range(1, chunks):
                first(0, g).start()

    def every_tile_row(action):
        size = stream_len // HALVES

        def body(index, carry):
            action(pl.ds(pl.multiple_of(index * size, size), size))
            return carry

        lax.fori_loop(0, HALVES, body, 0)

    def return_half(h, g):
        y = split_product(forward, slice(h * block * 4, (h + 1) * block * 4), slice(None), damped.at[g])
        out2[h, g] = y.reshape(count, 2, width, LANES)

    def physical(again):
        early, late = slice(0, stream_len // HALVES), slice(stream_len // HALVES, stream_len)
        first(1, 0).finish()
        for g in range(1, chunks):
            first(1, g).start()
        for g in range(chunks):
            first(0, g).arrive()
            fill_pair(pair, early, in1[0, g].reshape(-1, LANES))

            def begin(at):
                partial[g, at, :] = split_product(inverse, at, early, pair.at[early])

            every_tile_row(begin)
        for g in range(chunks):
            first(1, g).arrive()
            fill_pair(pair, late, in1[1, g].reshape(-1, LANES))
            if again:
                second(1, g).finish()

            def damp(at):
                y = partial[g, at, :] + split_product(inverse, at, late, pair.at[late])
                fill_pair(damped.at[g], at, y * drag[g, at, :])

            every_tile_row(damp)
            return_half(0, g)
            second(0, g).start()
        for g in range(chunks):
            return_half(1, g)
            first(0, g).finish()
            if g:
                first(1, g).finish()

    def send_rest():
        second(0, 0).finish()
        second(1, 0).start()
        for g in range(1, chunks):
            second(0, g).finish()

    def collect(h, low=0, high=chunks):
        parts = []
        for part in range(2):
            for g in range(low, high):
                columns = []
                for group in range(groups):
                    pieces = [in2[h, g, QUAD * group + i, part] for i in range(QUAD)]
                    columns.append(jnp.concatenate(swap_groups(pieces), axis=0))
                parts.append(jnp.concatenate(columns, axis=1))
        w = span_product(jnp.concatenate(parts, axis=0), span)
        size = w.shape[0] // 2
        shape = (size // width, width, span_count)
        lines = slice(QUAD * low, QUAD * high)
        drag_term[0, lines] = (w[:size, :span_count] + w[size:, span_count:]).reshape(shape)
        drag_term[1, lines] = (w[size:, :span_count] - w[:size, span_count:]).reshape(shape)

    def receive(h):
        for g in range(chunks):
            second(h, g).arrive()

        @pl.when(h == 0)
        def _():
            for g in range(1, chunks):
                second(1, g).start()

        collect(h)

    def spread(h, forced):
        def body(at, sub, column):
            kx, kz = waves(h, sub, column)
            keep = 1.0 - DIFFUSION * (2.0 + kx * kx + kz * kz)

            def smooth(lines):
                return [
                    lines[i] * keep + DIFFUSION * (lines[i - 1] + lines[i + 1]) for i in range(1, len(lines) - 1)
                ]

            def wide(halo, c, p):
                line = halo[(h, p) + at]
                return [has_above * line] + [fields[(c, p, y, h) + at] for y in range(rows)] + [has_below * line]

            stream = [smooth(wide(halo_u, 0, p)) for p in range(2)]
            across_span = [smooth(wide(halo_w, 2, p)) for p in range(2)]
            for p in range(2):
                outer, inner = halo_v[(h, p, 0) + at], halo_v[(h, p, 1) + at]
                lines = [has_above * outer, has_above * inner]
                lines += [fields[(1, p, y, h) + at] for y in range(rows)]
                lines += [has_below * outer, has_below * inner]
                lines = smooth(lines)
                if forced:
                    hat = control_hat[(p, h) + at]
                    places = [slab * (rows - 1)] + [slab * rows + y for y in range(rows)] + [rows]
                    lines = [line + lift[place] * hat for line, place in zip(lines, places)]
                lines = [has_above * lines[0]] + lines[1:-1] + [has_below * lines[-1]]
                beyond[(h, p) + at] = lines[0] + lines[-1]
                if not forced:
                    total = wall[(p, h) + at]
                    for y in range(rows):
                        total = total + lift[slab * rows + y] * lines[y + 1]
                    wall[(p, h) + at] = total
                sign = -1.0 if p == 0 else 1.0
                for y in range(rows):
                    base[(0, p, y, h) + at] = stream[p][y]
                    base[(1, p, y, h) + at] = lines[y + 1]
                    base[(2, p, y, h) + at] = across_span[p][y]
                    turned = sign * (kx * stream[1 - p][y] + kz * across_span[1 - p][y])
                    source[(p, y, h) + at] = turned + 0.5 * (lines[y + 2] - lines[y])

        every_tile(body)

    def apply_blocks(h, at, values, transposed):
        for i in range(rows):
            totals = [None, None]
            for j in range(rows):
                place = (j, i) if transposed else (i, j)
                factor = schur[place + (h,) + at]
                for p in range(2):
                    term = factor * values[p][j]
                    totals[p] = term if totals[p] is None else totals[p] + term
            for p in range(2):
                direct[(p, i) + at] = totals[p]

    def begin_solve(h):
        def body(at, sub, column):
            kx, _ = waves(h, sub, column)
            values = [
                [source[(0, y, h) + at] + kx * drag_term[(1, y) + at] for y in range(rows)],
                [source[(1, y, h) + at] - kx * drag_term[(0, y) + at] for y in range(rows)],
            ]
            apply_blocks(h, at, values, False)

        every_tile(body)

    def swap_rims(h, turn):
        copy = rim_copy(h, turn)
        copy.start()
        copy.wait_recv()
        copy.wait_send()

    def pressure_at(h, at, transposed):
        turn = corner[(1 - edge_at, h) + at]
        reach = [schur[((edge, i) if transposed else (i, edge)) + (h,) + at] for i in range(rows)]
        own = schur[(edge, edge, h) + at]
        wide = []
        for p in range(2):
            far = rim[(int(transposed), h, p, 1 - edge_at) + at]
            known = direct[(p, edge) + at] + has_above * (own * far)
            next_row = far + turn * known
            outer = has_above * far + has_below * next_row
            inside = [direct[(p, y) + at] + reach[y] * outer for y in range(rows)]
            wide.append([has_above * next_row] + inside + [has_below * next_row])
        return wide

    def finish_solve(h, target):
        def body(at, sub, column):
            kx, kz = waves(h, sub, column)
            wide = pressure_at(h, at, False)
            for p in range(2):
                sign = 1.0 if p == 0 else -1.0
                for y in range(rows):
                    turned = sign * wide[1 - p][y + 1]
                    slope = 0.5 * (wide[p][y + 2] - wide[p][y])
                    target[(0, p, y, h) + at] = base[(0, p, y, h) + at] - drag_term[(p, y) + at] + kx * turned
                    target[(1, p, y, h) + at] = base[(1, p, y, h) + at] - slope
                    target[(2, p, y, h) + at] = base[(2, p, y, h) + at] + kz * turned

        every_tile(body)

    def finish_and_reverse(h):
        def body(at, sub, column):
            kx, kz = waves(h, sub, column)
            wide = pressure_at(h, at, False)
            turn = corner[(edge_at, h) + at]
            own = schur[(edge, edge, h) + at]
            stream, normal, across_span = [], [], []
            for p in range(2):
                sign = 1.0 if p == 0 else -1.0
                far = rim[(0, h, p, 1 - edge_at) + at]
                known = direct[(p, edge) + at] + has_above * (own * far)
                inner_row = rim[(0, h, p, edge_at) + at] + turn * known
                edge_row = has_below * wide[p][rows] + has_above * wide[p][1]
                outside = beyond[(h, p) + at] + 0.5 * (has_above - has_below) * (inner_row - edge_row)
                lines = [has_above * outside]
                for y in range(rows):
                    turned = sign * wide[1 - p][y + 1]
                    slope = 0.5 * (wide[p][y + 2] - wide[p][y])
                    stream.append(base[(0, p, y, h) + at] - drag_term[(p, y) + at] + kx * turned)
                    lines.append(base[(1, p, y, h) + at] - slope)
                    across_span.append(base[(2, p, y, h) + at] + kz * turned)
                    final[(0, p, y, h) + at] = stream[-1]
                    final[(1, p, y, h) + at] = lines[-1]
                    final[(2, p, y, h) + at] = across_span[-1]
                normal.append(lines + [has_below * outside])
            values = []
            for p in range(2):
                sign = -1.0 if p == 0 else 1.0
                values.append(
                    [
                        sign * (kx * stream[rows * (1 - p) + y] + kz * across_span[rows * (1 - p) + y])
                        + 0.5 * (normal[p][y + 2] - normal[p][y])
                        for y in range(rows)
                    ]
                )
            for p in range(2):
                for y in range(rows):
                    source[(p, y, h) + at] = values[p][y]

        every_tile(body)

        def reverse(at, sub, column):
            values = [[source[(p, y, h) + at] for y in range(rows)] for p in range(2)]
            apply_blocks(h, at, values, True)

        every_tile(reverse)

    def finish_adjoint(h):
        def body(at, sub, column):
            kx, kz = waves(h, sub, column)
            wide = pressure_at(h, at, True)
            for p in range(2):
                sign = 1.0 if p == 0 else -1.0
                total = None
                for y in range(rows):
                    turned = sign * wide[1 - p][y + 1]
                    normal = final[(1, p, y, h) + at] - 0.5 * (wide[p][y + 2] - wide[p][y])
                    fields[(0, p, y, h) + at] = final[(0, p, y, h) + at] + kx * turned
                    fields[(1, p, y, h) + at] = normal
                    fields[(2, p, y, h) + at] = final[(2, p, y, h) + at] + kz * turned
                    term = lift[slab * rows + y] * normal
                    total = term if total is None else total + term
                wall[(p, h) + at] = total

        every_tile(body)

    def start_reply():
        reach_up = [has_above * lift[slab * (rows - 1)]] + [lift[slab * rows + y] for y in range(rows - 1)]
        reach_down = [lift[slab * rows + y] for y in range(1, rows)] + [has_below * lift[rows]]
        lift_slope = [0.5 * (down - up) for up, down in zip(reach_up, reach_down)]

        def body(h):
            def tile(at, sub, column):
                for i in range(rows):
                    total = None
                    for j in range(rows):
                        term = schur[(i, j, h) + at] * lift_slope[j]
                        total = term if total is None else total + term
                    reply[(i, h) + at] = total

            every_tile(tile)

        every_half(body)
        reply_copy.start()

    def finish_reply():
        reply_copy.wait_recv()
        reply_copy.wait_send()

        def body(h):
            def tile(at, sub, column):
                far = reply_rim[(h,) + at]
                outer = far + has_below * (corner[(1 - edge_at, h) + at] * reply[(edge, h) + at])
                for y in range(rows):
                    reply[(y, h) + at] = reply[(y, h) + at] + schur[(y, edge, h) + at] * outer

            every_tile(tile)

        every_half(body)

    def close_wall(h, g):
        def body(at, sub, column):
            kx, _ = waves(h, sub, column)
            kx = kx * mode_weight(h, sub)
            for p in range(2):
                sign = 1.0 if p == 0 else -1.0
                total = wall[(p, h) + at]
                for y in range(QUAD * g, QUAD * (g + 1)):
                    value = source[(p, y, h) + at] + sign * (kx * drag_term[(1 - p, y) + at])
                    total = total + reply[(y, h) + at] * value
                wall[(p, h) + at] = total

        every_tile(body)

    def start_halos(h):
        for copy in halo_copies(h):
            copy.start()

    def spread_all(forced):
        def body(h):
            for copy in halo_copies(h):
                copy.wait_recv()
                copy.wait_send()
            spread(h, forced)

        every_half(body)

    loads["stream"].wait()
    loads["span"].wait()
    for name in ("lift", "control", "forward", "rest", "schur", "drag", "inverse"):
        loads[name].start()
    for g in range(chunks):
        pack_first(0, True, g, g + 1)
        if g == 0:
            pl.semaphore_wait(barrier, count)
        first(0, g).start()
    pack_first(1, True)
    first(1, 0).start()

    loads["control"].wait()
    loads["forward"].wait()
    lines = control[...]
    blank = jnp.zeros((LANES - lines.shape[0], stream_len), jnp.float32)
    fill_pair(pair, slice(None), jnp.concatenate([lines, blank], axis=0).T)

    half = forward.shape[1] // HALVES
    places = pl.ds(pl.multiple_of(slab * half, half), half)
    y = mxu(forward[0, places, :], pair[...])
    y = y[:, :LANES] + (y[:, LANES:] + mxu(forward[1, places, :], pair[:, :LANES]))
    y = y.reshape(count, QUAD, SUBLANES, LANES)
    moved = y[:, 0]
    for j in range(1, QUAD):
        moved = moved + pltpu.roll(y[:, j], j * LANES // QUAD, 2)
    outc[...] = moved
    third.start()
    loads["rest"].wait()
    every_half(start_halos)
    loads["schur"].wait()
    loads["lift"].wait()
    corner_copy.start()
    start_reply()
    loads["drag"].wait()
    for g in range(chunks):
        drag[g] = drag_raw[QUAD * g : QUAD * (g + 1)].reshape(LANES, stream_len).T
    loads["inverse"].wait()
    physical(False)

    third.arrive()
    columns = []
    for group in range(groups):
        pieces = [inc[QUAD * group + i] for i in range(QUAD)]
        columns.append(jnp.concatenate(swap_groups(pieces), axis=0))
    w = span_product(jnp.concatenate(columns, axis=1), span)
    control_hat[0, slab] = w[:width, :span_count] + w[width:, span_count:]
    control_hat[1, slab] = w[width:, :span_count] - w[:width, span_count:]
    third.finish()
    control_copy.start()
    corner_copy.wait_recv()
    corner_copy.wait_send()
    finish_reply()
    control_copy.wait_recv()
    control_copy.wait_send()
    spread_all(True)
    send_rest()

    def step(h):
        receive(h)
        begin_solve(h)
        swap_rims(h, 0)
        finish_solve(h, fields)
        send_first(h, True)
        start_halos(h)

    every_half(step)
    physical(True)
    spread_all(True)
    send_rest()

    def turn(h):
        receive(h)
        begin_solve(h)
        swap_rims(h, 0)
        finish_and_reverse(h)
        swap_rims(h, 1)
        finish_adjoint(h)
        send_first(h, False)
        start_halos(h)

    every_half(turn)
    physical(True)
    spread_all(False)
    send_rest()

    def close(h):
        for g in range(chunks):
            second(h, g).arrive()
            if g == chunks - 1:

                @pl.when(h == 0)
                def _():
                    for later in range(1, chunks):
                        second(1, later).start()

                @pl.when(h == 1)
                def _():
                    fourth(0).start()

            collect(h, g, g + 1)
            close_wall(h, g)
        w = span_product(wall[:, h].reshape(2 * width, span_count), span)
        halfway = (
            w[:width, :span_count] - w[width:, span_count:],
            w[:width, span_count:] + w[width:, :span_count],
        )
        for group in range(groups):
            lanes = slice(LANES * group, LANES * (group + 1))
            pieces = [half[at : at + SUBLANES, lanes] for half in halfway for at in range(0, width, SUBLANES)]
            for i, tile in enumerate(swap_groups(pieces)):
                outp[h, QUAD * group + i] = tile

    def open_plane(h):
        fourth(h).arrive()
        copy = plane_copy(h)
        copy.start()
        copy.wait_recv()
        copy.wait_send()
        x = inp[h] + inp_other[h]
        turned = [x] + [pltpu.roll(x, LANES - j * LANES // QUAD, 2) for j in range(1, QUAD)]
        x = jnp.concatenate(turned, axis=1).reshape(-1, LANES)
        terms = slice(h * x.shape[0], (h + 1) * x.shape[0])
        fill_pair(pair, terms, x)
        places = pl.ds(pl.multiple_of(slab * gradient.shape[1], LANES), gradient.shape[1])
        y = mxu(inverse[0, places, terms], pair[terms, :])
        return y[:, :LANES] + (y[:, LANES:] + mxu(inverse[1, places, terms], pair[terms, :LANES]))

    every_half(close)
    fourth(1).start()
    share[...] = open_plane(0)
    gradient[...] = (share[...] + open_plane(1)).T[: gradient.shape[0]]
    for h in range(HALVES):
        fourth(h).finish()
    for g in range(chunks):
        second(1, g).finish()


VMEM = pl.BlockSpec(memory_space=pltpu.VMEM)
FAR = pl.BlockSpec(memory_space=pltpu.HBM)


def fused_call(count, initial_state, drag_rate, wall_control, lift_profile, schur_inverse):
    _, _, rows, modes, span_count = initial_state.shape
    stream_len = drag_rate.shape[2]
    narrow = wall_control.shape[0]
    width = modes // HALVES
    chunks = rows // QUAD
    span, inverse, forward = host_tables(stream_len, span_count, count)
    state = initial_state.reshape(3, 2, rows, HALVES, width, span_count)
    schur = schur_inverse.reshape(rows, rows, HALVES, width, span_count)
    plane = (2, rows, HALVES, width, span_count)
    half_plane = (2, rows, width, span_count)
    box = (HALVES, chunks, count, 2, width, LANES)
    thin = (HALVES, count, SUBLANES, LANES)
    line = (HALVES, 2, width, span_count)

    kept = 4 * (math.prod(state.shape) + narrow * stream_len // 2 + 16 * SUBLANES * LANES)

    def buffer(*shape):
        return pltpu.VMEM(shape, jnp.float32)

    pairs = pltpu.VMEM((stream_len, 2 * LANES), jnp.bfloat16)
    scratch = [pltpu.SMEM(lift_profile.shape, jnp.float32)] + [buffer(*state.shape)] * 2 + [buffer(*plane), buffer(*half_plane), buffer(*half_plane)]
    scratch += [buffer(*schur.shape), buffer(*drag_rate.shape), buffer(chunks, stream_len, LANES)]
    scratch += [buffer(*wall_control.shape), buffer(*line)]
    scratch += [pltpu.VMEM(table.shape, jnp.bfloat16) for table in (span, inverse, forward)]
    scratch += [buffer(*box)] * 4 + [pairs, pltpu.VMEM((chunks, stream_len, 2 * LANES), jnp.bfloat16), buffer(chunks, stream_len, LANES)] + [buffer(*thin[1:])] * 2 + [buffer(*thin)] * 2
    scratch += [buffer(*line), buffer(HALVES, 2, 2, width, span_count), buffer(*line), buffer(*line)]
    scratch += [buffer(2, HALVES, 2, 2, width, span_count), buffer(2, HALVES, width, span_count), buffer(*line)]
    scratch += [buffer(rows, HALVES, width, span_count), buffer(HALVES, width, span_count)]
    scratch += [buffer(*thin), buffer(stream_len // 2, LANES)]
    scratch += [pltpu.SemaphoreType.DMA((9,))]
    scratch += [pltpu.SemaphoreType.DMA((2, HALVES, chunks))] * 2
    scratch += [pltpu.SemaphoreType.DMA((2, HALVES))] * 2
    scratch += [pltpu.SemaphoreType.DMA((6 * HALVES + 3,))] * 2
    final, gradient = pl.pallas_call(
        functools.partial(fused_kernel, count, stream_len),
        out_shape=[
            pltpu.VMEM(state.shape, jnp.float32),
            pltpu.VMEM((narrow, stream_len // 2), jnp.float32),
        ],
        in_specs=[FAR] * 8,
        out_specs=[VMEM, VMEM],
        scratch_shapes=scratch,
        compiler_params=pltpu.CompilerParams(
            collective_id=0, has_side_effects=True, vmem_limit_bytes=VMEM_BYTES - kept
        ),
        cost_estimate=pl.CostEstimate(flops=60_000_000_000, bytes_accessed=32_000_000, transcendentals=0),
    )(lift_profile, state, drag_rate, wall_control, schur, span, inverse, forward)
    return final.reshape(initial_state.shape), gradient


def phase_pair(outer_size, inner_size, period, factor):
    outer_ids = jnp.arange(outer_size, dtype=jnp.int32)[:, None]
    inner_ids = jnp.arange(inner_size, dtype=jnp.int32)[None, :]
    angle = 2.0 * math.pi / period * (outer_ids * inner_ids % period).astype(jnp.float32)
    return (jnp.cos(angle) * factor, jnp.sin(angle) * factor)


def plain_transforms(count, rows, modes, span_count, stream_len):
    half_len = stream_len // 2
    cos_x, sin_x = phase_pair(stream_len, half_len, stream_len, 1.0 / math.sqrt(stream_len))
    cos_z, sin_z = phase_pair(span_count, span_count, span_count, 1.0 / math.sqrt(span_count))

    def to_spectral(physical):
        real_half = jnp.einsum("yzn,nk->yzk", physical, cos_x, precision=HIGHEST)
        imag_half = -jnp.einsum("yzn,nk->yzk", physical, sin_x, precision=HIGHEST)
        halfway = jnp.stack([real_half, imag_half])
        pieces = lax.all_to_all(halfway, "xz", split_axis=3, concat_axis=2, tiled=True)
        with_cos = jnp.einsum("cyzk,zq->cykq", pieces, cos_z, precision=HIGHEST)
        with_sin = jnp.einsum("cyzk,zq->cykq", pieces, sin_z, precision=HIGHEST)
        return jnp.stack([with_cos[0] + with_sin[1], with_cos[1] - with_sin[0]])

    def to_physical(spectral):
        with_cos = jnp.einsum("cykq,qz->cykz", spectral, cos_z, precision=HIGHEST)
        with_sin = jnp.einsum("cykq,qz->cykz", spectral, sin_z, precision=HIGHEST)
        halfway = jnp.stack([with_cos[0] - with_sin[1], with_sin[0] + with_cos[1]])
        pieces = lax.all_to_all(halfway, "xz", split_axis=3, concat_axis=2, tiled=True)
        return jnp.einsum("ykz,nk->yzn", pieces[0], cos_x, precision=HIGHEST) - jnp.einsum(
            "ykz,nk->yzn", pieces[1], sin_x, precision=HIGHEST
        )

    def begin(drag_rate, control):
        def drag_map(s):
            return to_spectral(drag_rate * to_physical(s))

        return drag_map, (lambda s: (drag_map(s), to_spectral(control[None])[:, 0]))

    def plane(spectral):
        return to_physical(spectral[:, None])[0]

    return begin, plane


def rotate(spectrum, factor):
    return jnp.stack([-factor * spectrum[1], factor * spectrum[0]])


def per_device(initial_state, drag_rate, wall_control, lift_profile, schur_inverse):
    row_count = initial_state.shape[2]
    mode_count = initial_state.shape[3]
    span_count = initial_state.shape[4]
    stream_len = drag_rate.shape[2]
    last_row = row_count - 1
    slab_count = lax.axis_size("gy")
    slab_index = lax.axis_index("gy")
    pencil_count = lax.axis_size("xz")
    pencil_index = lax.axis_index("xz")
    mode_ids = pencil_index * mode_count + jnp.arange(mode_count)
    stream_factor = (2.0 * math.pi / stream_len * mode_ids.astype(jnp.float32))[:, None]
    mode_weight = jnp.where(mode_ids == 0, 1.0, 2.0).astype(jnp.float32)[:, None]
    span_ids = jnp.arange(span_count)
    signed = jnp.where(span_ids < span_count // 2, span_ids, span_ids - span_count)
    span_wave = jnp.where(
        span_ids == span_count // 2, 0.0, 2.0 * math.pi / span_count * signed.astype(jnp.float32)
    )
    wave_square = stream_factor**2 + span_wave[None, :] ** 2
    fits = (
        slab_count == 2
        and QUAD * mode_count == LANES
        and QUAD * drag_rate.shape[1] == LANES
        and row_count == SUBLANES
        and pencil_count * mode_count * 2 == stream_len
        and pencil_count * drag_rate.shape[1] == span_count
        and pencil_count & (pencil_count - 1) == 0
        and pencil_count % QUAD == 0
    )
    if fits:
        return fused_call(pencil_count, initial_state, drag_rate, wall_control, lift_profile, schur_inverse)
    begin, plane = plain_transforms(pencil_count, row_count, mode_count, span_count, stream_len)
    drag_map, first_map = begin(drag_rate, wall_control)

    ends = slab_count - 1

    def from_above(tail):
        return lax.ppermute(tail, "gy", [(i, i + 1) for i in range(ends)])

    def from_below(head):
        return lax.ppermute(head, "gy", [(i + 1, i) for i in range(ends)])

    def every_slab(values):
        if slab_count == 2:
            other = lax.ppermute(values, "gy", [(0, 1), (1, 0)])
            return [jnp.where(slab_index == 0, values, other), jnp.where(slab_index == 0, other, values)]
        gathered = lax.all_gather(values, "gy", axis=0)
        return [gathered[i] for i in range(slab_count)]

    has_above = (slab_index > 0).astype(jnp.float32)
    has_below = (slab_index < slab_count - 1).astype(jnp.float32)
    corners = every_slab(
        jnp.stack(
            [
                schur_inverse[0, 0],
                schur_inverse[0, last_row],
                schur_inverse[last_row, 0],
                schur_inverse[last_row, last_row],
            ]
        )
    )
    corner_above = jnp.zeros_like(corners[0][3])
    for member in range(slab_count - 1):
        corner_above = jnp.where(slab_index == member + 1, corners[member][3], corner_above)

    padded_lift = jnp.pad(lift_profile, 1)
    lift_near = lax.dynamic_slice_in_dim(padded_lift, slab_index * row_count, row_count + 2)
    lift_own = lift_near[1 : row_count + 1]

    def halos(fields):
        tail = jnp.concatenate([fields[0, :, last_row:], fields[1, :, last_row - 1 :], fields[2, :, last_row:]], axis=1)
        head = jnp.concatenate([fields[0, :, :1], fields[1, :, :2], fields[2, :, :1]], axis=1)
        return from_above(tail), from_below(head)

    def smooth(wide):
        own = wide[:, 1:-1]
        laplace = wide[:, 2:] - 2.0 * own + wide[:, :-2]
        return own + DIFFUSION * (laplace - wave_square * own)

    def slope(wide):
        return 0.5 * (wide[:, 2:] - wide[:, :-2])

    def advance(fields, drag_term, control_hat):
        above, below = halos(fields)
        stream_star = smooth(jnp.concatenate([above[:, 0:1], fields[0], below[:, 0:1]], axis=1)) - drag_term
        span_star = smooth(jnp.concatenate([above[:, 3:4], fields[2], below[:, 3:4]], axis=1))
        normal_wide = smooth(jnp.concatenate([above[:, 1:3], fields[1], below[:, 1:3]], axis=1))
        if control_hat is not None:
            normal_wide = normal_wide + lift_near[:, None, None] * control_hat[:, None]
        normal_wide = jnp.concatenate(
            [has_above * normal_wide[:, :1], normal_wide[:, 1:-1], has_below * normal_wide[:, -1:]], axis=1
        )
        return stream_star, normal_wide[:, 1:-1], span_star, slope(normal_wide)

    def apply_blocks(values, transposed):
        summed = None
        for column in range(row_count):
            factor = schur_inverse[column] if transposed else schur_inverse[:, column]
            term = factor[None] * values[:, column : column + 1]
            summed = term if summed is None else summed + term
        return summed

    def solve(source, transposed):
        if transposed:
            first_column, last_column = schur_inverse[0], schur_inverse[last_row]
            ratio_at, turn_at = 1, 2
        else:
            first_column, last_column = schur_inverse[:, 0], schur_inverse[:, last_row]
            ratio_at, turn_at = 2, 1
        direct = apply_blocks(source, transposed)
        rims = every_slab(jnp.stack([direct[:, 0], direct[:, last_row]]))
        running = jnp.zeros_like(direct[:, 0])
        before = []
        for member in range(slab_count):
            before.append(running)
            running = rims[member][1] + corners[member][ratio_at][None] * running
        running = jnp.zeros_like(direct[:, 0])
        behind = [running] * slab_count
        for member in reversed(range(slab_count)):
            behind[member] = running
            top = rims[member][0] + corners[member][0][None] * before[member]
            running = top + corners[member][turn_at][None] * running
        entering, leaving = before[0], behind[0]
        for member in range(1, slab_count):
            entering = jnp.where(slab_index == member, before[member], entering)
            leaving = jnp.where(slab_index == member, behind[member], leaving)
        pressure = direct + first_column[None] * entering[:, None] + last_column[None] * leaving[:, None]
        row_above = entering + corner_above[None] * pressure[:, 0]
        return jnp.concatenate([row_above[:, None], pressure, leaving[:, None]], axis=1)

    def project(stream_part, normal_part, span_part, normal_slope, transposed):
        divergence = rotate(stream_part, stream_factor) + normal_slope + rotate(span_part, span_wave)
        wide = solve(divergence, transposed)
        pressure = wide[:, 1:-1]
        return jnp.stack(
            [
                stream_part - rotate(pressure, stream_factor),
                normal_part - slope(wide),
                span_part - rotate(pressure, span_wave),
            ]
        )

    fields = initial_state
    control_hat = None
    for section_index in range(STEPS):
        weighted = mode_weight * fields[0]
        if section_index == 0:
            drag_term, control_hat = first_map(weighted)
        else:
            drag_term = drag_map(weighted)
        fields = project(*advance(fields, drag_term, control_hat), False)
    final = fields
    normal_slope = slope(
        jnp.concatenate([from_above(final[1, :, last_row:]), final[1], from_below(final[1, :, :1])], axis=1)
    )
    parts = (final[0], final[1], final[2], normal_slope)
    wall_sum = jnp.zeros_like(control_hat)
    for section_index in range(STEPS):
        projected = project(*parts, True)
        wall_sum = wall_sum + jnp.sum(lift_own[:, None, None] * projected[1], axis=1)
        if section_index + 1 < STEPS:
            parts = advance(projected, mode_weight * drag_map(projected[0]), None)
    share = plane(wall_sum)
    if slab_count == 2:
        half = stream_len // 2
        first, second = share[:, :half], share[:, half:]
        upper = slab_index == 0
        other = lax.ppermute(jnp.where(upper, second, first), "gy", [(0, 1), (1, 0)])
        control_gradient = jnp.where(upper, first, second) + other
    else:
        control_gradient = lax.psum_scatter(share, "gy", scatter_dimension=1, tiled=True)
    return (final, control_gradient)


def solution(mesh):
    return jax.shard_map(
        per_device,
        mesh=mesh,
        in_specs=(
            P(None, None, "gy", "xz", None),
            P("gy", "xz", None),
            P("xz", None),
            P(),
            P("gy", None, "xz", None),
        ),
        out_specs=(P(None, None, "gy", "xz", None), P("xz", "gy")),
        check_vma=False,
    )
```

```python
import functools
import math

import jax
import jax.numpy as jnp
import ml_dtypes
import numpy as np
from jax import lax
from jax.experimental import pallas as pl
from jax.experimental.pallas import tpu as pltpu
from jax.sharding import PartitionSpec as P

STEPS = 2


DIFFUSION = 0.04
HIGHEST = lax.Precision.HIGHEST
MESH = pl.DeviceIdType.MESH
LANES = 128
QUAD = 4
HALVES = 2
SUBLANES = 8
FAR_FIRST = (3, 2, 0, 1)
VMEM_BYTES = 67_043_328


def split_host(table):
    high = table.astype(ml_dtypes.bfloat16)
    low = (table - high.astype(np.float64)).astype(ml_dtypes.bfloat16)
    return np.stack([high, low])


def host_tables(stream_len, span_count, count):
    z = np.arange(span_count)
    angle = 2.0 * math.pi / span_count * (np.outer(z, z) % span_count)
    span = np.concatenate([np.cos(angle), np.sin(angle)], axis=1) / math.sqrt(span_count)
    n = np.arange(stream_len)
    k = np.arange(stream_len // 2)
    angle = 2.0 * math.pi / stream_len * (np.outer(k, n) % stream_len)
    stream = np.stack([np.cos(angle), -np.sin(angle)]) / math.sqrt(stream_len)
    stream = stream.reshape(2, count, HALVES, -1, stream_len).transpose(2, 1, 0, 3, 4).reshape(-1, stream_len)
    return split_host(span), split_host(stream.T.copy()), split_host(stream)


def split_pair(x):
    high = x.astype(jnp.bfloat16)
    low = (x - high.astype(jnp.float32)).astype(jnp.bfloat16)
    return high, low


def mxu(a, b):
    return jnp.dot(a, b, preferred_element_type=jnp.float32)


def span_product(x, table):
    high, low = split_pair(x)
    both = mxu(jnp.concatenate([high, low], axis=0), table[0])
    return both[: x.shape[0]] + (both[x.shape[0] :] + mxu(high, table[1]))


def split_product(table, rows, terms, pair):
    wide = mxu(table[0, rows, terms], pair[...])
    narrow = mxu(table[1, rows, terms], pair[:, :LANES])
    return wide[:, :LANES] + (wide[:, LANES:] + narrow)


def fill_pair(pair, rows, x):
    high, low = split_pair(x)
    pair[rows, :LANES] = high
    pair[rows, LANES:] = low


def swap_groups(tiles):
    a0, a1, a2, a3 = tiles
    group = lax.broadcasted_iota(jnp.int32, a0.shape, a0.ndim - 1) // (LANES // QUAD)
    lower = group < 2
    even = group % 2 == 0
    axis = a0.ndim - 1
    half = LANES // 2
    step = LANES // QUAD

    def far(x, y):
        return (
            jnp.where(lower, x, pltpu.roll(y, half, axis)),
            jnp.where(lower, pltpu.roll(x, half, axis), y),
        )

    def near(x, y):
        return (
            jnp.where(even, x, pltpu.roll(y, step, axis)),
            jnp.where(even, pltpu.roll(x, LANES - step, axis), y),
        )

    b0, b2 = far(a0, a2)
    b1, b3 = far(a1, a3)
    return near(b0, b1) + near(b2, b3)


def peer_at(count, me, step):
    peer = 0
    unit = 1
    while unit < count:
        peer = peer + lax.rem(lax.div(me, unit) + lax.div(step, unit), 2) * unit
        unit *= 2
    return peer


class Exchange:
    def __init__(self, peers, me, outbox, inbox, send_sem, recv_sem):
        self.peers, self.me = peers, me
        self.outbox, self.inbox, self.send_sem, self.recv_sem = outbox, inbox, send_sem, recv_sem

    def copy(self, src, dst, peer):
        return pltpu.make_async_remote_copy(
            src_ref=self.outbox.at[src],
            dst_ref=self.inbox.at[dst],
            send_sem=self.send_sem,
            recv_sem=self.recv_sem,
            device_id={"xz": peer},
            device_id_type=MESH,
        )

    def every(self):
        others = pl.ds(0, len(self.peers))
        return self.copy(others, others, self.peers[0])

    def start(self):
        for peer in self.peers:
            self.copy(peer, self.me, peer).start()
        self.inbox[self.me] = self.outbox[self.me]

    def arrive(self):
        self.every().wait_recv()

    def finish(self):
        self.every().wait_send()


def fused_kernel(count, stream_len, *refs):
    refs = list(refs)
    lift_far, state_far, drag_far, control_far, schur_far, span_far, inverse_far, forward_far = refs[:8]
    final, gradient = refs[8:10]
    (
        lift, fields, base, source, drag_term, direct, schur, drag_raw, drag, control, control_hat,
        span, inverse, forward, out1, in1, out2, in2, pair, damped, partial, outc, inc, outp, inp,
        halo_u, halo_v, halo_w, beyond, rim, corner, wall, reply, reply_rim, inp_other, share,
        load_sem, send_sem, recv_sem, plane_send, plane_recv, near_send, near_recv,
    ) = refs[10:]
    me = lax.axis_index("xz")
    slab = lax.axis_index("gy")
    rows, width, span_count = fields.shape[2], fields.shape[4], fields.shape[5]
    modes = HALVES * width
    chunks = rows // QUAD
    groups = count // QUAD
    tiles_q = span_count // LANES
    tiles = width // SUBLANES * tiles_q
    block = rows * width
    edge = (rows - 1) * (1 - slab)
    edge_pair = (rows - 2) * (1 - slab)
    edge_at = 1 - slab
    has_above = slab.astype(jnp.float32)
    has_below = 1.0 - has_above

    loads = {
        "stream": (state_far.at[0], fields.at[0]),
        "span": (span_far, span),
        "forward": (forward_far, forward),
        "control": (control_far, control),
        "inverse": (inverse_far, inverse),
        "drag": (drag_far, drag_raw),
        "rest": (state_far.at[1:3], fields.at[1:3]),
        "schur": (schur_far, schur),
        "lift": (lift_far, lift),
    }
    loads = {
        name: pltpu.make_async_copy(far, near, load_sem.at[i]) for i, (name, (far, near)) in enumerate(loads.items())
    }
    loads["stream"].start()
    loads["span"].start()
    order = sorted(range(1, count), key=lambda step: (FAR_FIRST[step * QUAD // count], -step))
    peers = [peer_at(count, me, step) for step in order]
    barrier = pltpu.get_barrier_semaphore()
    for peer in peers:
        pl.semaphore_signal(barrier, inc=1, device_id={"xz": peer}, device_id_type=MESH)
    pl.semaphore_signal(barrier, inc=1, device_id={"gy": 1 - slab}, device_id_type=MESH)

    def first(h, g):
        return Exchange(peers, me, out1.at[h, g], in1.at[h, g], send_sem.at[0, h, g], recv_sem.at[0, h, g])

    def second(h, g):
        return Exchange(peers, me, out2.at[h, g], in2.at[h, g], send_sem.at[1, h, g], recv_sem.at[1, h, g])

    third = Exchange(peers, me, outc, inc, plane_send.at[0, 0], plane_recv.at[0, 0])

    def fourth(h):
        return Exchange(peers, me, outp.at[h], inp.at[h], plane_send.at[1, h], plane_recv.at[1, h])

    def across(src, dst, index):
        return pltpu.make_async_remote_copy(
            src_ref=src,
            dst_ref=dst,
            send_sem=near_send.at[index],
            recv_sem=near_recv.at[index],
            device_id={"gy": 1 - slab},
            device_id_type=MESH,
        )

    def halo_copies(h):
        return [
            across(fields.at[0, :, edge, h], halo_u.at[h], h),
            across(fields.at[1, :, pl.ds(edge_pair, 2), h], halo_v.at[h], HALVES + h),
            across(fields.at[2, :, edge, h], halo_w.at[h], 2 * HALVES + h),
        ]

    def rim_copy(h, turn):
        return across(direct.at[:, pl.ds(edge_pair, 2)], rim.at[turn, h], (3 + turn) * HALVES + h)

    def plane_copy(h):
        return across(inp.at[h], inp_other.at[h], 5 * HALVES + h)

    corner_copy = across(schur.at[pl.ds(edge_pair, 2), edge], corner, 6 * HALVES)
    control_copy = across(control_hat.at[:, slab], control_hat.at[:, slab], 6 * HALVES + 2)
    reply_copy = across(reply.at[edge], reply_rim, 6 * HALVES + 1)

    def every_half(action):
        def body(h, carry):
            action(h)
            return carry

        lax.fori_loop(0, HALVES, body, 0)

    def every_tile(action):
        def body(t, carry):
            sub = lax.div(t, tiles_q)
            column = lax.rem(t, tiles_q)
            at = (
                pl.ds(pl.multiple_of(sub * SUBLANES, SUBLANES), SUBLANES),
                pl.ds(pl.multiple_of(column * LANES, LANES), LANES),
            )
            action(at, sub, column)
            return carry

        lax.fori_loop(0, tiles, body, 0)

    def mode_ids(h, sub):
        return me * modes + h * width + sub * SUBLANES + lax.broadcasted_iota(jnp.int32, (SUBLANES, LANES), 0)

    def waves(h, sub, column):
        kx = 2.0 * math.pi / stream_len * mode_ids(h, sub).astype(jnp.float32)
        q = column * LANES + lax.broadcasted_iota(jnp.int32, (SUBLANES, LANES), 1)
        signed = jnp.where(q < span_count // 2, q, q - span_count)
        kz = jnp.where(q == span_count // 2, 0.0, 2.0 * math.pi / span_count * signed.astype(jnp.float32))
        return kx, kz

    def mode_weight(h, sub):
        return jnp.where(mode_ids(h, sub) == 0, 1.0, 2.0)

    def pack_first(h, weighted, low=0, high=chunks):
        x = fields[0, :, QUAD * low : QUAD * high, h]
        if weighted:
            ids = me * modes + h * width + lax.broadcasted_iota(jnp.int32, x.shape, 2)
            x = x * jnp.where(ids == 0, 1.0, 2.0)
        size = x.shape[1] * width
        w = span_product(x.reshape(2 * size, span_count), span)
        halfway = (
            w[:size, :span_count] - w[size:, span_count:],
            w[:size, span_count:] + w[size:, :span_count],
        )
        for g in range(low, high):
            for part in range(2):
                for group in range(groups):
                    lanes = slice(LANES * group, LANES * (group + 1))
                    start = width * QUAD * (g - low)
                    parts = [halfway[part][start + width * y : start + width * (y + 1), lanes] for y in range(QUAD)]
                    for i, tile in enumerate(swap_groups(parts)):
                        out1[h, g, QUAD * group + i, part] = tile

    def send_first(h, weighted):
        pack_first(h, weighted)
        first(h, 0).start()

        @pl.when(h == 0)
        def _():
            for g in range(1, chunks):
                first(0, g).start()

    def every_tile_row(action):
        size = stream_len // HALVES

        def body(index, carry):
            action(pl.ds(pl.multiple_of(index * size, size), size))
            return carry

        lax.fori_loop(0, HALVES, body, 0)

    def return_half(h, g):
        y = split_product(forward, slice(h * block * 4, (h + 1) * block * 4), slice(None), damped.at[g])
        out2[h, g] = y.reshape(count, 2, width, LANES)

    def physical(again):
        early, late = slice(0, stream_len // HALVES), slice(stream_len // HALVES, stream_len)
        for g in range(1, chunks):
            first(1, g).start()
        for g in range(chunks):
            first(0, g).arrive()
            fill_pair(pair, early, in1[0, g].reshape(-1, LANES))

            def begin(at):
                partial[g, at, :] = split_product(inverse, at, early, pair.at[early])

            every_tile_row(begin)
        for g in range(chunks):
            first(1, g).arrive()
            fill_pair(pair, late, in1[1, g].reshape(-1, LANES))
            if again:
                second(1, g).finish()

            def damp(at):
                y = partial[g, at, :] + split_product(inverse, at, late, pair.at[late])
                fill_pair(damped.at[g], at, y * drag[g, at, :])

            every_tile_row(damp)
            return_half(0, g)
            second(0, g).start()
        for g in range(chunks):
            return_half(1, g)
            first(0, g).finish()
            first(1, g).finish()

    def send_rest():
        second(0, 0).finish()
        second(1, 0).start()
        for g in range(1, chunks):
            second(0, g).finish()

    def collect(h, low=0, high=chunks):
        parts = []
        for part in range(2):
            for g in range(low, high):
                columns = []
                for group in range(groups):
                    pieces = [in2[h, g, QUAD * group + i, part] for i in range(QUAD)]
                    columns.append(jnp.concatenate(swap_groups(pieces), axis=0))
                parts.append(jnp.concatenate(columns, axis=1))
        w = span_product(jnp.concatenate(parts, axis=0), span)
        size = w.shape[0] // 2
        shape = (size // width, width, span_count)
        lines = slice(QUAD * low, QUAD * high)
        drag_term[0, lines] = (w[:size, :span_count] + w[size:, span_count:]).reshape(shape)
        drag_term[1, lines] = (w[size:, :span_count] - w[:size, span_count:]).reshape(shape)

    def receive(h):
        for g in range(chunks):
            second(h, g).arrive()

        @pl.when(h == 0)
        def _():
            for g in range(1, chunks):
                second(1, g).start()

        collect(h)

    def spread(h, forced):
        def body(at, sub, column):
            kx, kz = waves(h, sub, column)
            keep = 1.0 - DIFFUSION * (2.0 + kx * kx + kz * kz)

            def smooth(lines):
                return [
                    lines[i] * keep + DIFFUSION * (lines[i - 1] + lines[i + 1]) for i in range(1, len(lines) - 1)
                ]

            def wide(halo, c, p):
                line = halo[(h, p) + at]
                return [has_above * line] + [fields[(c, p, y, h) + at] for y in range(rows)] + [has_below * line]

            stream = [smooth(wide(halo_u, 0, p)) for p in range(2)]
            across_span = [smooth(wide(halo_w, 2, p)) for p in range(2)]
            for p in range(2):
                outer, inner = halo_v[(h, p, 0) + at], halo_v[(h, p, 1) + at]
                lines = [has_above * outer, has_above * inner]
                lines += [fields[(1, p, y, h) + at] for y in range(rows)]
                lines += [has_below * outer, has_below * inner]
                lines = smooth(lines)
                if forced:
                    hat = control_hat[(p, h) + at]
                    places = [slab * (rows - 1)] + [slab * rows + y for y in range(rows)] + [rows]
                    lines = [line + lift[place] * hat for line, place in zip(lines, places)]
                lines = [has_above * lines[0]] + lines[1:-1] + [has_below * lines[-1]]
                beyond[(h, p) + at] = lines[0] + lines[-1]
                if not forced:
                    total = wall[(p, h) + at]
                    for y in range(rows):
                        total = total + lift[slab * rows + y] * lines[y + 1]
                    wall[(p, h) + at] = total
                sign = -1.0 if p == 0 else 1.0
                for y in range(rows):
                    base[(0, p, y, h) + at] = stream[p][y]
                    base[(1, p, y, h) + at] = lines[y + 1]
                    base[(2, p, y, h) + at] = across_span[p][y]
                    turned = sign * (kx * stream[1 - p][y] + kz * across_span[1 - p][y])
                    source[(p, y, h) + at] = turned + 0.5 * (lines[y + 2] - lines[y])

        every_tile(body)

    def apply_blocks(h, at, values, transposed):
        for i in range(rows):
            totals = [None, None]
            for j in range(rows):
                place = (j, i) if transposed else (i, j)
                factor = schur[place + (h,) + at]
                for p in range(2):
                    term = factor * values[p][j]
                    totals[p] = term if totals[p] is None else totals[p] + term
            for p in range(2):
                direct[(p, i) + at] = totals[p]

    def begin_solve(h):
        def body(at, sub, column):
            kx, _ = waves(h, sub, column)
            values = [
                [source[(0, y, h) + at] + kx * drag_term[(1, y) + at] for y in range(rows)],
                [source[(1, y, h) + at] - kx * drag_term[(0, y) + at] for y in range(rows)],
            ]
            apply_blocks(h, at, values, False)

        every_tile(body)

    def swap_rims(h, turn):
        copy = rim_copy(h, turn)
        copy.start()
        copy.wait_recv()
        copy.wait_send()

    def pressure_at(h, at, transposed):
        turn = corner[(1 - edge_at, h) + at]
        reach = [schur[((edge, i) if transposed else (i, edge)) + (h,) + at] for i in range(rows)]
        own = schur[(edge, edge, h) + at]
        wide = []
        for p in range(2):
            far = rim[(int(transposed), h, p, 1 - edge_at) + at]
            known = direct[(p, edge) + at] + has_above * (own * far)
            next_row = far + turn * known
            outer = has_above * far + has_below * next_row
            inside = [direct[(p, y) + at] + reach[y] * outer for y in range(rows)]
            wide.append([has_above * next_row] + inside + [has_below * next_row])
        return wide

    def finish_solve(h, target):
        def body(at, sub, column):
            kx, kz = waves(h, sub, column)
            wide = pressure_at(h, at, False)
            for p in range(2):
                sign = 1.0 if p == 0 else -1.0
                for y in range(rows):
                    turned = sign * wide[1 - p][y + 1]
                    slope = 0.5 * (wide[p][y + 2] - wide[p][y])
                    target[(0, p, y, h) + at] = base[(0, p, y, h) + at] - drag_term[(p, y) + at] + kx * turned
                    target[(1, p, y, h) + at] = base[(1, p, y, h) + at] - slope
                    target[(2, p, y, h) + at] = base[(2, p, y, h) + at] + kz * turned

        every_tile(body)

    def finish_and_reverse(h):
        def body(at, sub, column):
            kx, kz = waves(h, sub, column)
            wide = pressure_at(h, at, False)
            turn = corner[(edge_at, h) + at]
            own = schur[(edge, edge, h) + at]
            stream, normal, across_span = [], [], []
            for p in range(2):
                sign = 1.0 if p == 0 else -1.0
                far = rim[(0, h, p, 1 - edge_at) + at]
                known = direct[(p, edge) + at] + has_above * (own * far)
                inner_row = rim[(0, h, p, edge_at) + at] + turn * known
                edge_row = has_below * wide[p][rows] + has_above * wide[p][1]
                outside = beyond[(h, p) + at] + 0.5 * (has_above - has_below) * (inner_row - edge_row)
                lines = [has_above * outside]
                for y in range(rows):
                    turned = sign * wide[1 - p][y + 1]
                    slope = 0.5 * (wide[p][y + 2] - wide[p][y])
                    stream.append(base[(0, p, y, h) + at] - drag_term[(p, y) + at] + kx * turned)
                    lines.append(base[(1, p, y, h) + at] - slope)
                    across_span.append(base[(2, p, y, h) + at] + kz * turned)
                    final[(0, p, y, h) + at] = stream[-1]
                    final[(1, p, y, h) + at] = lines[-1]
                    final[(2, p, y, h) + at] = across_span[-1]
                normal.append(lines + [has_below * outside])
            values = []
            for p in range(2):
                sign = -1.0 if p == 0 else 1.0
                values.append(
                    [
                        sign * (kx * stream[rows * (1 - p) + y] + kz * across_span[rows * (1 - p) + y])
                        + 0.5 * (normal[p][y + 2] - normal[p][y])
                        for y in range(rows)
                    ]
                )
            for p in range(2):
                for y in range(rows):
                    source[(p, y, h) + at] = values[p][y]

        every_tile(body)

        def reverse(at, sub, column):
            values = [[source[(p, y, h) + at] for y in range(rows)] for p in range(2)]
            apply_blocks(h, at, values, True)

        every_tile(reverse)

    def finish_adjoint(h):
        def body(at, sub, column):
            kx, kz = waves(h, sub, column)
            wide = pressure_at(h, at, True)
            for p in range(2):
                sign = 1.0 if p == 0 else -1.0
                total = None
                for y in range(rows):
                    turned = sign * wide[1 - p][y + 1]
                    normal = final[(1, p, y, h) + at] - 0.5 * (wide[p][y + 2] - wide[p][y])
                    fields[(0, p, y, h) + at] = final[(0, p, y, h) + at] + kx * turned
                    fields[(1, p, y, h) + at] = normal
                    fields[(2, p, y, h) + at] = final[(2, p, y, h) + at] + kz * turned
                    term = lift[slab * rows + y] * normal
                    total = term if total is None else total + term
                wall[(p, h) + at] = total

        every_tile(body)

    def start_reply():
        reach_up = [has_above * lift[slab * (rows - 1)]] + [lift[slab * rows + y] for y in range(rows - 1)]
        reach_down = [lift[slab * rows + y] for y in range(1, rows)] + [has_below * lift[rows]]
        lift_slope = [0.5 * (down - up) for up, down in zip(reach_up, reach_down)]

        def body(h):
            def tile(at, sub, column):
                for i in range(rows):
                    total = None
                    for j in range(rows):
                        term = schur[(i, j, h) + at] * lift_slope[j]
                        total = term if total is None else total + term
                    reply[(i, h) + at] = total

            every_tile(tile)

        every_half(body)
        reply_copy.start()

    def finish_reply():
        reply_copy.wait_recv()
        reply_copy.wait_send()

        def body(h):
            def tile(at, sub, column):
                far = reply_rim[(h,) + at]
                outer = far + has_below * (corner[(1 - edge_at, h) + at] * reply[(edge, h) + at])
                for y in range(rows):
                    reply[(y, h) + at] = reply[(y, h) + at] + schur[(y, edge, h) + at] * outer

            every_tile(tile)

        every_half(body)

    def close_wall(h, g):
        def body(at, sub, column):
            kx, _ = waves(h, sub, column)
            kx = kx * mode_weight(h, sub)
            for p in range(2):
                sign = 1.0 if p == 0 else -1.0
                total = wall[(p, h) + at]
                for y in range(QUAD * g, QUAD * (g + 1)):
                    value = source[(p, y, h) + at] + sign * (kx * drag_term[(1 - p, y) + at])
                    total = total + reply[(y, h) + at] * value
                wall[(p, h) + at] = total

        every_tile(body)

    def start_halos(h):
        for copy in halo_copies(h):
            copy.start()

    def spread_all(forced):
        def body(h):
            for copy in halo_copies(h):
                copy.wait_recv()
                copy.wait_send()
            spread(h, forced)

        every_half(body)

    loads["stream"].wait()
    loads["span"].wait()
    for name in ("lift", "control", "forward", "rest", "schur", "drag", "inverse"):
        loads[name].start()
    for g in range(chunks):
        pack_first(0, True, g, g + 1)
        if g == 0:
            pl.semaphore_wait(barrier, count)
        first(0, g).start()
    pack_first(1, True)
    first(1, 0).start()

    loads["control"].wait()
    loads["forward"].wait()
    lines = control[...]
    blank = jnp.zeros((LANES - lines.shape[0], stream_len), jnp.float32)
    fill_pair(pair, slice(None), jnp.concatenate([lines, blank], axis=0).T)

    half = forward.shape[1] // HALVES
    places = pl.ds(pl.multiple_of(slab * half, half), half)
    y = mxu(forward[0, places, :], pair[...])
    y = y[:, :LANES] + (y[:, LANES:] + mxu(forward[1, places, :], pair[:, :LANES]))
    y = y.reshape(count, QUAD, SUBLANES, LANES)
    moved = y[:, 0]
    for j in range(1, QUAD):
        moved = moved + pltpu.roll(y[:, j], j * LANES // QUAD, 2)
    outc[...] = moved
    third.start()
    loads["rest"].wait()
    every_half(start_halos)
    loads["schur"].wait()
    loads["lift"].wait()
    corner_copy.start()
    start_reply()
    loads["drag"].wait()
    for g in range(chunks):
        drag[g] = drag_raw[QUAD * g : QUAD * (g + 1)].reshape(LANES, stream_len).T
    loads["inverse"].wait()
    physical(False)

    third.arrive()
    columns = []
    for group in range(groups):
        pieces = [inc[QUAD * group + i] for i in range(QUAD)]
        columns.append(jnp.concatenate(swap_groups(pieces), axis=0))
    w = span_product(jnp.concatenate(columns, axis=1), span)
    control_hat[0, slab] = w[:width, :span_count] + w[width:, span_count:]
    control_hat[1, slab] = w[width:, :span_count] - w[:width, span_count:]
    third.finish()
    control_copy.start()
    corner_copy.wait_recv()
    corner_copy.wait_send()
    finish_reply()
    control_copy.wait_recv()
    control_copy.wait_send()
    spread_all(True)
    send_rest()

    def step(h):
        receive(h)
        begin_solve(h)
        swap_rims(h, 0)
        finish_solve(h, fields)
        send_first(h, True)
        start_halos(h)

    every_half(step)
    physical(True)
    spread_all(True)
    send_rest()

    def turn(h):
        receive(h)
        begin_solve(h)
        swap_rims(h, 0)
        finish_and_reverse(h)
        swap_rims(h, 1)
        finish_adjoint(h)
        send_first(h, False)
        start_halos(h)

    every_half(turn)
    physical(True)
    spread_all(False)
    send_rest()

    def close(h):
        for g in range(chunks):
            second(h, g).arrive()
            if g == chunks - 1:

                @pl.when(h == 0)
                def _():
                    for later in range(1, chunks):
                        second(1, later).start()

                @pl.when(h == 1)
                def _():
                    fourth(0).start()

            collect(h, g, g + 1)
            close_wall(h, g)
        w = span_product(wall[:, h].reshape(2 * width, span_count), span)
        halfway = (
            w[:width, :span_count] - w[width:, span_count:],
            w[:width, span_count:] + w[width:, :span_count],
        )
        for group in range(groups):
            lanes = slice(LANES * group, LANES * (group + 1))
            pieces = [half[at : at + SUBLANES, lanes] for half in halfway for at in range(0, width, SUBLANES)]
            for i, tile in enumerate(swap_groups(pieces)):
                outp[h, QUAD * group + i] = tile

    def open_plane(h):
        fourth(h).arrive()
        copy = plane_copy(h)
        copy.start()
        copy.wait_recv()
        copy.wait_send()
        x = inp[h] + inp_other[h]
        turned = [x] + [pltpu.roll(x, LANES - j * LANES // QUAD, 2) for j in range(1, QUAD)]
        x = jnp.concatenate(turned, axis=1).reshape(-1, LANES)
        terms = slice(h * x.shape[0], (h + 1) * x.shape[0])
        fill_pair(pair, terms, x)
        places = pl.ds(pl.multiple_of(slab * gradient.shape[1], LANES), gradient.shape[1])
        y = mxu(inverse[0, places, terms], pair[terms, :])
        return y[:, :LANES] + (y[:, LANES:] + mxu(inverse[1, places, terms], pair[terms, :LANES]))

    every_half(close)
    fourth(1).start()
    share[...] = open_plane(0)
    gradient[...] = (share[...] + open_plane(1)).T[: gradient.shape[0]]
    for h in range(HALVES):
        fourth(h).finish()
    for g in range(chunks):
        second(1, g).finish()


VMEM = pl.BlockSpec(memory_space=pltpu.VMEM)
FAR = pl.BlockSpec(memory_space=pltpu.HBM)


def fused_call(count, initial_state, drag_rate, wall_control, lift_profile, schur_inverse):
    _, _, rows, modes, span_count = initial_state.shape
    stream_len = drag_rate.shape[2]
    narrow = wall_control.shape[0]
    width = modes // HALVES
    chunks = rows // QUAD
    span, inverse, forward = host_tables(stream_len, span_count, count)
    state = initial_state.reshape(3, 2, rows, HALVES, width, span_count)
    schur = schur_inverse.reshape(rows, rows, HALVES, width, span_count)
    plane = (2, rows, HALVES, width, span_count)
    half_plane = (2, rows, width, span_count)
    box = (HALVES, chunks, count, 2, width, LANES)
    thin = (HALVES, count, SUBLANES, LANES)
    line = (HALVES, 2, width, span_count)

    kept = 4 * (math.prod(state.shape) + narrow * stream_len // 2 + 16 * SUBLANES * LANES)

    def buffer(*shape):
        return pltpu.VMEM(shape, jnp.float32)

    pairs = pltpu.VMEM((stream_len, 2 * LANES), jnp.bfloat16)
    scratch = [pltpu.SMEM(lift_profile.shape, jnp.float32)] + [buffer(*state.shape)] * 2 + [buffer(*plane), buffer(*half_plane), buffer(*half_plane)]
    scratch += [buffer(*schur.shape), buffer(*drag_rate.shape), buffer(chunks, stream_len, LANES)]
    scratch += [buffer(*wall_control.shape), buffer(*line)]
    scratch += [pltpu.VMEM(table.shape, jnp.bfloat16) for table in (span, inverse, forward)]
    scratch += [buffer(*box)] * 4 + [pairs, pltpu.VMEM((chunks, stream_len, 2 * LANES), jnp.bfloat16), buffer(chunks, stream_len, LANES)] + [buffer(*thin[1:])] * 2 + [buffer(*thin)] * 2
    scratch += [buffer(*line), buffer(HALVES, 2, 2, width, span_count), buffer(*line), buffer(*line)]
    scratch += [buffer(2, HALVES, 2, 2, width, span_count), buffer(2, HALVES, width, span_count), buffer(*line)]
    scratch += [buffer(rows, HALVES, width, span_count), buffer(HALVES, width, span_count)]
    scratch += [buffer(*thin), buffer(stream_len // 2, LANES)]
    scratch += [pltpu.SemaphoreType.DMA((9,))]
    scratch += [pltpu.SemaphoreType.DMA((2, HALVES, chunks))] * 2
    scratch += [pltpu.SemaphoreType.DMA((2, HALVES))] * 2
    scratch += [pltpu.SemaphoreType.DMA((6 * HALVES + 3,))] * 2
    final, gradient = pl.pallas_call(
        functools.partial(fused_kernel, count, stream_len),
        out_shape=[
            pltpu.VMEM(state.shape, jnp.float32),
            pltpu.VMEM((narrow, stream_len // 2), jnp.float32),
        ],
        in_specs=[FAR] * 8,
        out_specs=[VMEM, VMEM],
        scratch_shapes=scratch,
        compiler_params=pltpu.CompilerParams(
            collective_id=0, has_side_effects=True, vmem_limit_bytes=VMEM_BYTES - kept
        ),
        cost_estimate=pl.CostEstimate(flops=60_000_000_000, bytes_accessed=32_000_000, transcendentals=0),
    )(lift_profile, state, drag_rate, wall_control, schur, span, inverse, forward)
    return final.reshape(initial_state.shape), gradient


def phase_pair(outer_size, inner_size, period, factor):
    outer_ids = jnp.arange(outer_size, dtype=jnp.int32)[:, None]
    inner_ids = jnp.arange(inner_size, dtype=jnp.int32)[None, :]
    angle = 2.0 * math.pi / period * (outer_ids * inner_ids % period).astype(jnp.float32)
    return (jnp.cos(angle) * factor, jnp.sin(angle) * factor)


def plain_transforms(count, rows, modes, span_count, stream_len):
    half_len = stream_len // 2
    cos_x, sin_x = phase_pair(stream_len, half_len, stream_len, 1.0 / math.sqrt(stream_len))
    cos_z, sin_z = phase_pair(span_count, span_count, span_count, 1.0 / math.sqrt(span_count))

    def to_spectral(physical):
        real_half = jnp.einsum("yzn,nk->yzk", physical, cos_x, precision=HIGHEST)
        imag_half = -jnp.einsum("yzn,nk->yzk", physical, sin_x, precision=HIGHEST)
        halfway = jnp.stack([real_half, imag_half])
        pieces = lax.all_to_all(halfway, "xz", split_axis=3, concat_axis=2, tiled=True)
        with_cos = jnp.einsum("cyzk,zq->cykq", pieces, cos_z, precision=HIGHEST)
        with_sin = jnp.einsum("cyzk,zq->cykq", pieces, sin_z, precision=HIGHEST)
        return jnp.stack([with_cos[0] + with_sin[1], with_cos[1] - with_sin[0]])

    def to_physical(spectral):
        with_cos = jnp.einsum("cykq,qz->cykz", spectral, cos_z, precision=HIGHEST)
        with_sin = jnp.einsum("cykq,qz->cykz", spectral, sin_z, precision=HIGHEST)
        halfway = jnp.stack([with_cos[0] - with_sin[1], with_sin[0] + with_cos[1]])
        pieces = lax.all_to_all(halfway, "xz", split_axis=3, concat_axis=2, tiled=True)
        return jnp.einsum("ykz,nk->yzn", pieces[0], cos_x, precision=HIGHEST) - jnp.einsum(
            "ykz,nk->yzn", pieces[1], sin_x, precision=HIGHEST
        )

    def begin(drag_rate, control):
        def drag_map(s):
            return to_spectral(drag_rate * to_physical(s))

        return drag_map, (lambda s: (drag_map(s), to_spectral(control[None])[:, 0]))

    def plane(spectral):
        return to_physical(spectral[:, None])[0]

    return begin, plane


def rotate(spectrum, factor):
    return jnp.stack([-factor * spectrum[1], factor * spectrum[0]])


def per_device(initial_state, drag_rate, wall_control, lift_profile, schur_inverse):
    row_count = initial_state.shape[2]
    mode_count = initial_state.shape[3]
    span_count = initial_state.shape[4]
    stream_len = drag_rate.shape[2]
    last_row = row_count - 1
    slab_count = lax.axis_size("gy")
    slab_index = lax.axis_index("gy")
    pencil_count = lax.axis_size("xz")
    pencil_index = lax.axis_index("xz")
    mode_ids = pencil_index * mode_count + jnp.arange(mode_count)
    stream_factor = (2.0 * math.pi / stream_len * mode_ids.astype(jnp.float32))[:, None]
    mode_weight = jnp.where(mode_ids == 0, 1.0, 2.0).astype(jnp.float32)[:, None]
    span_ids = jnp.arange(span_count)
    signed = jnp.where(span_ids < span_count // 2, span_ids, span_ids - span_count)
    span_wave = jnp.where(
        span_ids == span_count // 2, 0.0, 2.0 * math.pi / span_count * signed.astype(jnp.float32)
    )
    wave_square = stream_factor**2 + span_wave[None, :] ** 2
    fits = (
        slab_count == 2
        and QUAD * mode_count == LANES
        and QUAD * drag_rate.shape[1] == LANES
        and row_count == SUBLANES
        and pencil_count * mode_count * 2 == stream_len
        and pencil_count * drag_rate.shape[1] == span_count
        and pencil_count & (pencil_count - 1) == 0
        and pencil_count % QUAD == 0
    )
    if fits:
        return fused_call(pencil_count, initial_state, drag_rate, wall_control, lift_profile, schur_inverse)
    begin, plane = plain_transforms(pencil_count, row_count, mode_count, span_count, stream_len)
    drag_map, first_map = begin(drag_rate, wall_control)

    ends = slab_count - 1

    def from_above(tail):
        return lax.ppermute(tail, "gy", [(i, i + 1) for i in range(ends)])

    def from_below(head):
        return lax.ppermute(head, "gy", [(i + 1, i) for i in range(ends)])

    def every_slab(values):
        if slab_count == 2:
            other = lax.ppermute(values, "gy", [(0, 1), (1, 0)])
            return [jnp.where(slab_index == 0, values, other), jnp.where(slab_index == 0, other, values)]
        gathered = lax.all_gather(values, "gy", axis=0)
        return [gathered[i] for i in range(slab_count)]

    has_above = (slab_index > 0).astype(jnp.float32)
    has_below = (slab_index < slab_count - 1).astype(jnp.float32)
    corners = every_slab(
        jnp.stack(
            [
                schur_inverse[0, 0],
                schur_inverse[0, last_row],
                schur_inverse[last_row, 0],
                schur_inverse[last_row, last_row],
            ]
        )
    )
    corner_above = jnp.zeros_like(corners[0][3])
    for member in range(slab_count - 1):
        corner_above = jnp.where(slab_index == member + 1, corners[member][3], corner_above)

    padded_lift = jnp.pad(lift_profile, 1)
    lift_near = lax.dynamic_slice_in_dim(padded_lift, slab_index * row_count, row_count + 2)
    lift_own = lift_near[1 : row_count + 1]

    def halos(fields):
        tail = jnp.concatenate([fields[0, :, last_row:], fields[1, :, last_row - 1 :], fields[2, :, last_row:]], axis=1)
        head = jnp.concatenate([fields[0, :, :1], fields[1, :, :2], fields[2, :, :1]], axis=1)
        return from_above(tail), from_below(head)

    def smooth(wide):
        own = wide[:, 1:-1]
        laplace = wide[:, 2:] - 2.0 * own + wide[:, :-2]
        return own + DIFFUSION * (laplace - wave_square * own)

    def slope(wide):
        return 0.5 * (wide[:, 2:] - wide[:, :-2])

    def advance(fields, drag_term, control_hat):
        above, below = halos(fields)
        stream_star = smooth(jnp.concatenate([above[:, 0:1], fields[0], below[:, 0:1]], axis=1)) - drag_term
        span_star = smooth(jnp.concatenate([above[:, 3:4], fields[2], below[:, 3:4]], axis=1))
        normal_wide = smooth(jnp.concatenate([above[:, 1:3], fields[1], below[:, 1:3]], axis=1))
        if control_hat is not None:
            normal_wide = normal_wide + lift_near[:, None, None] * control_hat[:, None]
        normal_wide = jnp.concatenate(
            [has_above * normal_wide[:, :1], normal_wide[:, 1:-1], has_below * normal_wide[:, -1:]], axis=1
        )
        return stream_star, normal_wide[:, 1:-1], span_star, slope(normal_wide)

    def apply_blocks(values, transposed):
        summed = None
        for column in range(row_count):
            factor = schur_inverse[column] if transposed else schur_inverse[:, column]
            term = factor[None] * values[:, column : column + 1]
            summed = term if summed is None else summed + term
        return summed

    def solve(source, transposed):
        if transposed:
            first_column, last_column = schur_inverse[0], schur_inverse[last_row]
            ratio_at, turn_at = 1, 2
        else:
            first_column, last_column = schur_inverse[:, 0], schur_inverse[:, last_row]
            ratio_at, turn_at = 2, 1
        direct = apply_blocks(source, transposed)
        rims = every_slab(jnp.stack([direct[:, 0], direct[:, last_row]]))
        running = jnp.zeros_like(direct[:, 0])
        before = []
        for member in range(slab_count):
            before.append(running)
            running = rims[member][1] + corners[member][ratio_at][None] * running
        running = jnp.zeros_like(direct[:, 0])
        behind = [running] * slab_count
        for member in reversed(range(slab_count)):
            behind[member] = running
            top = rims[member][0] + corners[member][0][None] * before[member]
            running = top + corners[member][turn_at][None] * running
        entering, leaving = before[0], behind[0]
        for member in range(1, slab_count):
            entering = jnp.where(slab_index == member, before[member], entering)
            leaving = jnp.where(slab_index == member, behind[member], leaving)
        pressure = direct + first_column[None] * entering[:, None] + last_column[None] * leaving[:, None]
        row_above = entering + corner_above[None] * pressure[:, 0]
        return jnp.concatenate([row_above[:, None], pressure, leaving[:, None]], axis=1)

    def project(stream_part, normal_part, span_part, normal_slope, transposed):
        divergence = rotate(stream_part, stream_factor) + normal_slope + rotate(span_part, span_wave)
        wide = solve(divergence, transposed)
        pressure = wide[:, 1:-1]
        return jnp.stack(
            [
                stream_part - rotate(pressure, stream_factor),
                normal_part - slope(wide),
                span_part - rotate(pressure, span_wave),
            ]
        )

    fields = initial_state
    control_hat = None
    for section_index in range(STEPS):
        weighted = mode_weight * fields[0]
        if section_index == 0:
            drag_term, control_hat = first_map(weighted)
        else:
            drag_term = drag_map(weighted)
        fields = project(*advance(fields, drag_term, control_hat), False)
    final = fields
    normal_slope = slope(
        jnp.concatenate([from_above(final[1, :, last_row:]), final[1], from_below(final[1, :, :1])], axis=1)
    )
    parts = (final[0], final[1], final[2], normal_slope)
    wall_sum = jnp.zeros_like(control_hat)
    for section_index in range(STEPS):
        projected = project(*parts, True)
        wall_sum = wall_sum + jnp.sum(lift_own[:, None, None] * projected[1], axis=1)
        if section_index + 1 < STEPS:
            parts = advance(projected, mode_weight * drag_map(projected[0]), None)
    share = plane(wall_sum)
    if slab_count == 2:
        half = stream_len // 2
        first, second = share[:, :half], share[:, half:]
        upper = slab_index == 0
        other = lax.ppermute(jnp.where(upper, second, first), "gy", [(0, 1), (1, 0)])
        control_gradient = jnp.where(upper, first, second) + other
    else:
        control_gradient = lax.psum_scatter(share, "gy", scatter_dimension=1, tiled=True)
    return (final, control_gradient)


def solution(mesh):
    return jax.shard_map(
        per_device,
        mesh=mesh,
        in_specs=(
            P(None, None, "gy", "xz", None),
            P("gy", "xz", None),
            P("xz", None),
            P(),
            P("gy", None, "xz", None),
        ),
        out_specs=(P(None, None, "gy", "xz", None), P("xz", "gy")),
        check_vma=False,
    )
```

```python
import functools
import math

import jax
import jax.numpy as jnp
import ml_dtypes
import numpy as np
from jax import lax
from jax.experimental import pallas as pl
from jax.experimental.pallas import tpu as pltpu
from jax.sharding import PartitionSpec as P

STEPS = 2


DIFFUSION = 0.04
HIGHEST = lax.Precision.HIGHEST
MESH = pl.DeviceIdType.MESH
LANES = 128
QUAD = 4
HALVES = 2
SUBLANES = 8
FAR_FIRST = (3, 2, 0, 1)
VMEM_BYTES = 67_043_328


def split_host(table):
    high = table.astype(ml_dtypes.bfloat16)
    low = (table - high.astype(np.float64)).astype(ml_dtypes.bfloat16)
    return np.stack([high, low])


def host_tables(stream_len, span_count, count):
    z = np.arange(span_count)
    angle = 2.0 * math.pi / span_count * (np.outer(z, z) % span_count)
    span = np.concatenate([np.cos(angle), np.sin(angle)], axis=1) / math.sqrt(span_count)
    n = np.arange(stream_len)
    k = np.arange(stream_len // 2)
    angle = 2.0 * math.pi / stream_len * (np.outer(k, n) % stream_len)
    stream = np.stack([np.cos(angle), -np.sin(angle)]) / math.sqrt(stream_len)
    stream = stream.reshape(2, count, HALVES, -1, stream_len).transpose(2, 1, 0, 3, 4).reshape(-1, stream_len)
    return split_host(span), split_host(stream.T.copy()), split_host(stream)


def split_pair(x):
    high = x.astype(jnp.bfloat16)
    low = (x - high.astype(jnp.float32)).astype(jnp.bfloat16)
    return high, low


def mxu(a, b):
    return jnp.dot(a, b, preferred_element_type=jnp.float32)


def span_product(x, table):
    high, low = split_pair(x)
    both = mxu(jnp.concatenate([high, low], axis=0), table[0])
    return both[: x.shape[0]] + (both[x.shape[0] :] + mxu(high, table[1]))


def split_product(table, rows, terms, pair):
    wide = mxu(table[0, rows, terms], pair[...])
    narrow = mxu(table[1, rows, terms], pair[:, :LANES])
    return wide[:, :LANES] + (wide[:, LANES:] + narrow)


def fill_pair(pair, rows, x):
    high, low = split_pair(x)
    pair[rows, :LANES] = high
    pair[rows, LANES:] = low


def swap_groups(tiles):
    a0, a1, a2, a3 = tiles
    group = lax.broadcasted_iota(jnp.int32, a0.shape, a0.ndim - 1) // (LANES // QUAD)
    lower = group < 2
    even = group % 2 == 0
    axis = a0.ndim - 1
    half = LANES // 2
    step = LANES // QUAD

    def far(x, y):
        return (
            jnp.where(lower, x, pltpu.roll(y, half, axis)),
            jnp.where(lower, pltpu.roll(x, half, axis), y),
        )

    def near(x, y):
        return (
            jnp.where(even, x, pltpu.roll(y, step, axis)),
            jnp.where(even, pltpu.roll(x, LANES - step, axis), y),
        )

    b0, b2 = far(a0, a2)
    b1, b3 = far(a1, a3)
    return near(b0, b1) + near(b2, b3)


def peer_at(count, me, step):
    peer = 0
    unit = 1
    while unit < count:
        peer = peer + lax.rem(lax.div(me, unit) + lax.div(step, unit), 2) * unit
        unit *= 2
    return peer


class Exchange:
    def __init__(self, peers, me, outbox, inbox, send_sem, recv_sem):
        self.peers, self.me = peers, me
        self.outbox, self.inbox, self.send_sem, self.recv_sem = outbox, inbox, send_sem, recv_sem

    def copy(self, src, dst, peer):
        return pltpu.make_async_remote_copy(
            src_ref=self.outbox.at[src],
            dst_ref=self.inbox.at[dst],
            send_sem=self.send_sem,
            recv_sem=self.recv_sem,
            device_id={"xz": peer},
            device_id_type=MESH,
        )

    def every(self):
        others = pl.ds(0, len(self.peers))
        return self.copy(others, others, self.peers[0])

    def start(self):
        for peer in self.peers:
            self.copy(peer, self.me, peer).start()
        self.inbox[self.me] = self.outbox[self.me]

    def arrive(self):
        self.every().wait_recv()

    def finish(self):
        self.every().wait_send()


def fused_kernel(count, stream_len, *refs):
    refs = list(refs)
    lift_far, state_far, drag_far, control_far, schur_far, span_far, inverse_far, forward_far = refs[:8]
    final, gradient = refs[8:10]
    (
        lift, fields, base, source, drag_term, direct, schur, drag_raw, drag, control, control_hat,
        span, inverse, forward, out1, in1, out2, in2, pair, damped, partial, outc, inc, outp, inp,
        halo_u, halo_v, halo_w, beyond, rim, corner, wall, reply, reply_rim, inp_other, share,
        load_sem, send_sem, recv_sem, plane_send, plane_recv, near_send, near_recv,
    ) = refs[10:]
    me = lax.axis_index("xz")
    slab = lax.axis_index("gy")
    rows, width, span_count = fields.shape[2], fields.shape[4], fields.shape[5]
    modes = HALVES * width
    chunks = rows // QUAD
    groups = count // QUAD
    tiles_q = span_count // LANES
    tiles = width // SUBLANES * tiles_q
    block = rows * width
    edge = (rows - 1) * (1 - slab)
    edge_pair = (rows - 2) * (1 - slab)
    edge_at = 1 - slab
    has_above = slab.astype(jnp.float32)
    has_below = 1.0 - has_above

    loads = {
        "stream": (state_far.at[0], fields.at[0]),
        "span": (span_far, span),
        "forward": (forward_far, forward),
        "control": (control_far, control),
        "inverse": (inverse_far, inverse),
        "drag": (drag_far, drag_raw),
        "rest": (state_far.at[1:3], fields.at[1:3]),
        "schur": (schur_far, schur),
        "lift": (lift_far, lift),
    }
    loads = {
        name: pltpu.make_async_copy(far, near, load_sem.at[i]) for i, (name, (far, near)) in enumerate(loads.items())
    }
    loads["stream"].start()
    loads["span"].start()
    order = sorted(range(1, count), key=lambda step: (FAR_FIRST[step * QUAD // count], -step))
    peers = [peer_at(count, me, step) for step in order]
    barrier = pltpu.get_barrier_semaphore()
    for peer in peers:
        pl.semaphore_signal(barrier, inc=1, device_id={"xz": peer}, device_id_type=MESH)
    pl.semaphore_signal(barrier, inc=1, device_id={"gy": 1 - slab}, device_id_type=MESH)

    def first(h, g):
        return Exchange(peers, me, out1.at[h, g], in1.at[h, g], send_sem.at[0, h, g], recv_sem.at[0, h, g])

    def second(h, g):
        return Exchange(peers, me, out2.at[h, g], in2.at[h, g], send_sem.at[1, h, g], recv_sem.at[1, h, g])

    third = Exchange(peers, me, outc, inc, plane_send.at[0, 0], plane_recv.at[0, 0])

    def fourth(h):
        return Exchange(peers, me, outp.at[h], inp.at[h], plane_send.at[1, h], plane_recv.at[1, h])

    def across(src, dst, index):
        return pltpu.make_async_remote_copy(
            src_ref=src,
            dst_ref=dst,
            send_sem=near_send.at[index],
            recv_sem=near_recv.at[index],
            device_id={"gy": 1 - slab},
            device_id_type=MESH,
        )

    def halo_copies(h):
        return [
            across(fields.at[0, :, edge, h], halo_u.at[h], h),
            across(fields.at[1, :, pl.ds(edge_pair, 2), h], halo_v.at[h], HALVES + h),
            across(fields.at[2, :, edge, h], halo_w.at[h], 2 * HALVES + h),
        ]

    def rim_copy(h, turn):
        return across(direct.at[:, pl.ds(edge_pair, 2)], rim.at[turn, h], (3 + turn) * HALVES + h)

    def plane_copy(h):
        return across(inp.at[h], inp_other.at[h], 5 * HALVES + h)

    corner_copy = across(schur.at[pl.ds(edge_pair, 2), edge], corner, 6 * HALVES)
    control_copy = across(control_hat.at[:, slab], control_hat.at[:, slab], 6 * HALVES + 2)
    reply_copy = across(reply.at[edge], reply_rim, 6 * HALVES + 1)

    def every_half(action):
        def body(h, carry):
            action(h)
            return carry

        lax.fori_loop(0, HALVES, body, 0)

    def every_tile(action):
        def body(t, carry):
            sub = lax.div(t, tiles_q)
            column = lax.rem(t, tiles_q)
            at = (
                pl.ds(pl.multiple_of(sub * SUBLANES, SUBLANES), SUBLANES),
                pl.ds(pl.multiple_of(column * LANES, LANES), LANES),
            )
            action(at, sub, column)
            return carry

        lax.fori_loop(0, tiles, body, 0)

    def mode_ids(h, sub):
        return me * modes + h * width + sub * SUBLANES + lax.broadcasted_iota(jnp.int32, (SUBLANES, LANES), 0)

    def waves(h, sub, column):
        kx = 2.0 * math.pi / stream_len * mode_ids(h, sub).astype(jnp.float32)
        q = column * LANES + lax.broadcasted_iota(jnp.int32, (SUBLANES, LANES), 1)
        signed = jnp.where(q < span_count // 2, q, q - span_count)
        kz = jnp.where(q == span_count // 2, 0.0, 2.0 * math.pi / span_count * signed.astype(jnp.float32))
        return kx, kz

    def mode_weight(h, sub):
        return jnp.where(mode_ids(h, sub) == 0, 1.0, 2.0)

    def pack_first(h, weighted, low=0, high=chunks):
        x = fields[0, :, QUAD * low : QUAD * high, h]
        if weighted:
            ids = me * modes + h * width + lax.broadcasted_iota(jnp.int32, x.shape, 2)
            x = x * jnp.where(ids == 0, 1.0, 2.0)
        size = x.shape[1] * width
        w = span_product(x.reshape(2 * size, span_count), span)
        halfway = (
            w[:size, :span_count] - w[size:, span_count:],
            w[:size, span_count:] + w[size:, :span_count],
        )
        for g in range(low, high):
            for part in range(2):
                for group in range(groups):
                    lanes = slice(LANES * group, LANES * (group + 1))
                    start = width * QUAD * (g - low)
                    parts = [halfway[part][start + width * y : start + width * (y + 1), lanes] for y in range(QUAD)]
                    for i, tile in enumerate(swap_groups(parts)):
                        out1[h, g, QUAD * group + i, part] = tile

    def send_first(h, weighted):
        pack_first(h, weighted)
        first(h, 0).start()

        @pl.when(h == 0)
        def _():
            for g in range(1, chunks):
                first(0, g).start()

    def every_tile_row(action):
        size = stream_len // HALVES

        def body(index, carry):
            action(pl.ds(pl.multiple_of(index * size, size), size))
            return carry

        lax.fori_loop(0, HALVES, body, 0)

    def return_half(h, g):
        y = split_product(forward, slice(h * block * 4, (h + 1) * block * 4), slice(None), damped.at[g])
        out2[h, g] = y.reshape(count, 2, width, LANES)

    def physical(again):
        early, late = slice(0, stream_len // HALVES), slice(stream_len // HALVES, stream_len)
        for g in range(1, chunks):
            first(1, g).start()
        for g in range(chunks):
            first(0, g).arrive()
            fill_pair(pair, early, in1[0, g].reshape(-1, LANES))

            def begin(at):
                partial[g, at, :] = split_product(inverse, at, early, pair.at[early])

            every_tile_row(begin)
        for g in range(chunks):
            first(1, g).arrive()
            fill_pair(pair, late, in1[1, g].reshape(-1, LANES))
            if again:
                second(1, g).finish()

            def damp(at):
                y = partial[g, at, :] + split_product(inverse, at, late, pair.at[late])
                fill_pair(damped.at[g], at, y * drag[g, at, :])

            every_tile_row(damp)
            return_half(0, g)
            second(0, g).start()
        for g in range(chunks):
            return_half(1, g)
            first(0, g).finish()
            first(1, g).finish()

    def send_rest():
        second(1, 0).start()
        for g in range(chunks):
            second(0, g).finish()

    def collect(h, low=0, high=chunks):
        parts = []
        for part in range(2):
            for g in range(low, high):
                columns = []
                for group in range(groups):
                    pieces = [in2[h, g, QUAD * group + i, part] for i in range(QUAD)]
                    columns.append(jnp.concatenate(swap_groups(pieces), axis=0))
                parts.append(jnp.concatenate(columns, axis=1))
        w = span_product(jnp.concatenate(parts, axis=0), span)
        size = w.shape[0] // 2
        shape = (size // width, width, span_count)
        lines = slice(QUAD * low, QUAD * high)
        drag_term[0, lines] = (w[:size, :span_count] + w[size:, span_count:]).reshape(shape)
        drag_term[1, lines] = (w[size:, :span_count] - w[:size, span_count:]).reshape(shape)

    def receive(h):
        for g in range(chunks):
            second(h, g).arrive()

        @pl.when(h == 0)
        def _():
            for g in range(1, chunks):
                second(1, g).start()

        collect(h)

    def spread(h, forced):
        def body(at, sub, column):
            kx, kz = waves(h, sub, column)
            keep = 1.0 - DIFFUSION * (2.0 + kx * kx + kz * kz)

            def smooth(lines):
                return [
                    lines[i] * keep + DIFFUSION * (lines[i - 1] + lines[i + 1]) for i in range(1, len(lines) - 1)
                ]

            def wide(halo, c, p):
                line = halo[(h, p) + at]
                return [has_above * line] + [fields[(c, p, y, h) + at] for y in range(rows)] + [has_below * line]

            stream = [smooth(wide(halo_u, 0, p)) for p in range(2)]
            across_span = [smooth(wide(halo_w, 2, p)) for p in range(2)]
            for p in range(2):
                outer, inner = halo_v[(h, p, 0) + at], halo_v[(h, p, 1) + at]
                lines = [has_above * outer, has_above * inner]
                lines += [fields[(1, p, y, h) + at] for y in range(rows)]
                lines += [has_below * outer, has_below * inner]
                lines = smooth(lines)
                if forced:
                    hat = control_hat[(p, h) + at]
                    places = [slab * (rows - 1)] + [slab * rows + y for y in range(rows)] + [rows]
                    lines = [line + lift[place] * hat for line, place in zip(lines, places)]
                lines = [has_above * lines[0]] + lines[1:-1] + [has_below * lines[-1]]
                beyond[(h, p) + at] = lines[0] + lines[-1]
                if not forced:
                    total = wall[(p, h) + at]
                    for y in range(rows):
                        total = total + lift[slab * rows + y] * lines[y + 1]
                    wall[(p, h) + at] = total
                sign = -1.0 if p == 0 else 1.0
                for y in range(rows):
                    base[(0, p, y, h) + at] = stream[p][y]
                    base[(1, p, y, h) + at] = lines[y + 1]
                    base[(2, p, y, h) + at] = across_span[p][y]
                    turned = sign * (kx * stream[1 - p][y] + kz * across_span[1 - p][y])
                    source[(p, y, h) + at] = turned + 0.5 * (lines[y + 2] - lines[y])

        every_tile(body)

    def apply_blocks(h, at, values, transposed):
        for i in range(rows):
            totals = [None, None]
            for j in range(rows):
                place = (j, i) if transposed else (i, j)
                factor = schur[place + (h,) + at]
                for p in range(2):
                    term = factor * values[p][j]
                    totals[p] = term if totals[p] is None else totals[p] + term
            for p in range(2):
                direct[(p, i) + at] = totals[p]

    def begin_solve(h):
        def body(at, sub, column):
            kx, _ = waves(h, sub, column)
            values = [
                [source[(0, y, h) + at] + kx * drag_term[(1, y) + at] for y in range(rows)],
                [source[(1, y, h) + at] - kx * drag_term[(0, y) + at] for y in range(rows)],
            ]
            apply_blocks(h, at, values, False)

        every_tile(body)

    def swap_rims(h, turn):
        copy = rim_copy(h, turn)
        copy.start()
        copy.wait_recv()
        copy.wait_send()

    def pressure_at(h, at, transposed):
        turn = corner[(1 - edge_at, h) + at]
        reach = [schur[((edge, i) if transposed else (i, edge)) + (h,) + at] for i in range(rows)]
        own = schur[(edge, edge, h) + at]
        wide = []
        for p in range(2):
            far = rim[(int(transposed), h, p, 1 - edge_at) + at]
            known = direct[(p, edge) + at] + has_above * (own * far)
            next_row = far + turn * known
            outer = has_above * far + has_below * next_row
            inside = [direct[(p, y) + at] + reach[y] * outer for y in range(rows)]
            wide.append([has_above * next_row] + inside + [has_below * next_row])
        return wide

    def finish_solve(h, target):
        def body(at, sub, column):
            kx, kz = waves(h, sub, column)
            wide = pressure_at(h, at, False)
            for p in range(2):
                sign = 1.0 if p == 0 else -1.0
                for y in range(rows):
                    turned = sign * wide[1 - p][y + 1]
                    slope = 0.5 * (wide[p][y + 2] - wide[p][y])
                    target[(0, p, y, h) + at] = base[(0, p, y, h) + at] - drag_term[(p, y) + at] + kx * turned
                    target[(1, p, y, h) + at] = base[(1, p, y, h) + at] - slope
                    target[(2, p, y, h) + at] = base[(2, p, y, h) + at] + kz * turned

        every_tile(body)

    def finish_and_reverse(h):
        def body(at, sub, column):
            kx, kz = waves(h, sub, column)
            wide = pressure_at(h, at, False)
            turn = corner[(edge_at, h) + at]
            own = schur[(edge, edge, h) + at]
            stream, normal, across_span = [], [], []
            for p in range(2):
                sign = 1.0 if p == 0 else -1.0
                far = rim[(0, h, p, 1 - edge_at) + at]
                known = direct[(p, edge) + at] + has_above * (own * far)
                inner_row = rim[(0, h, p, edge_at) + at] + turn * known
                edge_row = has_below * wide[p][rows] + has_above * wide[p][1]
                outside = beyond[(h, p) + at] + 0.5 * (has_above - has_below) * (inner_row - edge_row)
                lines = [has_above * outside]
                for y in range(rows):
                    turned = sign * wide[1 - p][y + 1]
                    slope = 0.5 * (wide[p][y + 2] - wide[p][y])
                    stream.append(base[(0, p, y, h) + at] - drag_term[(p, y) + at] + kx * turned)
                    lines.append(base[(1, p, y, h) + at] - slope)
                    across_span.append(base[(2, p, y, h) + at] + kz * turned)
                    final[(0, p, y, h) + at] = stream[-1]
                    final[(1, p, y, h) + at] = lines[-1]
                    final[(2, p, y, h) + at] = across_span[-1]
                normal.append(lines + [has_below * outside])
            values = []
            for p in range(2):
                sign = -1.0 if p == 0 else 1.0
                values.append(
                    [
                        sign * (kx * stream[rows * (1 - p) + y] + kz * across_span[rows * (1 - p) + y])
                        + 0.5 * (normal[p][y + 2] - normal[p][y])
                        for y in range(rows)
                    ]
                )
            for p in range(2):
                for y in range(rows):
                    source[(p, y, h) + at] = values[p][y]

        every_tile(body)

        def reverse(at, sub, column):
            values = [[source[(p, y, h) + at] for y in range(rows)] for p in range(2)]
            apply_blocks(h, at, values, True)

        every_tile(reverse)

    def finish_adjoint(h):
        def body(at, sub, column):
            kx, kz = waves(h, sub, column)
            wide = pressure_at(h, at, True)
            for p in range(2):
                sign = 1.0 if p == 0 else -1.0
                total = None
                for y in range(rows):
                    turned = sign * wide[1 - p][y + 1]
                    normal = final[(1, p, y, h) + at] - 0.5 * (wide[p][y + 2] - wide[p][y])
                    fields[(0, p, y, h) + at] = final[(0, p, y, h) + at] + kx * turned
                    fields[(1, p, y, h) + at] = normal
                    fields[(2, p, y, h) + at] = final[(2, p, y, h) + at] + kz * turned
                    term = lift[slab * rows + y] * normal
                    total = term if total is None else total + term
                wall[(p, h) + at] = total

        every_tile(body)

    def start_reply():
        reach_up = [has_above * lift[slab * (rows - 1)]] + [lift[slab * rows + y] for y in range(rows - 1)]
        reach_down = [lift[slab * rows + y] for y in range(1, rows)] + [has_below * lift[rows]]
        lift_slope = [0.5 * (down - up) for up, down in zip(reach_up, reach_down)]

        def body(h):
            def tile(at, sub, column):
                for i in range(rows):
                    total = None
                    for j in range(rows):
                        term = schur[(i, j, h) + at] * lift_slope[j]
                        total = term if total is None else total + term
                    reply[(i, h) + at] = total

            every_tile(tile)

        every_half(body)
        reply_copy.start()

    def finish_reply():
        reply_copy.wait_recv()
        reply_copy.wait_send()

        def body(h):
            def tile(at, sub, column):
                far = reply_rim[(h,) + at]
                outer = far + has_below * (corner[(1 - edge_at, h) + at] * reply[(edge, h) + at])
                for y in range(rows):
                    reply[(y, h) + at] = reply[(y, h) + at] + schur[(y, edge, h) + at] * outer

            every_tile(tile)

        every_half(body)

    def close_wall(h, g):
        def body(at, sub, column):
            kx, _ = waves(h, sub, column)
            kx = kx * mode_weight(h, sub)
            for p in range(2):
                sign = 1.0 if p == 0 else -1.0
                total = wall[(p, h) + at]
                for y in range(QUAD * g, QUAD * (g + 1)):
                    value = source[(p, y, h) + at] + sign * (kx * drag_term[(1 - p, y) + at])
                    total = total + reply[(y, h) + at] * value
                wall[(p, h) + at] = total

        every_tile(body)

    def start_halos(h):
        for copy in halo_copies(h):
            copy.start()

    def spread_all(forced):
        def body(h):
            for copy in halo_copies(h):
                copy.wait_recv()
                copy.wait_send()
            spread(h, forced)

        every_half(body)

    loads["stream"].wait()
    loads["span"].wait()
    for name in ("lift", "control", "forward", "rest", "schur", "drag", "inverse"):
        loads[name].start()
    for g in range(chunks):
        pack_first(0, True, g, g + 1)
        if g == 0:
            pl.semaphore_wait(barrier, count)
        first(0, g).start()
    pack_first(1, True)
    first(1, 0).start()

    loads["control"].wait()
    loads["forward"].wait()
    lines = control[...]
    blank = jnp.zeros((LANES - lines.shape[0], stream_len), jnp.float32)
    fill_pair(pair, slice(None), jnp.concatenate([lines, blank], axis=0).T)

    half = forward.shape[1] // HALVES
    places = pl.ds(pl.multiple_of(slab * half, half), half)
    y = mxu(forward[0, places, :], pair[...])
    y = y[:, :LANES] + (y[:, LANES:] + mxu(forward[1, places, :], pair[:, :LANES]))
    y = y.reshape(count, QUAD, SUBLANES, LANES)
    moved = y[:, 0]
    for j in range(1, QUAD):
        moved = moved + pltpu.roll(y[:, j], j * LANES // QUAD, 2)
    outc[...] = moved
    third.start()
    loads["rest"].wait()
    every_half(start_halos)
    loads["schur"].wait()
    loads["lift"].wait()
    corner_copy.start()
    start_reply()
    loads["drag"].wait()
    for g in range(chunks):
        drag[g] = drag_raw[QUAD * g : QUAD * (g + 1)].reshape(LANES, stream_len).T
    loads["inverse"].wait()
    physical(False)

    third.arrive()
    columns = []
    for group in range(groups):
        pieces = [inc[QUAD * group + i] for i in range(QUAD)]
        columns.append(jnp.concatenate(swap_groups(pieces), axis=0))
    w = span_product(jnp.concatenate(columns, axis=1), span)
    control_hat[0, slab] = w[:width, :span_count] + w[width:, span_count:]
    control_hat[1, slab] = w[width:, :span_count] - w[:width, span_count:]
    third.finish()
    control_copy.start()
    corner_copy.wait_recv()
    corner_copy.wait_send()
    finish_reply()
    control_copy.wait_recv()
    control_copy.wait_send()
    spread_all(True)
    send_rest()

    def step(h):
        receive(h)
        begin_solve(h)
        swap_rims(h, 0)
        finish_solve(h, fields)
        send_first(h, True)
        start_halos(h)

    every_half(step)
    physical(True)
    spread_all(True)
    send_rest()

    def turn(h):
        receive(h)
        begin_solve(h)
        swap_rims(h, 0)
        finish_and_reverse(h)
        swap_rims(h, 1)
        finish_adjoint(h)
        send_first(h, False)
        start_halos(h)

    every_half(turn)
    physical(True)
    spread_all(False)
    send_rest()

    def close(h):
        for g in range(chunks):
            second(h, g).arrive()
            if g == chunks - 1:

                @pl.when(h == 0)
                def _():
                    for later in range(1, chunks):
                        second(1, later).start()

                @pl.when(h == 1)
                def _():
                    fourth(0).start()

            collect(h, g, g + 1)
            close_wall(h, g)
        w = span_product(wall[:, h].reshape(2 * width, span_count), span)
        halfway = (
            w[:width, :span_count] - w[width:, span_count:],
            w[:width, span_count:] + w[width:, :span_count],
        )
        for group in range(groups):
            lanes = slice(LANES * group, LANES * (group + 1))
            pieces = [half[at : at + SUBLANES, lanes] for half in halfway for at in range(0, width, SUBLANES)]
            for i, tile in enumerate(swap_groups(pieces)):
                outp[h, QUAD * group + i] = tile

    def open_plane(h):
        fourth(h).arrive()
        copy = plane_copy(h)
        copy.start()
        copy.wait_recv()
        copy.wait_send()
        x = inp[h] + inp_other[h]
        turned = [x] + [pltpu.roll(x, LANES - j * LANES // QUAD, 2) for j in range(1, QUAD)]
        x = jnp.concatenate(turned, axis=1).reshape(-1, LANES)
        terms = slice(h * x.shape[0], (h + 1) * x.shape[0])
        fill_pair(pair, terms, x)
        places = pl.ds(pl.multiple_of(slab * gradient.shape[1], LANES), gradient.shape[1])
        y = mxu(inverse[0, places, terms], pair[terms, :])
        return y[:, :LANES] + (y[:, LANES:] + mxu(inverse[1, places, terms], pair[terms, :LANES]))

    every_half(close)
    fourth(1).start()
    share[...] = open_plane(0)
    gradient[...] = (share[...] + open_plane(1)).T[: gradient.shape[0]]
    for h in range(HALVES):
        fourth(h).finish()
    for g in range(chunks):
        second(1, g).finish()


VMEM = pl.BlockSpec(memory_space=pltpu.VMEM)
FAR = pl.BlockSpec(memory_space=pltpu.HBM)


def fused_call(count, initial_state, drag_rate, wall_control, lift_profile, schur_inverse):
    _, _, rows, modes, span_count = initial_state.shape
    stream_len = drag_rate.shape[2]
    narrow = wall_control.shape[0]
    width = modes // HALVES
    chunks = rows // QUAD
    span, inverse, forward = host_tables(stream_len, span_count, count)
    state = initial_state.reshape(3, 2, rows, HALVES, width, span_count)
    schur = schur_inverse.reshape(rows, rows, HALVES, width, span_count)
    plane = (2, rows, HALVES, width, span_count)
    half_plane = (2, rows, width, span_count)
    box = (HALVES, chunks, count, 2, width, LANES)
    thin = (HALVES, count, SUBLANES, LANES)
    line = (HALVES, 2, width, span_count)

    kept = 4 * (math.prod(state.shape) + narrow * stream_len // 2 + 16 * SUBLANES * LANES)

    def buffer(*shape):
        return pltpu.VMEM(shape, jnp.float32)

    pairs = pltpu.VMEM((stream_len, 2 * LANES), jnp.bfloat16)
    scratch = [pltpu.SMEM(lift_profile.shape, jnp.float32)] + [buffer(*state.shape)] * 2 + [buffer(*plane), buffer(*half_plane), buffer(*half_plane)]
    scratch += [buffer(*schur.shape), buffer(*drag_rate.shape), buffer(chunks, stream_len, LANES)]
    scratch += [buffer(*wall_control.shape), buffer(*line)]
    scratch += [pltpu.VMEM(table.shape, jnp.bfloat16) for table in (span, inverse, forward)]
    scratch += [buffer(*box)] * 4 + [pairs, pltpu.VMEM((chunks, stream_len, 2 * LANES), jnp.bfloat16), buffer(chunks, stream_len, LANES)] + [buffer(*thin[1:])] * 2 + [buffer(*thin)] * 2
    scratch += [buffer(*line), buffer(HALVES, 2, 2, width, span_count), buffer(*line), buffer(*line)]
    scratch += [buffer(2, HALVES, 2, 2, width, span_count), buffer(2, HALVES, width, span_count), buffer(*line)]
    scratch += [buffer(rows, HALVES, width, span_count), buffer(HALVES, width, span_count)]
    scratch += [buffer(*thin), buffer(stream_len // 2, LANES)]
    scratch += [pltpu.SemaphoreType.DMA((9,))]
    scratch += [pltpu.SemaphoreType.DMA((2, HALVES, chunks))] * 2
    scratch += [pltpu.SemaphoreType.DMA((2, HALVES))] * 2
    scratch += [pltpu.SemaphoreType.DMA((6 * HALVES + 3,))] * 2
    final, gradient = pl.pallas_call(
        functools.partial(fused_kernel, count, stream_len),
        out_shape=[
            pltpu.VMEM(state.shape, jnp.float32),
            pltpu.VMEM((narrow, stream_len // 2), jnp.float32),
        ],
        in_specs=[FAR] * 8,
        out_specs=[VMEM, VMEM],
        scratch_shapes=scratch,
        compiler_params=pltpu.CompilerParams(
            collective_id=0, has_side_effects=True, vmem_limit_bytes=VMEM_BYTES - kept
        ),
        cost_estimate=pl.CostEstimate(flops=60_000_000_000, bytes_accessed=32_000_000, transcendentals=0),
    )(lift_profile, state, drag_rate, wall_control, schur, span, inverse, forward)
    return final.reshape(initial_state.shape), gradient


def phase_pair(outer_size, inner_size, period, factor):
    outer_ids = jnp.arange(outer_size, dtype=jnp.int32)[:, None]
    inner_ids = jnp.arange(inner_size, dtype=jnp.int32)[None, :]
    angle = 2.0 * math.pi / period * (outer_ids * inner_ids % period).astype(jnp.float32)
    return (jnp.cos(angle) * factor, jnp.sin(angle) * factor)


def plain_transforms(count, rows, modes, span_count, stream_len):
    half_len = stream_len // 2
    cos_x, sin_x = phase_pair(stream_len, half_len, stream_len, 1.0 / math.sqrt(stream_len))
    cos_z, sin_z = phase_pair(span_count, span_count, span_count, 1.0 / math.sqrt(span_count))

    def to_spectral(physical):
        real_half = jnp.einsum("yzn,nk->yzk", physical, cos_x, precision=HIGHEST)
        imag_half = -jnp.einsum("yzn,nk->yzk", physical, sin_x, precision=HIGHEST)
        halfway = jnp.stack([real_half, imag_half])
        pieces = lax.all_to_all(halfway, "xz", split_axis=3, concat_axis=2, tiled=True)
        with_cos = jnp.einsum("cyzk,zq->cykq", pieces, cos_z, precision=HIGHEST)
        with_sin = jnp.einsum("cyzk,zq->cykq", pieces, sin_z, precision=HIGHEST)
        return jnp.stack([with_cos[0] + with_sin[1], with_cos[1] - with_sin[0]])

    def to_physical(spectral):
        with_cos = jnp.einsum("cykq,qz->cykz", spectral, cos_z, precision=HIGHEST)
        with_sin = jnp.einsum("cykq,qz->cykz", spectral, sin_z, precision=HIGHEST)
        halfway = jnp.stack([with_cos[0] - with_sin[1], with_sin[0] + with_cos[1]])
        pieces = lax.all_to_all(halfway, "xz", split_axis=3, concat_axis=2, tiled=True)
        return jnp.einsum("ykz,nk->yzn", pieces[0], cos_x, precision=HIGHEST) - jnp.einsum(
            "ykz,nk->yzn", pieces[1], sin_x, precision=HIGHEST
        )

    def begin(drag_rate, control):
        def drag_map(s):
            return to_spectral(drag_rate * to_physical(s))

        return drag_map, (lambda s: (drag_map(s), to_spectral(control[None])[:, 0]))

    def plane(spectral):
        return to_physical(spectral[:, None])[0]

    return begin, plane


def rotate(spectrum, factor):
    return jnp.stack([-factor * spectrum[1], factor * spectrum[0]])


def per_device(initial_state, drag_rate, wall_control, lift_profile, schur_inverse):
    row_count = initial_state.shape[2]
    mode_count = initial_state.shape[3]
    span_count = initial_state.shape[4]
    stream_len = drag_rate.shape[2]
    last_row = row_count - 1
    slab_count = lax.axis_size("gy")
    slab_index = lax.axis_index("gy")
    pencil_count = lax.axis_size("xz")
    pencil_index = lax.axis_index("xz")
    mode_ids = pencil_index * mode_count + jnp.arange(mode_count)
    stream_factor = (2.0 * math.pi / stream_len * mode_ids.astype(jnp.float32))[:, None]
    mode_weight = jnp.where(mode_ids == 0, 1.0, 2.0).astype(jnp.float32)[:, None]
    span_ids = jnp.arange(span_count)
    signed = jnp.where(span_ids < span_count // 2, span_ids, span_ids - span_count)
    span_wave = jnp.where(
        span_ids == span_count // 2, 0.0, 2.0 * math.pi / span_count * signed.astype(jnp.float32)
    )
    wave_square = stream_factor**2 + span_wave[None, :] ** 2
    fits = (
        slab_count == 2
        and QUAD * mode_count == LANES
        and QUAD * drag_rate.shape[1] == LANES
        and row_count == SUBLANES
        and pencil_count * mode_count * 2 == stream_len
        and pencil_count * drag_rate.shape[1] == span_count
        and pencil_count & (pencil_count - 1) == 0
        and pencil_count % QUAD == 0
    )
    if fits:
        return fused_call(pencil_count, initial_state, drag_rate, wall_control, lift_profile, schur_inverse)
    begin, plane = plain_transforms(pencil_count, row_count, mode_count, span_count, stream_len)
    drag_map, first_map = begin(drag_rate, wall_control)

    ends = slab_count - 1

    def from_above(tail):
        return lax.ppermute(tail, "gy", [(i, i + 1) for i in range(ends)])

    def from_below(head):
        return lax.ppermute(head, "gy", [(i + 1, i) for i in range(ends)])

    def every_slab(values):
        if slab_count == 2:
            other = lax.ppermute(values, "gy", [(0, 1), (1, 0)])
            return [jnp.where(slab_index == 0, values, other), jnp.where(slab_index == 0, other, values)]
        gathered = lax.all_gather(values, "gy", axis=0)
        return [gathered[i] for i in range(slab_count)]

    has_above = (slab_index > 0).astype(jnp.float32)
    has_below = (slab_index < slab_count - 1).astype(jnp.float32)
    corners = every_slab(
        jnp.stack(
            [
                schur_inverse[0, 0],
                schur_inverse[0, last_row],
                schur_inverse[last_row, 0],
                schur_inverse[last_row, last_row],
            ]
        )
    )
    corner_above = jnp.zeros_like(corners[0][3])
    for member in range(slab_count - 1):
        corner_above = jnp.where(slab_index == member + 1, corners[member][3], corner_above)

    padded_lift = jnp.pad(lift_profile, 1)
    lift_near = lax.dynamic_slice_in_dim(padded_lift, slab_index * row_count, row_count + 2)
    lift_own = lift_near[1 : row_count + 1]

    def halos(fields):
        tail = jnp.concatenate([fields[0, :, last_row:], fields[1, :, last_row - 1 :], fields[2, :, last_row:]], axis=1)
        head = jnp.concatenate([fields[0, :, :1], fields[1, :, :2], fields[2, :, :1]], axis=1)
        return from_above(tail), from_below(head)

    def smooth(wide):
        own = wide[:, 1:-1]
        laplace = wide[:, 2:] - 2.0 * own + wide[:, :-2]
        return own + DIFFUSION * (laplace - wave_square * own)

    def slope(wide):
        return 0.5 * (wide[:, 2:] - wide[:, :-2])

    def advance(fields, drag_term, control_hat):
        above, below = halos(fields)
        stream_star = smooth(jnp.concatenate([above[:, 0:1], fields[0], below[:, 0:1]], axis=1)) - drag_term
        span_star = smooth(jnp.concatenate([above[:, 3:4], fields[2], below[:, 3:4]], axis=1))
        normal_wide = smooth(jnp.concatenate([above[:, 1:3], fields[1], below[:, 1:3]], axis=1))
        if control_hat is not None:
            normal_wide = normal_wide + lift_near[:, None, None] * control_hat[:, None]
        normal_wide = jnp.concatenate(
            [has_above * normal_wide[:, :1], normal_wide[:, 1:-1], has_below * normal_wide[:, -1:]], axis=1
        )
        return stream_star, normal_wide[:, 1:-1], span_star, slope(normal_wide)

    def apply_blocks(values, transposed):
        summed = None
        for column in range(row_count):
            factor = schur_inverse[column] if transposed else schur_inverse[:, column]
            term = factor[None] * values[:, column : column + 1]
            summed = term if summed is None else summed + term
        return summed

    def solve(source, transposed):
        if transposed:
            first_column, last_column = schur_inverse[0], schur_inverse[last_row]
            ratio_at, turn_at = 1, 2
        else:
            first_column, last_column = schur_inverse[:, 0], schur_inverse[:, last_row]
            ratio_at, turn_at = 2, 1
        direct = apply_blocks(source, transposed)
        rims = every_slab(jnp.stack([direct[:, 0], direct[:, last_row]]))
        running = jnp.zeros_like(direct[:, 0])
        before = []
        for member in range(slab_count):
            before.append(running)
            running = rims[member][1] + corners[member][ratio_at][None] * running
        running = jnp.zeros_like(direct[:, 0])
        behind = [running] * slab_count
        for member in reversed(range(slab_count)):
            behind[member] = running
            top = rims[member][0] + corners[member][0][None] * before[member]
            running = top + corners[member][turn_at][None] * running
        entering, leaving = before[0], behind[0]
        for member in range(1, slab_count):
            entering = jnp.where(slab_index == member, before[member], entering)
            leaving = jnp.where(slab_index == member, behind[member], leaving)
        pressure = direct + first_column[None] * entering[:, None] + last_column[None] * leaving[:, None]
        row_above = entering + corner_above[None] * pressure[:, 0]
        return jnp.concatenate([row_above[:, None], pressure, leaving[:, None]], axis=1)

    def project(stream_part, normal_part, span_part, normal_slope, transposed):
        divergence = rotate(stream_part, stream_factor) + normal_slope + rotate(span_part, span_wave)
        wide = solve(divergence, transposed)
        pressure = wide[:, 1:-1]
        return jnp.stack(
            [
                stream_part - rotate(pressure, stream_factor),
                normal_part - slope(wide),
                span_part - rotate(pressure, span_wave),
            ]
        )

    fields = initial_state
    control_hat = None
    for section_index in range(STEPS):
        weighted = mode_weight * fields[0]
        if section_index == 0:
            drag_term, control_hat = first_map(weighted)
        else:
            drag_term = drag_map(weighted)
        fields = project(*advance(fields, drag_term, control_hat), False)
    final = fields
    normal_slope = slope(
        jnp.concatenate([from_above(final[1, :, last_row:]), final[1], from_below(final[1, :, :1])], axis=1)
    )
    parts = (final[0], final[1], final[2], normal_slope)
    wall_sum = jnp.zeros_like(control_hat)
    for section_index in range(STEPS):
        projected = project(*parts, True)
        wall_sum = wall_sum + jnp.sum(lift_own[:, None, None] * projected[1], axis=1)
        if section_index + 1 < STEPS:
            parts = advance(projected, mode_weight * drag_map(projected[0]), None)
    share = plane(wall_sum)
    if slab_count == 2:
        half = stream_len // 2
        first, second = share[:, :half], share[:, half:]
        upper = slab_index == 0
        other = lax.ppermute(jnp.where(upper, second, first), "gy", [(0, 1), (1, 0)])
        control_gradient = jnp.where(upper, first, second) + other
    else:
        control_gradient = lax.psum_scatter(share, "gy", scatter_dimension=1, tiled=True)
    return (final, control_gradient)


def solution(mesh):
    return jax.shard_map(
        per_device,
        mesh=mesh,
        in_specs=(
            P(None, None, "gy", "xz", None),
            P("gy", "xz", None),
            P("xz", None),
            P(),
            P("gy", None, "xz", None),
        ),
        out_specs=(P(None, None, "gy", "xz", None), P("xz", "gy")),
        check_vma=False,
    )
```
